32 devices in a mesh: stage: 4 (over x, y), data: 8 (over z, core).
Axes of the slice: x: 2, y: 2, z: 4, core: 2. Of those that a mesh axis runs over, the one named last changes fastest.
Arguments:
- w_qkv: float32 [12, 1024, 2048], P('stage', 'data'), parts along dimension 0
- m_qkv: float32 [12, 1024, 2048], P('stage', 'data'), parts along dimension 0
- g_qkv: bfloat16 [12, 1024, 2048], P('stage', 'data'), parts along dimension 0
- w_out: float32 [12, 1024, 1024], P('stage', 'data'), parts along dimension 0
- m_out: float32 [12, 1024, 1024], P('stage', 'data'), parts along dimension 0
- g_out: bfloat16 [12, 1024, 1024], P('stage', 'data'), parts along dimension 0
- w_up: float32 [48, 1024, 512], P('stage', 'data'), parts along dimension 0
- m_up: float32 [48, 1024, 512], P('stage', 'data'), parts along dimension 0
- g_up: bfloat16 [48, 1024, 512], P('stage', 'data'), parts along dimension 0
- w_down: float32 [48, 512, 1024], P('stage', 'data'), parts along dimension 0
- m_down: float32 [48, 512, 1024], P('stage', 'data'), parts along dimension 0
- g_down: bfloat16 [48, 512, 1024], P('stage', 'data'), parts along dimension 0
Outputs:
- output 1: float32 [12, 1024, 2048], P('stage', 'data'), parts along dimension 0
- output 2: float32 [12, 1024, 2048], P('stage', 'data'), parts along dimension 0
- output 3: float32 [12, 1024, 1024], P('stage', 'data'), parts along dimension 0
- output 4: float32 [12, 1024, 1024], P('stage', 'data'), parts along dimension 0
- output 5: float32 [48, 1024, 512], P('stage', 'data'), parts along dimension 0
- output 6: float32 [48, 1024, 512], P('stage', 'data'), parts along dimension 0
- output 7: float32 [48, 512, 1024], P('stage', 'data'), parts along dimension 0
- output 8: float32 [48, 512, 1024], P('stage', 'data'), parts along dimension 0
There are 4 independent parts. The reference program is written for one: setup_inputs(seed, part) draws one part's arguments, and reference() takes and returns one part's arrays. A program takes and returns all parts, laid end to end along the dimension named above; each array names one.
All inputs are finite; a program needn't handle non-finite values.
Results may differ from the reference program's by a relative error of at most 0.00416286.
Values are sent between devices in bfloat16 or wider.
A program may use at most 1 GiB of HBM per device.

```python
import math
import jax
import jax.numpy as jnp
from jax import lax

D = 1024
HEADS = 16
KV_HEADS = 8
HEAD = 64
FE = 512
LAYERS = 3
EXPERTS_TAKEN = 4
NS_STEPS = 5

Q_WIDTH = HEADS * HEAD
QKV_WIDTH = (HEADS + 2 * KV_HEADS) * HEAD
EXPERT_MATS = LAYERS * EXPERTS_TAKEN
COEF_A = 3.4445
COEF_B = -4.7750
COEF_C = 2.0315
MOMENTUM = 0.95
LEARN_RATE = 0.04
DECAY = 0.2
NORM_EPS = 1e-7
RMS_MATCH = 0.2


def draw_stack(base_key, mat_count, row_count, col_count):
    sub_keys = jax.random.split(base_key, 7)
    mom_rows = jnp.exp(jax.random.uniform(sub_keys[0], (mat_count, row_count, 1), minval=-0.7, maxval=0.7))
    weight = 0.05 * jax.random.normal(sub_keys[1], (mat_count, row_count, col_count))
    left_fac = jax.random.normal(sub_keys[2], (mat_count, row_count, 4))
    right_fac = jax.random.normal(sub_keys[3], (mat_count, 4, col_count))
    shared = 0.3 * jnp.einsum("krj,kjc->krc", left_fac, right_fac)
    momentum = (jax.random.normal(sub_keys[4], (mat_count, row_count, col_count)) + shared) * mom_rows
    grad_rows = jnp.exp(jax.random.uniform(sub_keys[5], (mat_count, row_count, 1), minval=-0.7, maxval=0.7))
    gradient = jax.random.normal(sub_keys[6], (mat_count, row_count, col_count)) * grad_rows
    return weight, momentum, gradient.astype(jnp.bfloat16)


def setup_inputs(seed: int = 0, part: int = 0) -> dict:
    part_key = jax.random.fold_in(jax.random.key(seed), part)
    sub_keys = jax.random.split(part_key, 4)
    w_qkv, m_qkv, g_qkv = draw_stack(sub_keys[0], LAYERS, D, QKV_WIDTH)
    w_out, m_out, g_out = draw_stack(sub_keys[1], LAYERS, Q_WIDTH, D)
    w_up, m_up, g_up = draw_stack(sub_keys[2], EXPERT_MATS, D, FE)
    w_down, m_down, g_down = draw_stack(sub_keys[3], EXPERT_MATS, FE, D)
    return {"w_qkv": w_qkv, "m_qkv": m_qkv, "g_qkv": g_qkv,
            "w_out": w_out, "m_out": m_out, "g_out": g_out,
            "w_up": w_up, "m_up": m_up, "g_up": g_up,
            "w_down": w_down, "m_down": m_down, "g_down": g_down}


def orthogonalize(momentum):
    row_count, col_count = momentum.shape
    norm_val = jnp.sqrt(jnp.sum(momentum * momentum))
    x_mat = (momentum / (norm_val + NORM_EPS)).astype(jnp.bfloat16)
    for _ in range(NS_STEPS):
        if row_count > col_count:
            gram_mat = jnp.dot(x_mat.T, x_mat, preferred_element_type=jnp.float32).astype(jnp.bfloat16)
        else:
            gram_mat = jnp.dot(x_mat, x_mat.T, preferred_element_type=jnp.float32).astype(jnp.bfloat16)
        gram_sq = jnp.dot(gram_mat, gram_mat, preferred_element_type=jnp.float32)
        poly_mat = (COEF_B * gram_mat.astype(jnp.float32) + COEF_C * gram_sq).astype(jnp.bfloat16)
        if row_count > col_count:
            product = jnp.dot(x_mat, poly_mat, preferred_element_type=jnp.float32)
        else:
            product = jnp.dot(poly_mat, x_mat, preferred_element_type=jnp.float32)
        x_mat = (COEF_A * x_mat.astype(jnp.float32) + product).astype(jnp.bfloat16)
    return x_mat.astype(jnp.float32) * (RMS_MATCH * math.sqrt(max(row_count, col_count)))


def stack_update(weight, momentum, gradient):
    new_mom = MOMENTUM * momentum + gradient.astype(jnp.float32)
    ortho_out = lax.map(orthogonalize, new_mom)
    new_weight = weight - LEARN_RATE * (ortho_out + DECAY * weight)
    return new_weight, new_mom


def reference(w_qkv, m_qkv, g_qkv, w_out, m_out, g_out, w_up, m_up, g_up, w_down, m_down, g_down):
    new_w_qkv, new_m_qkv = stack_update(w_qkv, m_qkv, g_qkv)
    new_w_out, new_m_out = stack_update(w_out, m_out, g_out)
    new_w_up, new_m_up = stack_update(w_up, m_up, g_up)
    new_w_down, new_m_down = stack_update(w_down, m_down, g_down)
    return (new_w_qkv, new_m_qkv, new_w_out, new_m_out, new_w_up, new_m_up, new_w_down, new_m_down)
```

```python
import functools
import math
import jax
import jax.numpy as jnp
from jax import lax
from jax.experimental import pallas as pl
from jax.experimental.pallas import tpu as pltpu
from jax.sharding import PartitionSpec as P

NS_STEPS = 5
COEF_A = 3.4445
COEF_B = -4.7750
COEF_C = 2.0315
MOMENTUM = 0.95
LEARN_RATE = 0.04
DECAY = 0.2
NORM_EPS = 1e-7
RMS_MATCH = 0.2

GROUP = 8
MESH = pl.DeviceIdType.MESH
NT = (((1,), (1,)), ((), ()))
F32 = jnp.float32
BF16 = jnp.bfloat16

QKV_OWNER = (0, 1, 7)
OUT_OWNER = (2, 4, 6)
EXPERT_COUNT = (0, 0, 3, 8, 3, 7, 3, 0)
EXPERT_BASE = (0, 0, 0, 3, 11, 14, 21, 24)
EXPERT_OWNER = tuple(d for d in range(GROUP) for _ in range(EXPERT_COUNT[d]))
N_DOWN = 12
MAX_EXPERTS = 8


def send_order():
    halves = ([], [])
    sizes = {"q": 4, "o": 2, "e": 1}
    for kind, owners in (("q", QKV_OWNER), ("o", OUT_OWNER)):
        for index, owner in enumerate(owners):
            halves[owner // 4].append((kind, index))
    for half in range(2):
        devices = [d for d in range(4 * half, 4 * half + 4) if EXPERT_COUNT[d]]
        slots = []
        for d in devices:
            for t in range(EXPERT_COUNT[d]):
                slots.append(((t + 0.5) / EXPERT_COUNT[d], d, t))
        for _, d, t in sorted(slots):
            halves[half].append(("e", EXPERT_BASE[d] + t))
    order, sent, place = [], [0, 0], [0, 0]
    while place[0] < len(halves[0]) or place[1] < len(halves[1]):
        half = 0 if sent[0] <= sent[1] else 1
        if place[half] == len(halves[half]):
            half = 1 - half
        item = halves[half][place[half]]
        place[half] += 1
        sent[half] += sizes[item[0]]
        order.append(item)
    return order


ORDER = send_order()


def pick(table, me):
    total = jnp.int32(0)
    for d, value in enumerate(table):
        if value:
            total = total + jnp.where(me == d, jnp.int32(value), jnp.int32(0))
    return total


def ns_step(src, dst, gram, poly, m, block):
    def rows_of(i):
        return pl.ds(pl.multiple_of(i * block, block), block)

    @pl.loop(0, m // block)
    def _(i):
        rows = rows_of(i)
        gram[rows, :] = lax.dot_general(src[rows, :], src[...], NT, preferred_element_type=F32).astype(BF16)

    @pl.loop(0, m // block)
    def _(i):
        rows = rows_of(i)
        part = gram[rows, :]
        square = jnp.dot(part, gram[...], preferred_element_type=F32)
        poly[rows, :] = (COEF_B * part.astype(F32) + COEF_C * square).astype(BF16)

    @pl.loop(0, m // block)
    def _(i):
        rows = rows_of(i)
        product = jnp.dot(poly[rows, :], src[...], preferred_element_type=F32)
        dst[rows, :] = (COEF_A * src[rows, :].astype(F32) + product).astype(BF16)


def kernel(xq, xo, xd, xu, rq, ro, rd, ru, qbuf, obuf, ebuf, gram, poly, gram_e, poly_e,
           fwd_send, fwd_recv, ret_send, ret_recv):
    me = lax.axis_index("data")
    barrier = pltpu.get_barrier_semaphore()
    for k in range(1, GROUP):
        pl.semaphore_signal(barrier, inc=1, device_id={"data": lax.rem(me + k, GROUP)}, device_id_type=MESH)
    pl.semaphore_wait(barrier, GROUP - 1)

    def block_of(kind, index, slot_ref, d):
        if kind == "q" or kind == "o":
            return slot_ref.at[pl.ds(d * 128, 128), :]
        if kind == "d":
            return slot_ref.at[pl.ds(d * 64, 64), :]
        return slot_ref.at[:, pl.ds(d * 128, 128)]

    for number, (kind, index) in enumerate(ORDER):
        if kind == "q":
            owner, src, slot, sub, sem = QKV_OWNER[index], xq.at[index], qbuf.at[0], "q", index
        elif kind == "o":
            owner, src, slot, sub, sem = OUT_OWNER[index], xo.at[index], obuf.at[0], "o", 3 + index
        else:
            owner = EXPERT_OWNER[index]
            slot, sem = ebuf.at[index - EXPERT_BASE[owner]], 6 + index
            sub, src = ("d", xd.at[index]) if index < N_DOWN else ("u", xu.at[index - N_DOWN])

        @pl.when(me != owner)
        def _():
            pltpu.make_async_remote_copy(
                src_ref=src, dst_ref=block_of(sub, index, slot, me), send_sem=fwd_send.at[sem], recv_sem=fwd_recv.at[sem],
                device_id={"data": owner}, device_id_type=MESH).start()

        @pl.when(me == owner)
        def _():
            pltpu.make_async_copy(src, block_of(sub, index, slot, me), fwd_recv.at[sem]).start()

    def wait_whole(slot, sem):
        pltpu.make_async_copy(slot, slot, sem).wait()

    def give_back(kind, slot, out, send_sem, recv_sem):
        for k in range(1, GROUP):
            dst = lax.rem(me + k, GROUP)
            pltpu.make_async_remote_copy(
                src_ref=block_of(kind, 0, slot, dst), dst_ref=out, send_sem=send_sem, recv_sem=recv_sem,
                device_id={"data": dst}, device_id_type=MESH).start()
        pltpu.make_async_copy(block_of(kind, 0, slot, me), out, recv_sem).start()

    def wait_given(kind, slot, send_sem):
        rows = {"q": 896, "o": 896, "d": 448}
        part = slot.at[:, pl.ds(0, 896)] if kind == "u" else slot.at[pl.ds(0, rows[kind]), :]
        pltpu.make_async_copy(part, part, send_sem).wait()

    for index, owner in enumerate(QKV_OWNER):
        @pl.when(me == owner)
        def _():
            wait_whole(qbuf.at[0], fwd_recv.at[index])

    @pl.when((me == QKV_OWNER[0]) | (me == QKV_OWNER[1]) | (me == QKV_OWNER[2]))
    def _():
        @pl.loop(0, NS_STEPS)
        def _(it):
            now = lax.rem(it, 2)
            ns_step(qbuf.at[now], qbuf.at[1 - now], gram, poly, 1024, 256)

    for index, owner in enumerate(QKV_OWNER):
        @pl.when(me == owner)
        def _():
            give_back("q", qbuf.at[1], rq.at[index], ret_send.at[0], ret_recv.at[index])

    for index, owner in enumerate(OUT_OWNER):
        @pl.when(me == owner)
        def _():
            wait_whole(obuf.at[0], fwd_recv.at[3 + index])

    @pl.when((me == OUT_OWNER[0]) | (me == OUT_OWNER[1]) | (me == OUT_OWNER[2]))
    def _():
        @pl.loop(0, NS_STEPS)
        def _(it):
            now = lax.rem(it, 2)
            ns_step(obuf.at[now], obuf.at[1 - now], gram, poly, 1024, 256)

    for index, owner in enumerate(OUT_OWNER):
        @pl.when(me == owner)
        def _():
            give_back("o", obuf.at[1], ro.at[index], ret_send.at[1], ret_recv.at[3 + index])

    base, count = pick(EXPERT_BASE, me), pick(EXPERT_COUNT, me)

    @pl.loop(0, count)
    def _(t):
        rank = base + t
        wait_whole(ebuf.at[t], fwd_recv.at[6 + rank])

        @pl.loop(0, NS_STEPS)
        def _(it):
            src = jnp.where(it == 0, t, MAX_EXPERTS + lax.rem(it + 1, 2))
            dst = jnp.where(it == NS_STEPS - 1, t, MAX_EXPERTS + lax.rem(it, 2))
            ns_step(ebuf.at[src], ebuf.at[dst], gram_e, poly_e, 512, 256)

        @pl.when(rank < N_DOWN)
        def _():
            give_back("d", ebuf.at[t], rd.at[rank], ret_send.at[2 + t], ret_recv.at[6 + rank])

        @pl.when(rank >= N_DOWN)
        def _():
            give_back("u", ebuf.at[t], ru.at[rank - N_DOWN], ret_send.at[2 + t], ret_recv.at[6 + rank])

    for number, (kind, index) in enumerate(ORDER):
        if kind == "q":
            owner, src, out, sem = QKV_OWNER[index], xq.at[index], rq.at[index], index
        elif kind == "o":
            owner, src, out, sem = OUT_OWNER[index], xo.at[index], ro.at[index], 3 + index
        else:
            owner, sem = EXPERT_OWNER[index], 6 + index
            if index < N_DOWN:
                src, out = xd.at[index], rd.at[index]
            else:
                src, out = xu.at[index - N_DOWN], ru.at[index - N_DOWN]

        @pl.when(me != owner)
        def _():
            pltpu.make_async_copy(src, src, fwd_send.at[sem]).wait()

        pltpu.make_async_copy(out, out, ret_recv.at[sem]).wait()

    for owner in QKV_OWNER:
        @pl.when(me == owner)
        def _():
            wait_given("q", qbuf.at[1], ret_send.at[0])
    for owner in OUT_OWNER:
        @pl.when(me == owner)
        def _():
            wait_given("o", obuf.at[1], ret_send.at[1])

    @pl.loop(0, count)
    def _(t):
        @pl.when(base + t < N_DOWN)
        def _():
            wait_given("d", ebuf.at[t], ret_send.at[2 + t])

        @pl.when(base + t >= N_DOWN)
        def _():
            wait_given("u", ebuf.at[t], ret_send.at[2 + t])


def exchange(xq, xo, xd, xu):
    any_space = pl.BlockSpec(memory_space=pl.ANY)
    return pl.pallas_call(
        kernel,
        out_shape=[jax.ShapeDtypeStruct(x.shape, BF16) for x in (xq, xo, xd, xu)],
        in_specs=[any_space] * 4,
        out_specs=[any_space] * 4,
        scratch_shapes=[
            pltpu.VMEM((2, 1024, 2048), BF16),
            pltpu.VMEM((2, 1024, 1024), BF16),
            pltpu.VMEM((MAX_EXPERTS + 2, 512, 1024), BF16),
            pltpu.VMEM((1024, 1024), BF16),
            pltpu.VMEM((1024, 1024), BF16),
            pltpu.VMEM((512, 512), BF16),
            pltpu.VMEM((512, 512), BF16),
            pltpu.SemaphoreType.DMA((30,)),
            pltpu.SemaphoreType.DMA((30,)),
            pltpu.SemaphoreType.DMA((2 + MAX_EXPERTS,)),
            pltpu.SemaphoreType.DMA((30,)),
        ],
        compiler_params=pltpu.CompilerParams(
            collective_id=0, has_side_effects=True, vmem_limit_bytes=58 * 1024 * 1024),
    )(xq, xo, xd, xu)


def solution(mesh):
    row_spec = P("stage", "data", None)

    def local_step(w_qkv, m_qkv, g_qkv, w_out, m_out, g_out, w_up, m_up, g_up, w_down, m_down, g_down):
        moms, sums = [], []
        for momentum, gradient in ((m_qkv, g_qkv), (m_out, g_out), (m_up, g_up), (m_down, g_down)):
            new_mom = MOMENTUM * momentum + gradient.astype(F32)
            moms.append(new_mom)
            sums.append(jnp.sum(new_mom * new_mom, axis=(1, 2)))
        sums = lax.psum(tuple(sums), "data")
        scaled = [(m / (jnp.sqrt(s)[:, None, None] + NORM_EPS)).astype(BF16) for m, s in zip(moms, sums)]
        xq, xo, xu, xd = scaled
        rq, ro, rd, ru = exchange(xq, xo, xd, xu.transpose(0, 2, 1))
        results = []
        for weight, new_mom, back in ((w_qkv, moms[0], rq), (w_out, moms[1], ro), (w_up, moms[2], ru.transpose(0, 2, 1)),
                                      (w_down, moms[3], rd)):
            rms_scale = RMS_MATCH * math.sqrt(max(weight.shape[1] * GROUP, weight.shape[2]))
            results.append(weight - LEARN_RATE * (rms_scale * back.astype(F32) + DECAY * weight))
            results.append(new_mom)
        return tuple(results)

    return jax.shard_map(local_step, mesh=mesh, in_specs=(row_spec,) * 12, out_specs=(row_spec,) * 8, check_vma=False)
```

```python
import math
import jax
import jax.numpy as jnp
from jax import lax
from jax.experimental import pallas as pl
from jax.experimental.pallas import tpu as pltpu
from jax.sharding import PartitionSpec as P

NS_STEPS = 5
COEF_A = 3.4445
COEF_B = -4.7750
COEF_C = 2.0315
MOMENTUM = 0.95
LEARN_RATE = 0.04
DECAY = 0.2
NORM_EPS = 1e-7
RMS_MATCH = 0.2

GROUP = 8
MESH = pl.DeviceIdType.MESH
NT = (((1,), (1,)), ((), ()))
F32 = jnp.float32
BF16 = jnp.bfloat16

QKV_OWNER = (0, 1, 7)
OUT_OWNER = (2, 4, 6)
EXPERT_COUNT = (0, 0, 3, 8, 3, 7, 3, 0)
EXPERT_BASE = (0, 0, 0, 3, 11, 14, 21, 24)
EXPERT_OWNER = tuple(d for d in range(GROUP) for _ in range(EXPERT_COUNT[d]))
N_DOWN = 12
MAX_EXPERTS = 8
VMEM_LIMIT = 40 * 1024 * 1024


def send_order():
    halves = ([], [])
    sizes = {"q": 4, "o": 2, "e": 1}
    for kind, owners in (("q", QKV_OWNER), ("o", OUT_OWNER)):
        for index, owner in enumerate(owners):
            halves[owner // 4].append((kind, index))
    for half in range(2):
        devices = [d for d in range(4 * half, 4 * half + 4) if EXPERT_COUNT[d]]
        slots = []
        for d in devices:
            for t in range(EXPERT_COUNT[d]):
                slots.append(((t + 0.5) / EXPERT_COUNT[d], d, t))
        for _, d, t in sorted(slots):
            halves[half].append(("e", EXPERT_BASE[d] + t))
    order, sent, place = [], [0, 0], [0, 0]
    while place[0] < len(halves[0]) or place[1] < len(halves[1]):
        half = 0 if sent[0] <= sent[1] else 1
        if place[half] == len(halves[half]):
            half = 1 - half
        item = halves[half][place[half]]
        place[half] += 1
        sent[half] += sizes[item[0]]
        order.append(item)
    return order


ORDER = send_order()


def pick(table, me):
    total = jnp.int32(0)
    for d, value in enumerate(table):
        if value:
            total = total + jnp.where(me == d, jnp.int32(value), jnp.int32(0))
    return total


def ns_step(src, dst, gram, poly, m, block):
    def rows_of(i):
        return pl.ds(pl.multiple_of(i * block, block), block)

    @pl.loop(0, m // block)
    def _(i):
        rows = rows_of(i)
        gram[rows, :] = lax.dot_general(src[rows, :], src[...], NT, preferred_element_type=F32).astype(BF16)

    @pl.loop(0, m // block)
    def _(i):
        rows = rows_of(i)
        part = gram[rows, :]
        square = jnp.dot(part, gram[...], preferred_element_type=F32)
        poly[rows, :] = (COEF_B * part.astype(F32) + COEF_C * square).astype(BF16)

    @pl.loop(0, m // block)
    def _(i):
        rows = rows_of(i)
        product = jnp.dot(poly[rows, :], src[...], preferred_element_type=F32)
        dst[rows, :] = (COEF_A * src[rows, :].astype(F32) + product).astype(BF16)


STACKS = {"q": (3, 128, 2048, 32, 0), "o": (3, 128, 1024, 64, 0), "d": (12, 64, 1024, 64, 3), "u": (12, 128, 512, 128, 15)}
SCALE = {"q": RMS_MATCH * math.sqrt(2048), "o": RMS_MATCH * math.sqrt(1024),
         "d": RMS_MATCH * math.sqrt(1024), "u": RMS_MATCH * math.sqrt(1024)}
SEM_BASE = {"q": 0, "o": 3, "d": 6, "u": 18}


def place_of(kind, index):
    if kind == "q":
        return "q", index, QKV_OWNER[index], 0
    if kind == "o":
        return "o", index, OUT_OWNER[index], 0
    owner = EXPERT_OWNER[index]
    slot = index - EXPERT_BASE[owner]
    return ("d", index, owner, slot) if index < N_DOWN else ("u", index - N_DOWN, owner, slot)


def return_order():
    keys = []
    for kind, index in ORDER:
        stack, position, owner, slot = place_of(kind, index)
        total = 4 if kind == "q" else EXPERT_COUNT[owner] + (2 if owner in OUT_OWNER else 0)
        if kind == "q":
            done = 0.6 * total
        else:
            done = 2 if kind == "o" else slot + 1 + (2 if owner in OUT_OWNER else 0)
        keys.append((done / total, len(keys), stack, position))
    return [(stack, position) for _, _, stack, position in sorted(keys)]


RETURNS = return_order()


def kernel(w_q, m_q, g_q, w_o, m_o, g_o, w_u, m_u, g_u, w_d, m_d, g_d,
           nw_q, nm_q, nw_o, nm_o, nw_u, nm_u, nw_d, nm_d,
           big, ebuf, gram, poly, xs_q, xs_o, xs_d, xs_u, bk_q, bk_o, bk_d, gs_u, bk_u,
           part_q, part_e, gath_q, gath_e, den_q, den_e,
           m_sem, g_sem, w_sem, norm_send, norm_recv, fwd_send, fwd_recv, ret_send, ret_recv):
    me = lax.axis_index("data")
    weights = {"q": w_q, "o": w_o, "d": w_d, "u": w_u}
    momenta = {"q": m_q, "o": m_o, "d": m_d, "u": m_u}
    gradients = {"q": g_q, "o": g_o, "d": g_d, "u": g_u}
    new_w = {"q": nw_q, "o": nw_o, "d": nw_d, "u": nw_u}
    new_m = {"q": nm_q, "o": nm_o, "d": nm_d, "u": nm_u}
    grad_in = {"q": bk_q, "o": bk_o, "d": bk_d, "u": gs_u}
    scaled = {"q": xs_q, "o": xs_o, "d": xs_d, "u": xs_u}
    back = {"q": bk_q, "o": bk_o, "d": bk_d, "u": bk_u}

    loads = {"q": [("q", i) for i in range(3)], "o": [("o", None)], "d": [("d", None)], "u": [("u", None)]}
    load_sem = {("q", 0): 0, ("q", 1): 1, ("q", 2): 2, ("o", None): 3, ("d", None): 4, ("u", None): 5}

    def part_of(ref, i):
        return ref if i is None else ref.at[i]

    def load_copies(key):
        stack, i = key
        sem = load_sem[key]
        return (pltpu.make_async_copy(part_of(momenta[stack], i), part_of(new_m[stack], i), m_sem.at[sem]),
                pltpu.make_async_copy(part_of(gradients[stack], i), part_of(grad_in[stack], i), g_sem.at[sem]))

    def weight_copy(stack, number):
        return pltpu.make_async_copy(weights[stack], new_w[stack], w_sem.at[number])

    for stack in ("q", "o", "d", "u"):
        for key in loads[stack]:
            for copy in load_copies(key):
                copy.start()

    barrier = pltpu.get_barrier_semaphore()
    for k in range(1, GROUP):
        pl.semaphore_signal(barrier, inc=1, device_id={"data": lax.rem(me + k, GROUP)}, device_id_type=MESH)

    part_q[...] = jnp.zeros_like(part_q)
    part_e[...] = jnp.zeros_like(part_e)

    def momentum_rows(stack, i, table, row):
        _, rows, cols, chunk, _ = STACKS[stack]
        lanes = jnp.zeros((1, 128), F32)
        for r in range(0, rows, chunk):
            at = pl.ds(r, chunk)
            mom = MOMENTUM * new_m[stack][i, at, :] + grad_in[stack][i, at, :].astype(F32)
            new_m[stack][i, at, :] = mom
            square = jnp.sum(mom * mom, axis=0, keepdims=True)
            for c in range(0, cols, 128):
                lanes = lanes + square[:, c:c + 128]
        table[pl.ds(row, 1), :] = lanes

    def push_norms(table, gathered, number):
        gathered[me] = table[...]
        for k in range(1, GROUP):
            pltpu.make_async_remote_copy(
                src_ref=table, dst_ref=gathered.at[me], send_sem=norm_send.at[number], recv_sem=norm_recv.at[number],
                device_id={"data": lax.rem(me + k, GROUP)}, device_id_type=MESH).start()

    def read_norms(gathered, den, number):
        seven = gathered.at[pl.ds(0, GROUP - 1)]
        pltpu.make_async_copy(seven, seven, norm_recv.at[number]).wait()
        total = gathered[0]
        for d in range(1, GROUP):
            total = total + gathered[d]
        total = jnp.sum(total, axis=1, keepdims=True)
        den[...] = jnp.broadcast_to(jnp.sqrt(total) + NORM_EPS, den.shape)

    def scale_rows(stack, i, den, row):
        _, rows, cols, chunk, _ = STACKS[stack]
        divisor = den[pl.ds(row, 1), 0:1]
        for r in range(0, rows, chunk):
            at = pl.ds(r, chunk)
            x = new_m[stack][i, at, :] / jnp.broadcast_to(divisor, (chunk, cols))
            if stack == "u":
                scaled[stack][i] = x.T.astype(BF16)
            else:
                scaled[stack][i, at, :] = x.astype(BF16)

    def block_of(stack, slot_ref, d):
        if stack == "u":
            return slot_ref.at[:, pl.ds(d * 128, 128)]
        rows = STACKS[stack][1]
        return slot_ref.at[pl.ds(d * rows, rows), :]

    def slot_of(stack, slot):
        if stack == "q":
            return big.at[0]
        if stack == "o":
            return big.at[0, :, pl.ds(0, 1024)]
        return ebuf.at[slot]

    def send_rows(stack, i, owner, slot):
        sem = SEM_BASE[stack] + i
        target = block_of(stack, slot_of(stack, slot), me)

        @pl.when(me != owner)
        def _():
            pltpu.make_async_remote_copy(
                src_ref=scaled[stack].at[i], dst_ref=target, send_sem=fwd_send.at[sem], recv_sem=fwd_recv.at[sem],
                device_id={"data": owner}, device_id_type=MESH).start()

        @pl.when(me == owner)
        def _():
            if stack == "u":
                for d in range(GROUP):
                    @pl.when(me == d)
                    def _():
                        ebuf[slot, :, d * 128:(d + 1) * 128] = scaled[stack][i]
            else:
                target[...] = scaled[stack][i]

    for i in range(3):
        for copy in load_copies(("q", i)):
            copy.wait()
        momentum_rows("q", i, part_q, i)
    pl.semaphore_wait(barrier, GROUP - 1)
    push_norms(part_q, gath_q, 0)

    for stack in ("o", "d", "u"):
        for copy in load_copies((stack, None)):
            copy.wait()

        @pl.loop(0, STACKS[stack][0])
        def _(i):
            momentum_rows(stack, i, part_e, STACKS[stack][4] + i)
    push_norms(part_e, gath_e, 1)

    read_norms(gath_q, den_q, 0)
    places = [place_of(kind, index) for kind, index in ORDER]
    for stack, i, owner, slot in [p for p in places if p[0] == "q"]:
        scale_rows(stack, i, den_q, i)
        send_rows(stack, i, owner, slot)
    read_norms(gath_e, den_e, 1)
    for stack in ("o", "d", "u"):
        @pl.loop(0, STACKS[stack][0])
        def _(i):
            scale_rows(stack, i, den_e, STACKS[stack][4] + i)
    for stack, i, owner, slot in [p for p in places if p[0] != "q"]:
        send_rows(stack, i, owner, slot)
    for number, stack in enumerate(("q", "o", "d", "u")):
        weight_copy(stack, number).start()

    def wait_parts(stack, slot_ref, sem):
        rows = 7 * STACKS[stack][1]
        part = slot_ref.at[:, pl.ds(0, rows)] if stack == "u" else slot_ref.at[pl.ds(0, rows), :]
        pltpu.make_async_copy(part, part, sem).wait()

    def give_back(stack, slot_ref, i, send_sem, recv_sem):
        for k in range(1, GROUP):
            dst = lax.rem(me + k, GROUP)
            pltpu.make_async_remote_copy(
                src_ref=block_of(stack, slot_ref, dst), dst_ref=back[stack].at[i], send_sem=send_sem, recv_sem=recv_sem,
                device_id={"data": dst}, device_id_type=MESH).start()

    def new_weight(w, x, stack):
        return w - LEARN_RATE * (SCALE[stack] * x.astype(F32) + DECAY * w)

    def finish(stack, i, source):
        _, rows, cols, chunk, _ = STACKS[stack]
        for r in range(0, rows, chunk):
            at = pl.ds(r, chunk)
            x = source(at)
            if stack == "u":
                x = x.astype(F32).T
            new_w[stack][i, at, :] = new_weight(new_w[stack][i, at, :], x, stack)

    for index, owner in enumerate(QKV_OWNER):
        @pl.when(me == owner)
        def _():
            wait_parts("q", big.at[0], fwd_recv.at[index])

    @pl.when((me == QKV_OWNER[0]) | (me == QKV_OWNER[1]) | (me == QKV_OWNER[2]))
    def _():
        @pl.loop(0, NS_STEPS)
        def _(it):
            now = lax.rem(it, 2)
            ns_step(big.at[now], big.at[1 - now], gram, poly, 1024, 256)

    for index, owner in enumerate(QKV_OWNER):
        @pl.when(me == owner)
        def _():
            give_back("q", big.at[1], index, ret_send.at[0], ret_recv.at[index])
            back["q"][index] = big[1, pl.ds(owner * 128, 128), :]

    for index, owner in enumerate(OUT_OWNER):
        @pl.when(me == owner)
        def _():
            wait_parts("o", big.at[0, :, pl.ds(0, 1024)], fwd_recv.at[3 + index])

    @pl.when((me == OUT_OWNER[0]) | (me == OUT_OWNER[1]) | (me == OUT_OWNER[2]))
    def _():
        @pl.loop(0, NS_STEPS)
        def _(it):
            now = lax.rem(it, 2)
            ns_step(big.at[now, :, pl.ds(0, 1024)], big.at[1 - now, :, pl.ds(0, 1024)], gram, poly, 1024, 256)

    for index, owner in enumerate(OUT_OWNER):
        @pl.when(me == owner)
        def _():
            give_back("o", big.at[1, :, pl.ds(0, 1024)], index, ret_send.at[1], ret_recv.at[3 + index])
            back["o"][index] = big[1, pl.ds(owner * 128, 128), 0:1024]

    base, count = pick(EXPERT_BASE, me), pick(EXPERT_COUNT, me)
    small_gram, small_poly = gram.at[pl.ds(0, 512), pl.ds(0, 512)], poly.at[pl.ds(0, 512), pl.ds(0, 512)]

    @pl.loop(0, count)
    def _(t):
        rank = base + t

        @pl.when(rank < N_DOWN)
        def _():
            wait_parts("d", ebuf.at[t], fwd_recv.at[6 + rank])

        @pl.when(rank >= N_DOWN)
        def _():
            wait_parts("u", ebuf.at[t], fwd_recv.at[6 + rank])

        @pl.loop(0, NS_STEPS)
        def _(it):
            src = jnp.where(it == 0, t, MAX_EXPERTS + lax.rem(it + 1, 2))
            dst = jnp.where(it == NS_STEPS - 1, t, MAX_EXPERTS + lax.rem(it, 2))
            ns_step(ebuf.at[src], ebuf.at[dst], small_gram, small_poly, 512, 256)

        @pl.when(rank < N_DOWN)
        def _():
            give_back("d", ebuf.at[t], rank, ret_send.at[2 + t], ret_recv.at[6 + rank])
            back["d"][rank] = ebuf[t, pl.ds(pl.multiple_of(me * 64, 64), 64), :]

        @pl.when(rank >= N_DOWN)
        def _():
            give_back("u", ebuf.at[t], rank - N_DOWN, ret_send.at[2 + t], ret_recv.at[6 + rank])
            for d in range(GROUP):
                if EXPERT_BASE[d] + EXPERT_COUNT[d] > N_DOWN and EXPERT_COUNT[d]:
                    @pl.when(me == d)
                    def _():
                        back["u"][rank - N_DOWN] = ebuf[t, :, d * 128:(d + 1) * 128]

    for number, stack in enumerate(("q", "o", "d", "u")):
        weight_copy(stack, number).wait()
    owners = {(stack, i): owner for stack, i, owner, _ in places}
    for stack, i in RETURNS:
        owner, sem = owners[stack, i], SEM_BASE[stack] + i

        @pl.when(me != owner)
        def _():
            row = back[stack].at[i]
            pltpu.make_async_copy(row, row, ret_recv.at[sem]).wait()

        if stack == "u":
            finish(stack, i, lambda at: back["u"][i])
        else:
            finish(stack, i, lambda at: back[stack][i, at, :])

    for number, (table, gathered) in enumerate(((part_q, gath_q), (part_e, gath_e))):
        seven = gathered.at[pl.ds(0, GROUP - 1)]
        pltpu.make_async_copy(seven, seven, norm_send.at[number]).wait()
    for stack, i, owner, slot in places:
        @pl.when(me != owner)
        def _():
            block = scaled[stack].at[i]
            pltpu.make_async_copy(block, block, fwd_send.at[SEM_BASE[stack] + i]).wait()
    for owner in QKV_OWNER:
        @pl.when(me == owner)
        def _():
            wait_parts("q", big.at[1], ret_send.at[0])
    for owner in OUT_OWNER:
        @pl.when(me == owner)
        def _():
            wait_parts("o", big.at[1, :, pl.ds(0, 1024)], ret_send.at[1])

    @pl.loop(0, count)
    def _(t):
        @pl.when(base + t < N_DOWN)
        def _():
            wait_parts("d", ebuf.at[t], ret_send.at[2 + t])

        @pl.when(base + t >= N_DOWN)
        def _():
            wait_parts("u", ebuf.at[t], ret_send.at[2 + t])


OUT_SPACE = pltpu.VMEM


def solution(mesh):
    row_spec = P("stage", "data", None)

    def local_step(*args):
        shapes = [args[k].shape for k in (0, 3, 6, 9) for _ in range(2)]
        any_space = pl.BlockSpec(memory_space=pl.ANY)
        return tuple(pl.pallas_call(
            kernel,
            out_shape=[OUT_SPACE(shape, F32) for shape in shapes],
            in_specs=[any_space] * 12,
            out_specs=[pl.BlockSpec(memory_space=OUT_SPACE)] * 8,
            scratch_shapes=[
                pltpu.VMEM((2, 1024, 2048), BF16),
                pltpu.VMEM((MAX_EXPERTS + 2, 512, 1024), BF16),
                pltpu.VMEM((1024, 1024), BF16),
                pltpu.VMEM((1024, 1024), BF16),
                pltpu.VMEM((3, 128, 2048), BF16),
                pltpu.VMEM((3, 128, 1024), BF16),
                pltpu.VMEM((12, 64, 1024), BF16),
                pltpu.VMEM((12, 512, 128), BF16),
                pltpu.VMEM((3, 128, 2048), BF16),
                pltpu.VMEM((3, 128, 1024), BF16),
                pltpu.VMEM((12, 64, 1024), BF16),
                pltpu.VMEM((12, 128, 512), BF16),
                pltpu.VMEM((12, 512, 128), BF16),
                pltpu.VMEM((8, 128), F32),
                pltpu.VMEM((32, 128), F32),
                pltpu.VMEM((GROUP, 8, 128), F32),
                pltpu.VMEM((GROUP, 32, 128), F32),
                pltpu.VMEM((8, 128), F32),
                pltpu.VMEM((32, 128), F32),
                pltpu.SemaphoreType.DMA((6,)),
                pltpu.SemaphoreType.DMA((6,)),
                pltpu.SemaphoreType.DMA((4,)),
                pltpu.SemaphoreType.DMA((2,)),
                pltpu.SemaphoreType.DMA((2,)),
                pltpu.SemaphoreType.DMA((30,)),
                pltpu.SemaphoreType.DMA((30,)),
                pltpu.SemaphoreType.DMA((2 + MAX_EXPERTS,)),
                pltpu.SemaphoreType.DMA((30,)),
            ],
            compiler_params=pltpu.CompilerParams(
                collective_id=0, has_side_effects=True, vmem_limit_bytes=VMEM_LIMIT),
        )(*args))

    return jax.shard_map(local_step, mesh=mesh, in_specs=(row_spec,) * 12, out_specs=(row_spec,) * 8, check_vma=False)
```

```python
import math
import jax
import jax.numpy as jnp
from jax import lax
from jax.experimental import pallas as pl
from jax.experimental.pallas import tpu as pltpu
from jax.sharding import PartitionSpec as P

NS_STEPS = 5
COEF_A = 3.4445
COEF_B = -4.7750
COEF_C = 2.0315
MOMENTUM = 0.95
LEARN_RATE = 0.04
DECAY = 0.2
NORM_EPS = 1e-7
RMS_MATCH = 0.2

GROUP = 8
MESH = pl.DeviceIdType.MESH
NT = (((1,), (1,)), ((), ()))
F32 = jnp.float32
BF16 = jnp.bfloat16

QKV_OWNER = (0, 1, 7)
OUT_OWNER = (2, 4, 6)
EXPERT_COUNT = (0, 0, 3, 8, 3, 7, 3, 0)
EXPERT_BASE = (0, 0, 0, 3, 11, 14, 21, 24)
EXPERT_OWNER = tuple(d for d in range(GROUP) for _ in range(EXPERT_COUNT[d]))
N_DOWN = 12
MAX_EXPERTS = 8
VMEM_LIMIT = 40 * 1024 * 1024


def send_order():
    halves = ([], [])
    sizes = {"q": 4, "o": 2, "e": 1}
    for kind, owners in (("q", QKV_OWNER), ("o", OUT_OWNER)):
        for index, owner in enumerate(owners):
            halves[owner // 4].append((kind, index))
    for half in range(2):
        devices = [d for d in range(4 * half, 4 * half + 4) if EXPERT_COUNT[d]]
        slots = []
        for d in devices:
            for t in range(EXPERT_COUNT[d]):
                slots.append(((t + 0.5) / EXPERT_COUNT[d], d, t))
        for _, d, t in sorted(slots):
            halves[half].append(("e", EXPERT_BASE[d] + t))
    order, sent, place = [], [0, 0], [0, 0]
    while place[0] < len(halves[0]) or place[1] < len(halves[1]):
        half = 0 if sent[0] <= sent[1] else 1
        if place[half] == len(halves[half]):
            half = 1 - half
        item = halves[half][place[half]]
        place[half] += 1
        sent[half] += sizes[item[0]]
        order.append(item)
    return order


ORDER = send_order()


def pick(table, me):
    total = jnp.int32(0)
    for d, value in enumerate(table):
        if value:
            total = total + jnp.where(me == d, jnp.int32(value), jnp.int32(0))
    return total


def ns_step(src, dst, gram, poly, m, block):
    def rows_of(i):
        return pl.ds(pl.multiple_of(i * block, block), block)

    @pl.loop(0, m // block)
    def _(i):
        rows = rows_of(i)
        gram[rows, :] = lax.dot_general(src[rows, :], src[...], NT, preferred_element_type=F32).astype(BF16)

    @pl.loop(0, m // block)
    def _(i):
        rows = rows_of(i)
        part = gram[rows, :]
        square = jnp.dot(part, gram[...], preferred_element_type=F32)
        poly[rows, :] = (COEF_B * part.astype(F32) + COEF_C * square).astype(BF16)

    @pl.loop(0, m // block)
    def _(i):
        rows = rows_of(i)
        product = jnp.dot(poly[rows, :], src[...], preferred_element_type=F32)
        dst[rows, :] = (COEF_A * src[rows, :].astype(F32) + product).astype(BF16)


STACKS = {"q": (3, 128, 2048, 32, 0), "o": (3, 128, 1024, 64, 0), "d": (12, 64, 1024, 64, 3), "u": (12, 128, 512, 128, 15)}
SCALE = {"q": RMS_MATCH * math.sqrt(2048), "o": RMS_MATCH * math.sqrt(1024),
         "d": RMS_MATCH * math.sqrt(1024), "u": RMS_MATCH * math.sqrt(1024)}
SEM_BASE = {"q": 0, "o": 3, "d": 6, "u": 18}


def place_of(kind, index):
    if kind == "q":
        return "q", index, QKV_OWNER[index], 0
    if kind == "o":
        return "o", index, OUT_OWNER[index], 0
    owner = EXPERT_OWNER[index]
    slot = index - EXPERT_BASE[owner]
    return ("d", index, owner, slot) if index < N_DOWN else ("u", index - N_DOWN, owner, slot)


def return_order():
    keys = []
    for kind, index in ORDER:
        stack, position, owner, slot = place_of(kind, index)
        total = 4 if kind == "q" else EXPERT_COUNT[owner] + (2 if owner in OUT_OWNER else 0)
        if kind == "q":
            done = 0.85 * total
        else:
            done = 2 if kind == "o" else slot + 1 + (2 if owner in OUT_OWNER else 0)
        keys.append((done / total, len(keys), stack, position))
    return [(stack, position) for _, _, stack, position in sorted(keys)]


RETURNS = return_order()


def kernel(w_q, m_q, g_q, w_o, m_o, g_o, w_u, m_u, g_u, w_d, m_d, g_d,
           nw_q, nm_q, nw_o, nm_o, nw_u, nm_u, nw_d, nm_d,
           big, ebuf, gram, poly, xs_q, xs_o, xs_d, xs_u, bk_q, bk_o, bk_d, gs_u, bk_u,
           part_q, part_e, gath_q, gath_e, den_q, den_e,
           m_sem, g_sem, w_sem, norm_send, norm_recv, fwd_send, fwd_recv, ret_send, ret_recv):
    me = lax.axis_index("data")
    weights = {"q": w_q, "o": w_o, "d": w_d, "u": w_u}
    momenta = {"q": m_q, "o": m_o, "d": m_d, "u": m_u}
    gradients = {"q": g_q, "o": g_o, "d": g_d, "u": g_u}
    new_w = {"q": nw_q, "o": nw_o, "d": nw_d, "u": nw_u}
    new_m = {"q": nm_q, "o": nm_o, "d": nm_d, "u": nm_u}
    grad_in = {"q": bk_q, "o": bk_o, "d": bk_d, "u": gs_u}
    scaled = {"q": xs_q, "o": xs_o, "d": xs_d, "u": xs_u}
    back = {"q": bk_q, "o": bk_o, "d": bk_d, "u": bk_u}

    loads = {"q": [("q", i) for i in range(3)], "o": [("o", None)], "d": [("d", None)], "u": [("u", None)]}
    load_sem = {("q", 0): 0, ("q", 1): 1, ("q", 2): 2, ("o", None): 3, ("d", None): 4, ("u", None): 5}

    def part_of(ref, i):
        return ref if i is None else ref.at[i]

    def load_copies(key):
        stack, i = key
        sem = load_sem[key]
        return (pltpu.make_async_copy(part_of(momenta[stack], i), part_of(new_m[stack], i), m_sem.at[sem]),
                pltpu.make_async_copy(part_of(gradients[stack], i), part_of(grad_in[stack], i), g_sem.at[sem]))

    def weight_copy(stack, number):
        return pltpu.make_async_copy(weights[stack], new_w[stack], w_sem.at[number])

    for key in loads["q"]:
        for copy in load_copies(key):
            copy.start()

    barrier = pltpu.get_barrier_semaphore()
    for k in range(1, GROUP):
        pl.semaphore_signal(barrier, inc=1, device_id={"data": lax.rem(me + k, GROUP)}, device_id_type=MESH)

    part_q[...] = jnp.zeros_like(part_q)
    part_e[...] = jnp.zeros_like(part_e)

    def momentum_rows(stack, i, table, row):
        _, rows, cols, chunk, _ = STACKS[stack]
        lanes = jnp.zeros((1, 128), F32)
        for r in range(0, rows, chunk):
            at = pl.ds(r, chunk)
            mom = MOMENTUM * new_m[stack][i, at, :] + grad_in[stack][i, at, :].astype(F32)
            new_m[stack][i, at, :] = mom
            square = jnp.sum(mom * mom, axis=0, keepdims=True)
            for c in range(0, cols, 128):
                lanes = lanes + square[:, c:c + 128]
        table[pl.ds(row, 1), :] = lanes

    def push_norms(table, gathered, number):
        gathered[me] = table[...]
        for k in range(1, GROUP):
            pltpu.make_async_remote_copy(
                src_ref=table, dst_ref=gathered.at[me], send_sem=norm_send.at[number], recv_sem=norm_recv.at[number],
                device_id={"data": lax.rem(me + k, GROUP)}, device_id_type=MESH).start()

    def read_norms(gathered, den, number):
        seven = gathered.at[pl.ds(0, GROUP - 1)]
        pltpu.make_async_copy(seven, seven, norm_recv.at[number]).wait()
        total = gathered[0]
        for d in range(1, GROUP):
            total = total + gathered[d]
        total = jnp.sum(total, axis=1, keepdims=True)
        den[...] = jnp.broadcast_to(jnp.sqrt(total) + NORM_EPS, den.shape)

    def scale_rows(stack, i, den, row):
        _, rows, cols, chunk, _ = STACKS[stack]
        divisor = den[pl.ds(row, 1), 0:1]
        for r in range(0, rows, chunk):
            at = pl.ds(r, chunk)
            x = new_m[stack][i, at, :] / jnp.broadcast_to(divisor, (chunk, cols))
            if stack == "u":
                scaled[stack][i] = x.T.astype(BF16)
            else:
                scaled[stack][i, at, :] = x.astype(BF16)

    def block_of(stack, slot_ref, d):
        if stack == "u":
            return slot_ref.at[:, pl.ds(d * 128, 128)]
        rows = STACKS[stack][1]
        return slot_ref.at[pl.ds(d * rows, rows), :]

    def slot_of(stack, slot):
        if stack == "q":
            return big.at[0]
        if stack == "o":
            return big.at[0, :, pl.ds(0, 1024)]
        return ebuf.at[slot]

    def send_rows(stack, i, owner, slot):
        sem = SEM_BASE[stack] + i
        target = block_of(stack, slot_of(stack, slot), me)

        @pl.when(me != owner)
        def _():
            pltpu.make_async_remote_copy(
                src_ref=scaled[stack].at[i], dst_ref=target, send_sem=fwd_send.at[sem], recv_sem=fwd_recv.at[sem],
                device_id={"data": owner}, device_id_type=MESH).start()

        @pl.when(me == owner)
        def _():
            if stack == "u":
                for d in range(GROUP):
                    @pl.when(me == d)
                    def _():
                        ebuf[slot, :, d * 128:(d + 1) * 128] = scaled[stack][i]
            else:
                target[...] = scaled[stack][i]

    def momentum_stack(stack):
        for copy in load_copies((stack, None)):
            copy.wait()

        @pl.loop(0, STACKS[stack][0])
        def _(i):
            momentum_rows(stack, i, part_e, STACKS[stack][4] + i)

    def scale_stack(stack):
        @pl.loop(0, STACKS[stack][0])
        def _(i):
            scale_rows(stack, i, den_e, STACKS[stack][4] + i)

    for i in range(3):
        for copy in load_copies(("q", i)):
            copy.wait()
        momentum_rows("q", i, part_q, i)
    for stack in ("o", "d", "u"):
        for copy in load_copies((stack, None)):
            copy.start()
    pl.semaphore_wait(barrier, GROUP - 1)
    push_norms(part_q, gath_q, 0)
    momentum_stack("o")
    momentum_stack("d")
    read_norms(gath_q, den_q, 0)
    places = [place_of(kind, index) for kind, index in ORDER]
    for stack, i, owner, slot in [p for p in places if p[0] == "q"]:
        scale_rows(stack, i, den_q, i)
        send_rows(stack, i, owner, slot)
    momentum_stack("u")
    push_norms(part_e, gath_e, 1)
    for number, stack in enumerate(("q", "o", "d", "u")):
        weight_copy(stack, number).start()
    read_norms(gath_e, den_e, 1)
    for stack in ("o", "d", "u"):
        scale_stack(stack)
    for stack, i, owner, slot in [p for p in places if p[0] != "q"]:
        send_rows(stack, i, owner, slot)

    def wait_parts(stack, slot_ref, sem):
        rows = 7 * STACKS[stack][1]
        part = slot_ref.at[:, pl.ds(0, rows)] if stack == "u" else slot_ref.at[pl.ds(0, rows), :]
        pltpu.make_async_copy(part, part, sem).wait()

    def give_back(stack, slot_ref, i, send_sem, recv_sem):
        for k in range(1, GROUP):
            dst = lax.rem(me + k, GROUP)
            pltpu.make_async_remote_copy(
                src_ref=block_of(stack, slot_ref, dst), dst_ref=back[stack].at[i], send_sem=send_sem, recv_sem=recv_sem,
                device_id={"data": dst}, device_id_type=MESH).start()

    def new_weight(w, x, stack):
        return w - LEARN_RATE * (SCALE[stack] * x.astype(F32) + DECAY * w)

    def finish(stack, i, source):
        _, rows, cols, chunk, _ = STACKS[stack]
        for r in range(0, rows, chunk):
            at = pl.ds(r, chunk)
            x = source(at)
            if stack == "u":
                x = x.astype(F32).T
            new_w[stack][i, at, :] = new_weight(new_w[stack][i, at, :], x, stack)

    for index, owner in enumerate(QKV_OWNER):
        @pl.when(me == owner)
        def _():
            wait_parts("q", big.at[0], fwd_recv.at[index])

    @pl.when((me == QKV_OWNER[0]) | (me == QKV_OWNER[1]) | (me == QKV_OWNER[2]))
    def _():
        @pl.loop(0, NS_STEPS)
        def _(it):
            now = lax.rem(it, 2)
            ns_step(big.at[now], big.at[1 - now], gram, poly, 1024, 256)

    for index, owner in enumerate(QKV_OWNER):
        @pl.when(me == owner)
        def _():
            give_back("q", big.at[1], index, ret_send.at[0], ret_recv.at[index])
            back["q"][index] = big[1, pl.ds(owner * 128, 128), :]

    for index, owner in enumerate(OUT_OWNER):
        @pl.when(me == owner)
        def _():
            wait_parts("o", big.at[0, :, pl.ds(0, 1024)], fwd_recv.at[3 + index])

    @pl.when((me == OUT_OWNER[0]) | (me == OUT_OWNER[1]) | (me == OUT_OWNER[2]))
    def _():
        @pl.loop(0, NS_STEPS)
        def _(it):
            now = lax.rem(it, 2)
            ns_step(big.at[now, :, pl.ds(0, 1024)], big.at[1 - now, :, pl.ds(0, 1024)], gram, poly, 1024, 256)

    for index, owner in enumerate(OUT_OWNER):
        @pl.when(me == owner)
        def _():
            give_back("o", big.at[1, :, pl.ds(0, 1024)], index, ret_send.at[1], ret_recv.at[3 + index])
            back["o"][index] = big[1, pl.ds(owner * 128, 128), 0:1024]

    base, count = pick(EXPERT_BASE, me), pick(EXPERT_COUNT, me)
    small_gram, small_poly = gram.at[pl.ds(0, 512), pl.ds(0, 512)], poly.at[pl.ds(0, 512), pl.ds(0, 512)]

    @pl.loop(0, count)
    def _(t):
        rank = base + t

        @pl.when(rank < N_DOWN)
        def _():
            wait_parts("d", ebuf.at[t], fwd_recv.at[6 + rank])

        @pl.when(rank >= N_DOWN)
        def _():
            wait_parts("u", ebuf.at[t], fwd_recv.at[6 + rank])

        @pl.loop(0, NS_STEPS)
        def _(it):
            src = jnp.where(it == 0, t, MAX_EXPERTS + lax.rem(it + 1, 2))
            dst = jnp.where(it == NS_STEPS - 1, t, MAX_EXPERTS + lax.rem(it, 2))
            ns_step(ebuf.at[src], ebuf.at[dst], small_gram, small_poly, 512, 256)

        @pl.when(rank < N_DOWN)
        def _():
            give_back("d", ebuf.at[t], rank, ret_send.at[2 + t], ret_recv.at[6 + rank])
            back["d"][rank] = ebuf[t, pl.ds(pl.multiple_of(me * 64, 64), 64), :]

        @pl.when(rank >= N_DOWN)
        def _():
            give_back("u", ebuf.at[t], rank - N_DOWN, ret_send.at[2 + t], ret_recv.at[6 + rank])
            for d in range(GROUP):
                if EXPERT_BASE[d] + EXPERT_COUNT[d] > N_DOWN and EXPERT_COUNT[d]:
                    @pl.when(me == d)
                    def _():
                        back["u"][rank - N_DOWN] = ebuf[t, :, d * 128:(d + 1) * 128]

    for number, stack in enumerate(("q", "o", "d", "u")):
        weight_copy(stack, number).wait()
    owners = {(stack, i): owner for stack, i, owner, _ in places}
    for stack, i in RETURNS:
        owner, sem = owners[stack, i], SEM_BASE[stack] + i

        @pl.when(me != owner)
        def _():
            row = back[stack].at[i]
            pltpu.make_async_copy(row, row, ret_recv.at[sem]).wait()

        if stack == "u":
            finish(stack, i, lambda at: back["u"][i])
        else:
            finish(stack, i, lambda at: back[stack][i, at, :])

    for number, (table, gathered) in enumerate(((part_q, gath_q), (part_e, gath_e))):
        seven = gathered.at[pl.ds(0, GROUP - 1)]
        pltpu.make_async_copy(seven, seven, norm_send.at[number]).wait()
    for stack, i, owner, slot in places:
        @pl.when(me != owner)
        def _():
            block = scaled[stack].at[i]
            pltpu.make_async_copy(block, block, fwd_send.at[SEM_BASE[stack] + i]).wait()
    for owner in QKV_OWNER:
        @pl.when(me == owner)
        def _():
            wait_parts("q", big.at[1], ret_send.at[0])
    for owner in OUT_OWNER:
        @pl.when(me == owner)
        def _():
            wait_parts("o", big.at[1, :, pl.ds(0, 1024)], ret_send.at[1])

    @pl.loop(0, count)
    def _(t):
        @pl.when(base + t < N_DOWN)
        def _():
            wait_parts("d", ebuf.at[t], ret_send.at[2 + t])

        @pl.when(base + t >= N_DOWN)
        def _():
            wait_parts("u", ebuf.at[t], ret_send.at[2 + t])


OUT_SPACE = pltpu.VMEM


def store_kernel(*refs):
    copies = [pltpu.make_async_copy(refs[k], refs[8 + k], refs[16].at[k]) for k in range(8)]
    for copy in copies:
        copy.start()
    for copy in copies:
        copy.wait()


def solution(mesh):
    row_spec = P("stage", "data", None)

    def local_step(*args):
        shapes = [args[k].shape for k in (0, 3, 6, 9) for _ in range(2)]
        any_space = pl.BlockSpec(memory_space=pl.ANY)
        kept = pl.pallas_call(
            kernel,
            out_shape=[OUT_SPACE(shape, F32) for shape in shapes],
            in_specs=[any_space] * 12,
            out_specs=[pl.BlockSpec(memory_space=OUT_SPACE)] * 8,
            scratch_shapes=[
                pltpu.VMEM((2, 1024, 2048), BF16),
                pltpu.VMEM((MAX_EXPERTS + 2, 512, 1024), BF16),
                pltpu.VMEM((1024, 1024), BF16),
                pltpu.VMEM((1024, 1024), BF16),
                pltpu.VMEM((3, 128, 2048), BF16),
                pltpu.VMEM((3, 128, 1024), BF16),
                pltpu.VMEM((12, 64, 1024), BF16),
                pltpu.VMEM((12, 512, 128), BF16),
                pltpu.VMEM((3, 128, 2048), BF16),
                pltpu.VMEM((3, 128, 1024), BF16),
                pltpu.VMEM((12, 64, 1024), BF16),
                pltpu.VMEM((12, 128, 512), BF16),
                pltpu.VMEM((12, 512, 128), BF16),
                pltpu.VMEM((8, 128), F32),
                pltpu.VMEM((32, 128), F32),
                pltpu.VMEM((GROUP, 8, 128), F32),
                pltpu.VMEM((GROUP, 32, 128), F32),
                pltpu.VMEM((8, 128), F32),
                pltpu.VMEM((32, 128), F32),
                pltpu.SemaphoreType.DMA((6,)),
                pltpu.SemaphoreType.DMA((6,)),
                pltpu.SemaphoreType.DMA((4,)),
                pltpu.SemaphoreType.DMA((2,)),
                pltpu.SemaphoreType.DMA((2,)),
                pltpu.SemaphoreType.DMA((30,)),
                pltpu.SemaphoreType.DMA((30,)),
                pltpu.SemaphoreType.DMA((2 + MAX_EXPERTS,)),
                pltpu.SemaphoreType.DMA((30,)),
            ],
            compiler_params=pltpu.CompilerParams(
                collective_id=0, has_side_effects=True, vmem_limit_bytes=VMEM_LIMIT),
        )(*args)
        return tuple(pl.pallas_call(
            store_kernel,
            out_shape=[jax.ShapeDtypeStruct(shape, F32) for shape in shapes],
            in_specs=[any_space] * 8,
            out_specs=[any_space] * 8,
            scratch_shapes=[pltpu.SemaphoreType.DMA((8,))],
            compiler_params=pltpu.CompilerParams(vmem_limit_bytes=1024 * 1024),
        )(*kept))

    return jax.shard_map(local_step, mesh=mesh, in_specs=(row_spec,) * 12, out_specs=(row_spec,) * 8, check_vma=False)
```

```python
import math
import jax
import jax.numpy as jnp
from jax import lax
from jax.experimental import pallas as pl
from jax.experimental.pallas import tpu as pltpu
from jax.sharding import PartitionSpec as P

NS_STEPS = 5
COEF_A = 3.4445
COEF_B = -4.7750
COEF_C = 2.0315
MOMENTUM = 0.95
LEARN_RATE = 0.04
DECAY = 0.2
NORM_EPS = 1e-7
RMS_MATCH = 0.2

GROUP = 8
MESH = pl.DeviceIdType.MESH
NT = (((1,), (1,)), ((), ()))
F32 = jnp.float32
BF16 = jnp.bfloat16

QKV_OWNER = (0, 1, 7)
OUT_OWNER = (2, 4, 6)
EXPERT_COUNT = (0, 0, 3, 8, 3, 7, 3, 0)
EXPERT_BASE = (0, 0, 0, 3, 11, 14, 21, 24)
EXPERT_OWNER = tuple(d for d in range(GROUP) for _ in range(EXPERT_COUNT[d]))
N_DOWN = 12
MAX_EXPERTS = 8
VMEM_LIMIT = 40 * 1024 * 1024


def send_order():
    halves = ([], [])
    sizes = {"q": 4, "o": 2, "e": 1}
    for kind, owners in (("q", QKV_OWNER), ("o", OUT_OWNER)):
        for index, owner in enumerate(owners):
            halves[owner // 4].append((kind, index))
    for half in range(2):
        devices = [d for d in range(4 * half, 4 * half + 4) if EXPERT_COUNT[d]]
        slots = []
        for d in devices:
            for t in range(EXPERT_COUNT[d]):
                slots.append(((t + 0.5) / EXPERT_COUNT[d], d, t))
        for _, d, t in sorted(slots):
            halves[half].append(("e", EXPERT_BASE[d] + t))
    order, sent, place = [], [0, 0], [0, 0]
    while place[0] < len(halves[0]) or place[1] < len(halves[1]):
        half = 0 if sent[0] <= sent[1] else 1
        if place[half] == len(halves[half]):
            half = 1 - half
        item = halves[half][place[half]]
        place[half] += 1
        sent[half] += sizes[item[0]]
        order.append(item)
    return order


ORDER = send_order()


def pick(table, me):
    total = jnp.int32(0)
    for d, value in enumerate(table):
        if value:
            total = total + jnp.where(me == d, jnp.int32(value), jnp.int32(0))
    return total


def ns_step(src, dst, gram, poly, m, block):
    def rows_of(i):
        return pl.ds(pl.multiple_of(i * block, block), block)

    @pl.loop(0, m // block)
    def _(i):
        rows = rows_of(i)
        gram[rows, :] = lax.dot_general(src[rows, :], src[...], NT, preferred_element_type=F32).astype(BF16)

    @pl.loop(0, m // block)
    def _(i):
        rows = rows_of(i)
        part = gram[rows, :]
        square = jnp.dot(part, gram[...], preferred_element_type=F32)
        poly[rows, :] = (COEF_B * part.astype(F32) + COEF_C * square).astype(BF16)

    @pl.loop(0, m // block)
    def _(i):
        rows = rows_of(i)
        product = jnp.dot(poly[rows, :], src[...], preferred_element_type=F32)
        dst[rows, :] = (COEF_A * src[rows, :].astype(F32) + product).astype(BF16)


STACKS = {"q": (3, 128, 2048, 32, 0), "o": (3, 128, 1024, 64, 0), "d": (12, 64, 1024, 64, 3), "u": (12, 128, 512, 128, 15)}
SCALE = {"q": RMS_MATCH * math.sqrt(2048), "o": RMS_MATCH * math.sqrt(1024),
         "d": RMS_MATCH * math.sqrt(1024), "u": RMS_MATCH * math.sqrt(1024)}
SEM_BASE = {"q": 0, "o": 3, "d": 6, "u": 18}


def place_of(kind, index):
    if kind == "q":
        return "q", index, QKV_OWNER[index], 0
    if kind == "o":
        return "o", index, OUT_OWNER[index], 0
    owner = EXPERT_OWNER[index]
    slot = index - EXPERT_BASE[owner]
    return ("d", index, owner, slot) if index < N_DOWN else ("u", index - N_DOWN, owner, slot)


def return_order():
    keys = []
    for kind, index in ORDER:
        stack, position, owner, slot = place_of(kind, index)
        total = 4 if kind == "q" else EXPERT_COUNT[owner] + (2 if owner in OUT_OWNER else 0)
        if kind == "q":
            done = 0.85 * total
        else:
            done = 2 if kind == "o" else slot + 1 + (2 if owner in OUT_OWNER else 0)
        keys.append((done / total, len(keys), stack, position))
    return [(stack, position) for _, _, stack, position in sorted(keys)]


RETURNS = return_order()


def kernel(w_q, m_q, g_q, w_o, m_o, g_o, w_u, m_u, g_u, w_d, m_d, g_d,
           nw_q, nm_q, nw_o, nm_o, nw_u, nm_u, nw_d, nm_d,
           big, ebuf, gram, poly, xs_q, xs_o, xs_d, xs_u, bk_q, bk_o, bk_d, gs_u, bk_u,
           part_q, part_e, gath_q, gath_e, den_q, den_e,
           m_sem, g_sem, w_sem, norm_send, norm_recv, fwd_send, fwd_recv, ret_send, ret_recv):
    me = lax.axis_index("data")
    weights = {"q": w_q, "o": w_o, "d": w_d, "u": w_u}
    momenta = {"q": m_q, "o": m_o, "d": m_d, "u": m_u}
    gradients = {"q": g_q, "o": g_o, "d": g_d, "u": g_u}
    new_w = {"q": nw_q, "o": nw_o, "d": nw_d, "u": nw_u}
    new_m = {"q": nm_q, "o": nm_o, "d": nm_d, "u": nm_u}
    grad_in = {"q": bk_q, "o": bk_o, "d": bk_d, "u": gs_u}
    scaled = {"q": xs_q, "o": xs_o, "d": xs_d, "u": xs_u}
    back = {"q": bk_q, "o": bk_o, "d": bk_d, "u": bk_u}

    loads = {"q": [("q", i) for i in range(3)], "o": [("o", None)], "d": [("d", None)], "u": [("u", None)]}
    load_sem = {("q", 0): 0, ("q", 1): 1, ("q", 2): 2, ("o", None): 3, ("d", None): 4, ("u", None): 5}

    def part_of(ref, i):
        return ref if i is None else ref.at[i]

    def load_copies(key):
        stack, i = key
        sem = load_sem[key]
        return (pltpu.make_async_copy(part_of(momenta[stack], i), part_of(new_m[stack], i), m_sem.at[sem]),
                pltpu.make_async_copy(part_of(gradients[stack], i), part_of(grad_in[stack], i), g_sem.at[sem]))

    def weight_copy(stack, number):
        return pltpu.make_async_copy(weights[stack], new_w[stack], w_sem.at[number])

    for key in loads["q"]:
        for copy in load_copies(key):
            copy.start()

    barrier = pltpu.get_barrier_semaphore()
    for k in range(1, GROUP):
        pl.semaphore_signal(barrier, inc=1, device_id={"data": lax.rem(me + k, GROUP)}, device_id_type=MESH)

    part_q[...] = jnp.zeros_like(part_q)
    part_e[...] = jnp.zeros_like(part_e)

    def momentum_rows(stack, i, table, row):
        _, rows, cols, chunk, _ = STACKS[stack]
        lanes = jnp.zeros((1, 128), F32)
        for r in range(0, rows, chunk):
            at = pl.ds(r, chunk)
            mom = MOMENTUM * new_m[stack][i, at, :] + grad_in[stack][i, at, :].astype(F32)
            new_m[stack][i, at, :] = mom
            square = jnp.sum(mom * mom, axis=0, keepdims=True)
            for c in range(0, cols, 128):
                lanes = lanes + square[:, c:c + 128]
        table[pl.ds(row, 1), :] = lanes

    def push_norms(table, gathered, number):
        gathered[me] = table[...]
        for k in range(1, GROUP):
            pltpu.make_async_remote_copy(
                src_ref=table, dst_ref=gathered.at[me], send_sem=norm_send.at[number], recv_sem=norm_recv.at[number],
                device_id={"data": lax.rem(me + k, GROUP)}, device_id_type=MESH).start()

    def read_norms(gathered, den, number):
        seven = gathered.at[pl.ds(0, GROUP - 1)]
        pltpu.make_async_copy(seven, seven, norm_recv.at[number]).wait()
        total = gathered[0]
        for d in range(1, GROUP):
            total = total + gathered[d]
        total = jnp.sum(total, axis=1, keepdims=True)
        den[...] = jnp.broadcast_to(jnp.sqrt(total) + NORM_EPS, den.shape)

    def scale_rows(stack, i, den, row):
        _, rows, cols, chunk, _ = STACKS[stack]
        divisor = den[pl.ds(row, 1), 0:1]
        for r in range(0, rows, chunk):
            at = pl.ds(r, chunk)
            x = new_m[stack][i, at, :] / jnp.broadcast_to(divisor, (chunk, cols))
            if stack == "u":
                scaled[stack][i] = x.T.astype(BF16)
            else:
                scaled[stack][i, at, :] = x.astype(BF16)

    def block_of(stack, slot_ref, d):
        if stack == "u":
            return slot_ref.at[:, pl.ds(d * 128, 128)]
        rows = STACKS[stack][1]
        return slot_ref.at[pl.ds(d * rows, rows), :]

    def slot_of(stack, slot):
        if stack == "q":
            return big.at[0]
        if stack == "o":
            return big.at[0, :, pl.ds(0, 1024)]
        return ebuf.at[slot]

    def send_rows(stack, i, owner, slot):
        sem = SEM_BASE[stack] + i
        target = block_of(stack, slot_of(stack, slot), me)

        @pl.when(me != owner)
        def _():
            pltpu.make_async_remote_copy(
                src_ref=scaled[stack].at[i], dst_ref=target, send_sem=fwd_send.at[sem], recv_sem=fwd_recv.at[sem],
                device_id={"data": owner}, device_id_type=MESH).start()

        @pl.when(me == owner)
        def _():
            if stack == "u":
                for d in range(GROUP):
                    @pl.when(me == d)
                    def _():
                        ebuf[slot, :, d * 128:(d + 1) * 128] = scaled[stack][i]
            else:
                target[...] = scaled[stack][i]

    def momentum_stack(stack):
        for copy in load_copies((stack, None)):
            copy.wait()

        @pl.loop(0, STACKS[stack][0])
        def _(i):
            momentum_rows(stack, i, part_e, STACKS[stack][4] + i)

    def scale_stack(stack):
        @pl.loop(0, STACKS[stack][0])
        def _(i):
            scale_rows(stack, i, den_e, STACKS[stack][4] + i)

    for i in range(3):
        for copy in load_copies(("q", i)):
            copy.wait()
        if i == 0:
            for stack in ("o", "d", "u"):
                for copy in load_copies((stack, None)):
                    copy.start()
        momentum_rows("q", i, part_q, i)
    pl.semaphore_wait(barrier, GROUP - 1)
    push_norms(part_q, gath_q, 0)
    momentum_stack("o")
    momentum_stack("d")
    momentum_stack("u")
    push_norms(part_e, gath_e, 1)
    read_norms(gath_q, den_q, 0)
    places = [place_of(kind, index) for kind, index in ORDER]
    for stack, i, owner, slot in [p for p in places if p[0] == "q"]:
        scale_rows(stack, i, den_q, i)
        send_rows(stack, i, owner, slot)
    for number, stack in enumerate(("q", "o", "d", "u")):
        weight_copy(stack, number).start()
    read_norms(gath_e, den_e, 1)
    for stack in ("o", "d", "u"):
        scale_stack(stack)
    for stack, i, owner, slot in [p for p in places if p[0] != "q"]:
        send_rows(stack, i, owner, slot)

    def wait_parts(stack, slot_ref, sem):
        rows = 7 * STACKS[stack][1]
        part = slot_ref.at[:, pl.ds(0, rows)] if stack == "u" else slot_ref.at[pl.ds(0, rows), :]
        pltpu.make_async_copy(part, part, sem).wait()

    def give_back(stack, slot_ref, i, send_sem, recv_sem):
        for k in range(1, GROUP):
            dst = lax.rem(me + k, GROUP)
            pltpu.make_async_remote_copy(
                src_ref=block_of(stack, slot_ref, dst), dst_ref=back[stack].at[i], send_sem=send_sem, recv_sem=recv_sem,
                device_id={"data": dst}, device_id_type=MESH).start()

    def new_weight(w, x, stack):
        return w - LEARN_RATE * (SCALE[stack] * x.astype(F32) + DECAY * w)

    def finish(stack, i, source):
        _, rows, cols, chunk, _ = STACKS[stack]
        for r in range(0, rows, chunk):
            at = pl.ds(r, chunk)
            x = source(at)
            if stack == "u":
                x = x.astype(F32).T
            new_w[stack][i, at, :] = new_weight(new_w[stack][i, at, :], x, stack)

    for index, owner in enumerate(QKV_OWNER):
        @pl.when(me == owner)
        def _():
            wait_parts("q", big.at[0], fwd_recv.at[index])

    @pl.when((me == QKV_OWNER[0]) | (me == QKV_OWNER[1]) | (me == QKV_OWNER[2]))
    def _():
        @pl.loop(0, NS_STEPS)
        def _(it):
            now = lax.rem(it, 2)
            ns_step(big.at[now], big.at[1 - now], gram, poly, 1024, 256)

    for index, owner in enumerate(QKV_OWNER):
        @pl.when(me == owner)
        def _():
            give_back("q", big.at[1], index, ret_send.at[0], ret_recv.at[index])
            back["q"][index] = big[1, pl.ds(owner * 128, 128), :]

    for index, owner in enumerate(OUT_OWNER):
        @pl.when(me == owner)
        def _():
            wait_parts("o", big.at[0, :, pl.ds(0, 1024)], fwd_recv.at[3 + index])

    @pl.when((me == OUT_OWNER[0]) | (me == OUT_OWNER[1]) | (me == OUT_OWNER[2]))
    def _():
        @pl.loop(0, NS_STEPS)
        def _(it):
            now = lax.rem(it, 2)
            ns_step(big.at[now, :, pl.ds(0, 1024)], big.at[1 - now, :, pl.ds(0, 1024)], gram, poly, 1024, 256)

    for index, owner in enumerate(OUT_OWNER):
        @pl.when(me == owner)
        def _():
            give_back("o", big.at[1, :, pl.ds(0, 1024)], index, ret_send.at[1], ret_recv.at[3 + index])
            back["o"][index] = big[1, pl.ds(owner * 128, 128), 0:1024]

    base, count = pick(EXPERT_BASE, me), pick(EXPERT_COUNT, me)
    small_gram, small_poly = gram.at[pl.ds(0, 512), pl.ds(0, 512)], poly.at[pl.ds(0, 512), pl.ds(0, 512)]

    @pl.loop(0, count)
    def _(t):
        rank = base + t

        @pl.when(rank < N_DOWN)
        def _():
            wait_parts("d", ebuf.at[t], fwd_recv.at[6 + rank])

        @pl.when(rank >= N_DOWN)
        def _():
            wait_parts("u", ebuf.at[t], fwd_recv.at[6 + rank])

        @pl.loop(0, NS_STEPS)
        def _(it):
            src = jnp.where(it == 0, t, MAX_EXPERTS + lax.rem(it + 1, 2))
            dst = jnp.where(it == NS_STEPS - 1, t, MAX_EXPERTS + lax.rem(it, 2))
            ns_step(ebuf.at[src], ebuf.at[dst], small_gram, small_poly, 512, 256)

        @pl.when(rank < N_DOWN)
        def _():
            give_back("d", ebuf.at[t], rank, ret_send.at[2 + t], ret_recv.at[6 + rank])
            back["d"][rank] = ebuf[t, pl.ds(pl.multiple_of(me * 64, 64), 64), :]

        @pl.when(rank >= N_DOWN)
        def _():
            give_back("u", ebuf.at[t], rank - N_DOWN, ret_send.at[2 + t], ret_recv.at[6 + rank])
            for d in range(GROUP):
                if EXPERT_BASE[d] + EXPERT_COUNT[d] > N_DOWN and EXPERT_COUNT[d]:
                    @pl.when(me == d)
                    def _():
                        back["u"][rank - N_DOWN] = ebuf[t, :, d * 128:(d + 1) * 128]

    for number, stack in enumerate(("q", "o", "d", "u")):
        weight_copy(stack, number).wait()
    owners = {(stack, i): owner for stack, i, owner, _ in places}
    for stack, i in RETURNS:
        owner, sem = owners[stack, i], SEM_BASE[stack] + i

        @pl.when(me != owner)
        def _():
            row = back[stack].at[i]
            pltpu.make_async_copy(row, row, ret_recv.at[sem]).wait()

        if stack == "u":
            finish(stack, i, lambda at: back["u"][i])
        else:
            finish(stack, i, lambda at: back[stack][i, at, :])

    for number, (table, gathered) in enumerate(((part_q, gath_q), (part_e, gath_e))):
        seven = gathered.at[pl.ds(0, GROUP - 1)]
        pltpu.make_async_copy(seven, seven, norm_send.at[number]).wait()
    for stack, i, owner, slot in places:
        @pl.when(me != owner)
        def _():
            block = scaled[stack].at[i]
            pltpu.make_async_copy(block, block, fwd_send.at[SEM_BASE[stack] + i]).wait()
    for owner in QKV_OWNER:
        @pl.when(me == owner)
        def _():
            wait_parts("q", big.at[1], ret_send.at[0])
    for owner in OUT_OWNER:
        @pl.when(me == owner)
        def _():
            wait_parts("o", big.at[1, :, pl.ds(0, 1024)], ret_send.at[1])

    @pl.loop(0, count)
    def _(t):
        @pl.when(base + t < N_DOWN)
        def _():
            wait_parts("d", ebuf.at[t], ret_send.at[2 + t])

        @pl.when(base + t >= N_DOWN)
        def _():
            wait_parts("u", ebuf.at[t], ret_send.at[2 + t])


OUT_SPACE = pltpu.VMEM


def store_kernel(*refs):
    copies = [pltpu.make_async_copy(refs[k], refs[8 + k], refs[16].at[k]) for k in range(8)]
    for copy in copies:
        copy.start()
    for copy in copies:
        copy.wait()


def solution(mesh):
    row_spec = P("stage", "data", None)

    def local_step(*args):
        shapes = [args[k].shape for k in (0, 3, 6, 9) for _ in range(2)]
        any_space = pl.BlockSpec(memory_space=pl.ANY)
        kept = pl.pallas_call(
            kernel,
            out_shape=[OUT_SPACE(shape, F32) for shape in shapes],
            in_specs=[any_space] * 12,
            out_specs=[pl.BlockSpec(memory_space=OUT_SPACE)] * 8,
            scratch_shapes=[
                pltpu.VMEM((2, 1024, 2048), BF16),
                pltpu.VMEM((MAX_EXPERTS + 2, 512, 1024), BF16),
                pltpu.VMEM((1024, 1024), BF16),
                pltpu.VMEM((1024, 1024), BF16),
                pltpu.VMEM((3, 128, 2048), BF16),
                pltpu.VMEM((3, 128, 1024), BF16),
                pltpu.VMEM((12, 64, 1024), BF16),
                pltpu.VMEM((12, 512, 128), BF16),
                pltpu.VMEM((3, 128, 2048), BF16),
                pltpu.VMEM((3, 128, 1024), BF16),
                pltpu.VMEM((12, 64, 1024), BF16),
                pltpu.VMEM((12, 128, 512), BF16),
                pltpu.VMEM((12, 512, 128), BF16),
                pltpu.VMEM((8, 128), F32),
                pltpu.VMEM((32, 128), F32),
                pltpu.VMEM((GROUP, 8, 128), F32),
                pltpu.VMEM((GROUP, 32, 128), F32),
                pltpu.VMEM((8, 128), F32),
                pltpu.VMEM((32, 128), F32),
                pltpu.SemaphoreType.DMA((6,)),
                pltpu.SemaphoreType.DMA((6,)),
                pltpu.SemaphoreType.DMA((4,)),
                pltpu.SemaphoreType.DMA((2,)),
                pltpu.SemaphoreType.DMA((2,)),
                pltpu.SemaphoreType.DMA((30,)),
                pltpu.SemaphoreType.DMA((30,)),
                pltpu.SemaphoreType.DMA((2 + MAX_EXPERTS,)),
                pltpu.SemaphoreType.DMA((30,)),
            ],
            compiler_params=pltpu.CompilerParams(
                collective_id=0, has_side_effects=True, vmem_limit_bytes=VMEM_LIMIT),
        )(*args)
        return tuple(pl.pallas_call(
            store_kernel,
            out_shape=[jax.ShapeDtypeStruct(shape, F32) for shape in shapes],
            in_specs=[any_space] * 8,
            out_specs=[any_space] * 8,
            scratch_shapes=[pltpu.SemaphoreType.DMA((8,))],
            compiler_params=pltpu.CompilerParams(vmem_limit_bytes=1024 * 1024),
        )(*kept))

    return jax.shard_map(local_step, mesh=mesh, in_specs=(row_spec,) * 12, out_specs=(row_spec,) * 8, check_vma=False)
```

```python
import math
import jax
import jax.numpy as jnp
from jax import lax
from jax.experimental import pallas as pl
from jax.experimental.pallas import tpu as pltpu
from jax.sharding import PartitionSpec as P

NS_STEPS = 5
COEF_A = 3.4445
COEF_B = -4.7750
COEF_C = 2.0315
MOMENTUM = 0.95
LEARN_RATE = 0.04
DECAY = 0.2
NORM_EPS = 1e-7
RMS_MATCH = 0.2

GROUP = 8
MESH = pl.DeviceIdType.MESH
NT = (((1,), (1,)), ((), ()))
F32 = jnp.float32
BF16 = jnp.bfloat16

QKV_OWNER = (2, 0, 5)
OUT_OWNER = (1, 6, 7)
EXPERT_COUNT = (0, 0, 7, 4, 7, 3, 1, 2)
EXPERT_BASE = tuple(sum(EXPERT_COUNT[:d]) for d in range(GROUP))
EXPERT_OWNER = tuple(d for d in range(GROUP) for _ in range(EXPERT_COUNT[d]))
N_DOWN = 12
MAX_EXPERTS = 8
VMEM_LIMIT = 40 * 1024 * 1024


def send_order():
    halves = ([], [])
    sizes = {"q": 4, "o": 2, "e": 1}
    for kind, owners in (("q", QKV_OWNER), ("o", OUT_OWNER)):
        for index, owner in enumerate(owners):
            halves[owner // 4].append((kind, index))
    for half in range(2):
        devices = [d for d in range(4 * half, 4 * half + 4) if EXPERT_COUNT[d]]
        slots = []
        for d in devices:
            for t in range(EXPERT_COUNT[d]):
                slots.append(((t + 0.5) / EXPERT_COUNT[d] + (d in QKV_OWNER), d, t))
        for _, d, t in sorted(slots):
            halves[half].append(("e", EXPERT_BASE[d] + t))
    order, sent, place = [], [0, 0], [0, 0]
    while place[0] < len(halves[0]) or place[1] < len(halves[1]):
        half = 0 if sent[0] <= sent[1] else 1
        if place[half] == len(halves[half]):
            half = 1 - half
        item = halves[half][place[half]]
        place[half] += 1
        sent[half] += sizes[item[0]]
        order.append(item)
    return order


ORDER = send_order()


def pick(table, me):
    total = jnp.int32(0)
    for d, value in enumerate(table):
        if value:
            total = total + jnp.where(me == d, jnp.int32(value), jnp.int32(0))
    return total


def ns_step(src, dst, gram, poly, m, block):
    def rows_of(i):
        return pl.ds(pl.multiple_of(i * block, block), block)

    @pl.loop(0, m // block)
    def _(i):
        rows = rows_of(i)
        gram[rows, :] = lax.dot_general(src[rows, :], src[...], NT, preferred_element_type=F32).astype(BF16)

    @pl.loop(0, m // block)
    def _(i):
        rows = rows_of(i)
        part = gram[rows, :]
        square = jnp.dot(part, gram[...], preferred_element_type=F32)
        poly[rows, :] = (COEF_B * part.astype(F32) + COEF_C * square).astype(BF16)

    @pl.loop(0, m // block)
    def _(i):
        rows = rows_of(i)
        product = jnp.dot(poly[rows, :], src[...], preferred_element_type=F32)
        dst[rows, :] = (COEF_A * src[rows, :].astype(F32) + product).astype(BF16)


STACKS = {"q": (3, 128, 2048, 32, 0), "o": (3, 128, 1024, 64, 0), "d": (12, 64, 1024, 64, 3), "u": (12, 128, 512, 128, 15)}
SCALE = {"q": RMS_MATCH * math.sqrt(2048), "o": RMS_MATCH * math.sqrt(1024),
         "d": RMS_MATCH * math.sqrt(1024), "u": RMS_MATCH * math.sqrt(1024)}
SEM_BASE = {"q": 0, "o": 3, "d": 6, "u": 18}


def place_of(kind, index):
    if kind == "q":
        return "q", index, QKV_OWNER[index], 0
    if kind == "o":
        return "o", index, OUT_OWNER[index], 0
    owner = EXPERT_OWNER[index]
    slot = index - EXPERT_BASE[owner]
    return ("d", index, owner, slot) if index < N_DOWN else ("u", index - N_DOWN, owner, slot)


def return_order():
    keys = []
    for number, (kind, index) in enumerate(ORDER):
        stack, position, owner, slot = place_of(kind, index)
        before = 75 * (owner in QKV_OWNER) + 42 * (owner in OUT_OWNER)
        work = before if kind != "e" else before + 10 * (slot + 1)
        keys.append((max(work, 2 * number) + (40 if kind == "q" else 0), len(keys), stack, position))
    return [(stack, position) for _, _, stack, position in sorted(keys)]


RETURNS = return_order()


def kernel(w_q, m_q, g_q, w_o, m_o, g_o, w_u, m_u, g_u, w_d, m_d, g_d,
           nw_q, nm_q, nw_o, nm_o, nw_u, nm_u, nw_d, nm_d,
           big, ebuf, gram, poly, xs_q, xs_o, xs_d, xs_u, bk_q, bk_o, bk_d, gs_u, bk_u,
           part_q, part_e, gath_q, gath_e, den_q, den_e,
           m_sem, g_sem, w_sem, norm_send, norm_recv, fwd_send, fwd_recv, ret_send, ret_recv):
    me = lax.axis_index("data")
    weights = {"q": w_q, "o": w_o, "d": w_d, "u": w_u}
    momenta = {"q": m_q, "o": m_o, "d": m_d, "u": m_u}
    gradients = {"q": g_q, "o": g_o, "d": g_d, "u": g_u}
    new_w = {"q": nw_q, "o": nw_o, "d": nw_d, "u": nw_u}
    new_m = {"q": nm_q, "o": nm_o, "d": nm_d, "u": nm_u}
    grad_in = {"q": bk_q, "o": bk_o, "d": bk_d, "u": gs_u}
    scaled = {"q": xs_q, "o": xs_o, "d": xs_d, "u": xs_u}
    back = {"q": bk_q, "o": bk_o, "d": bk_d, "u": bk_u}

    loads = {"q": [("q", i) for i in range(3)], "o": [("o", None)], "d": [("d", None)], "u": [("u", None)]}
    load_sem = {("q", 0): 0, ("q", 1): 1, ("q", 2): 2, ("o", None): 3, ("d", None): 4, ("u", None): 5}

    def part_of(ref, i):
        return ref if i is None else ref.at[i]

    def load_copies(key):
        stack, i = key
        sem = load_sem[key]
        return (pltpu.make_async_copy(part_of(momenta[stack], i), part_of(new_m[stack], i), m_sem.at[sem]),
                pltpu.make_async_copy(part_of(gradients[stack], i), part_of(grad_in[stack], i), g_sem.at[sem]))

    def weight_copy(stack, number):
        return pltpu.make_async_copy(weights[stack], new_w[stack], w_sem.at[number])

    for key in loads["q"]:
        for copy in load_copies(key):
            copy.start()

    barrier = pltpu.get_barrier_semaphore()
    for k in range(1, GROUP):
        pl.semaphore_signal(barrier, inc=1, device_id={"data": lax.rem(me + k, GROUP)}, device_id_type=MESH)

    part_q[...] = jnp.zeros_like(part_q)
    part_e[...] = jnp.zeros_like(part_e)

    def momentum_rows(stack, i, table, row):
        _, rows, cols, chunk, _ = STACKS[stack]
        lanes = jnp.zeros((1, 128), F32)
        for r in range(0, rows, chunk):
            at = pl.ds(r, chunk)
            mom = MOMENTUM * new_m[stack][i, at, :] + grad_in[stack][i, at, :].astype(F32)
            new_m[stack][i, at, :] = mom
            square = jnp.sum(mom * mom, axis=0, keepdims=True)
            for c in range(0, cols, 128):
                lanes = lanes + square[:, c:c + 128]
        table[pl.ds(row, 1), :] = lanes

    def push_norms(table, gathered, number):
        gathered[me] = table[...]
        for k in range(1, GROUP):
            pltpu.make_async_remote_copy(
                src_ref=table, dst_ref=gathered.at[me], send_sem=norm_send.at[number], recv_sem=norm_recv.at[number],
                device_id={"data": lax.rem(me + k, GROUP)}, device_id_type=MESH).start()

    def read_norms(gathered, den, number):
        seven = gathered.at[pl.ds(0, GROUP - 1)]
        pltpu.make_async_copy(seven, seven, norm_recv.at[number]).wait()
        total = gathered[0]
        for d in range(1, GROUP):
            total = total + gathered[d]
        total = jnp.sum(total, axis=1, keepdims=True)
        den[...] = jnp.broadcast_to(jnp.sqrt(total) + NORM_EPS, den.shape)

    def scale_rows(stack, i, den, row):
        _, rows, cols, chunk, _ = STACKS[stack]
        divisor = den[pl.ds(row, 1), 0:1]
        for r in range(0, rows, chunk):
            at = pl.ds(r, chunk)
            x = new_m[stack][i, at, :] / jnp.broadcast_to(divisor, (chunk, cols))
            if stack == "u":
                scaled[stack][i] = x.T.astype(BF16)
            else:
                scaled[stack][i, at, :] = x.astype(BF16)

    def block_of(stack, slot_ref, d):
        if stack == "u":
            return slot_ref.at[:, pl.ds(d * 128, 128)]
        rows = STACKS[stack][1]
        return slot_ref.at[pl.ds(d * rows, rows), :]

    def slot_of(stack, slot):
        if stack == "q":
            return big.at[0]
        if stack == "o":
            return big.at[0, :, pl.ds(0, 1024)]
        return ebuf.at[slot]

    def send_rows(stack, i, owner, slot):
        sem = SEM_BASE[stack] + i
        target = block_of(stack, slot_of(stack, slot), me)

        @pl.when(me != owner)
        def _():
            pltpu.make_async_remote_copy(
                src_ref=scaled[stack].at[i], dst_ref=target, send_sem=fwd_send.at[sem], recv_sem=fwd_recv.at[sem],
                device_id={"data": owner}, device_id_type=MESH).start()

        @pl.when(me == owner)
        def _():
            if stack == "u":
                for d in range(GROUP):
                    @pl.when(me == d)
                    def _():
                        ebuf[slot, :, d * 128:(d + 1) * 128] = scaled[stack][i]
            else:
                target[...] = scaled[stack][i]

    def momentum_stack(stack):
        for copy in load_copies((stack, None)):
            copy.wait()

        @pl.loop(0, STACKS[stack][0])
        def _(i):
            momentum_rows(stack, i, part_e, STACKS[stack][4] + i)

    def scale_stack(stack):
        @pl.loop(0, STACKS[stack][0])
        def _(i):
            scale_rows(stack, i, den_e, STACKS[stack][4] + i)

    for i in range(3):
        for copy in load_copies(("q", i)):
            copy.wait()
        if i == 0:
            for stack in ("o", "d", "u"):
                for copy in load_copies((stack, None)):
                    copy.start()
        momentum_rows("q", i, part_q, i)
    pl.semaphore_wait(barrier, GROUP - 1)
    push_norms(part_q, gath_q, 0)
    momentum_stack("o")
    momentum_stack("d")
    momentum_stack("u")
    push_norms(part_e, gath_e, 1)
    read_norms(gath_q, den_q, 0)
    places = [place_of(kind, index) for kind, index in ORDER]
    for stack, i, owner, slot in [p for p in places if p[0] == "q"]:
        scale_rows(stack, i, den_q, i)
        send_rows(stack, i, owner, slot)
    for number, stack in enumerate(("q", "o", "d", "u")):
        weight_copy(stack, number).start()
    read_norms(gath_e, den_e, 1)
    for stack in ("o", "d", "u"):
        scale_stack(stack)
    for stack, i, owner, slot in [p for p in places if p[0] != "q"]:
        send_rows(stack, i, owner, slot)

    def wait_parts(stack, slot_ref, sem):
        rows = 7 * STACKS[stack][1]
        part = slot_ref.at[:, pl.ds(0, rows)] if stack == "u" else slot_ref.at[pl.ds(0, rows), :]
        pltpu.make_async_copy(part, part, sem).wait()

    def give_back(stack, slot_ref, i, send_sem, recv_sem):
        half = me // 4
        crossing = [(1 - half) * 4 + k for k in range(4)]
        for dst in crossing + [half * 4 + lax.rem(me + k, 4) for k in range(1, 4)]:
            pltpu.make_async_remote_copy(
                src_ref=block_of(stack, slot_ref, dst), dst_ref=back[stack].at[i], send_sem=send_sem, recv_sem=recv_sem,
                device_id={"data": dst}, device_id_type=MESH).start()

    def new_weight(w, x, stack):
        return w - LEARN_RATE * (SCALE[stack] * x.astype(F32) + DECAY * w)

    def finish(stack, i, source):
        _, rows, cols, chunk, _ = STACKS[stack]
        for r in range(0, rows, chunk):
            at = pl.ds(r, chunk)
            x = source(at)
            if stack == "u":
                x = x.astype(F32).T
            new_w[stack][i, at, :] = new_weight(new_w[stack][i, at, :], x, stack)

    for index, owner in enumerate(QKV_OWNER):
        @pl.when(me == owner)
        def _():
            wait_parts("q", big.at[0], fwd_recv.at[index])

    @pl.when((me == QKV_OWNER[0]) | (me == QKV_OWNER[1]) | (me == QKV_OWNER[2]))
    def _():
        @pl.loop(0, NS_STEPS)
        def _(it):
            now = lax.rem(it, 2)
            ns_step(big.at[now], big.at[1 - now], gram, poly, 1024, 256)

    for index, owner in enumerate(QKV_OWNER):
        @pl.when(me == owner)
        def _():
            give_back("q", big.at[1], index, ret_send.at[0], ret_recv.at[index])
            back["q"][index] = big[1, pl.ds(owner * 128, 128), :]

    for index, owner in enumerate(OUT_OWNER):
        @pl.when(me == owner)
        def _():
            wait_parts("o", big.at[0, :, pl.ds(0, 1024)], fwd_recv.at[3 + index])

    @pl.when((me == OUT_OWNER[0]) | (me == OUT_OWNER[1]) | (me == OUT_OWNER[2]))
    def _():
        @pl.loop(0, NS_STEPS)
        def _(it):
            now = lax.rem(it, 2)
            ns_step(big.at[now, :, pl.ds(0, 1024)], big.at[1 - now, :, pl.ds(0, 1024)], gram, poly, 1024, 256)

    for index, owner in enumerate(OUT_OWNER):
        @pl.when(me == owner)
        def _():
            give_back("o", big.at[1, :, pl.ds(0, 1024)], index, ret_send.at[1], ret_recv.at[3 + index])
            back["o"][index] = big[1, pl.ds(owner * 128, 128), 0:1024]

    base, count = pick(EXPERT_BASE, me), pick(EXPERT_COUNT, me)
    small_gram, small_poly = gram.at[pl.ds(0, 512), pl.ds(0, 512)], poly.at[pl.ds(0, 512), pl.ds(0, 512)]

    @pl.loop(0, count)
    def _(t):
        rank = base + t

        @pl.when(rank < N_DOWN)
        def _():
            wait_parts("d", ebuf.at[t], fwd_recv.at[6 + rank])

        @pl.when(rank >= N_DOWN)
        def _():
            wait_parts("u", ebuf.at[t], fwd_recv.at[6 + rank])

        @pl.loop(0, NS_STEPS)
        def _(it):
            src = jnp.where(it == 0, t, MAX_EXPERTS + lax.rem(it + 1, 2))
            dst = jnp.where(it == NS_STEPS - 1, t, MAX_EXPERTS + lax.rem(it, 2))
            ns_step(ebuf.at[src], ebuf.at[dst], small_gram, small_poly, 512, 256)

        @pl.when(rank < N_DOWN)
        def _():
            give_back("d", ebuf.at[t], rank, ret_send.at[2 + t], ret_recv.at[6 + rank])
            back["d"][rank] = ebuf[t, pl.ds(pl.multiple_of(me * 64, 64), 64), :]

        @pl.when(rank >= N_DOWN)
        def _():
            give_back("u", ebuf.at[t], rank - N_DOWN, ret_send.at[2 + t], ret_recv.at[6 + rank])
            for d in range(GROUP):
                if EXPERT_BASE[d] + EXPERT_COUNT[d] > N_DOWN and EXPERT_COUNT[d]:
                    @pl.when(me == d)
                    def _():
                        back["u"][rank - N_DOWN] = ebuf[t, :, d * 128:(d + 1) * 128]

    for number, stack in enumerate(("q", "o", "d", "u")):
        weight_copy(stack, number).wait()
    owners = {(stack, i): owner for stack, i, owner, _ in places}
    for stack, i in RETURNS:
        owner, sem = owners[stack, i], SEM_BASE[stack] + i

        @pl.when(me != owner)
        def _():
            row = back[stack].at[i]
            pltpu.make_async_copy(row, row, ret_recv.at[sem]).wait()

        if stack == "u":
            finish(stack, i, lambda at: back["u"][i])
        else:
            finish(stack, i, lambda at: back[stack][i, at, :])

    for number, (table, gathered) in enumerate(((part_q, gath_q), (part_e, gath_e))):
        seven = gathered.at[pl.ds(0, GROUP - 1)]
        pltpu.make_async_copy(seven, seven, norm_send.at[number]).wait()
    for stack, i, owner, slot in places:
        @pl.when(me != owner)
        def _():
            block = scaled[stack].at[i]
            pltpu.make_async_copy(block, block, fwd_send.at[SEM_BASE[stack] + i]).wait()
    for owner in QKV_OWNER:
        @pl.when(me == owner)
        def _():
            wait_parts("q", big.at[1], ret_send.at[0])
    for owner in OUT_OWNER:
        @pl.when(me == owner)
        def _():
            wait_parts("o", big.at[1, :, pl.ds(0, 1024)], ret_send.at[1])

    @pl.loop(0, count)
    def _(t):
        @pl.when(base + t < N_DOWN)
        def _():
            wait_parts("d", ebuf.at[t], ret_send.at[2 + t])

        @pl.when(base + t >= N_DOWN)
        def _():
            wait_parts("u", ebuf.at[t], ret_send.at[2 + t])


OUT_SPACE = pltpu.VMEM


def store_kernel(*refs):
    copies = [pltpu.make_async_copy(refs[k], refs[8 + k], refs[16].at[k]) for k in range(8)]
    for copy in copies:
        copy.start()
    for copy in copies:
        copy.wait()


def solution(mesh):
    row_spec = P("stage", "data", None)

    def local_step(*args):
        shapes = [args[k].shape for k in (0, 3, 6, 9) for _ in range(2)]
        any_space = pl.BlockSpec(memory_space=pl.ANY)
        kept = pl.pallas_call(
            kernel,
            out_shape=[OUT_SPACE(shape, F32) for shape in shapes],
            in_specs=[any_space] * 12,
            out_specs=[pl.BlockSpec(memory_space=OUT_SPACE)] * 8,
            scratch_shapes=[
                pltpu.VMEM((2, 1024, 2048), BF16),
                pltpu.VMEM((MAX_EXPERTS + 2, 512, 1024), BF16),
                pltpu.VMEM((1024, 1024), BF16),
                pltpu.VMEM((1024, 1024), BF16),
                pltpu.VMEM((3, 128, 2048), BF16),
                pltpu.VMEM((3, 128, 1024), BF16),
                pltpu.VMEM((12, 64, 1024), BF16),
                pltpu.VMEM((12, 512, 128), BF16),
                pltpu.VMEM((3, 128, 2048), BF16),
                pltpu.VMEM((3, 128, 1024), BF16),
                pltpu.VMEM((12, 64, 1024), BF16),
                pltpu.VMEM((12, 128, 512), BF16),
                pltpu.VMEM((12, 512, 128), BF16),
                pltpu.VMEM((8, 128), F32),
                pltpu.VMEM((32, 128), F32),
                pltpu.VMEM((GROUP, 8, 128), F32),
                pltpu.VMEM((GROUP, 32, 128), F32),
                pltpu.VMEM((8, 128), F32),
                pltpu.VMEM((32, 128), F32),
                pltpu.SemaphoreType.DMA((6,)),
                pltpu.SemaphoreType.DMA((6,)),
                pltpu.SemaphoreType.DMA((4,)),
                pltpu.SemaphoreType.DMA((2,)),
                pltpu.SemaphoreType.DMA((2,)),
                pltpu.SemaphoreType.DMA((30,)),
                pltpu.SemaphoreType.DMA((30,)),
                pltpu.SemaphoreType.DMA((2 + MAX_EXPERTS,)),
                pltpu.SemaphoreType.DMA((30,)),
            ],
            compiler_params=pltpu.CompilerParams(
                collective_id=0, has_side_effects=True, vmem_limit_bytes=VMEM_LIMIT),
        )(*args)
        return tuple(pl.pallas_call(
            store_kernel,
            out_shape=[jax.ShapeDtypeStruct(shape, F32) for shape in shapes],
            in_specs=[any_space] * 8,
            out_specs=[any_space] * 8,
            scratch_shapes=[pltpu.SemaphoreType.DMA((8,))],
            compiler_params=pltpu.CompilerParams(vmem_limit_bytes=1024 * 1024),
        )(*kept))

    return jax.shard_map(local_step, mesh=mesh, in_specs=(row_spec,) * 12, out_specs=(row_spec,) * 8, check_vma=False)
```

```python
import math
import jax
import jax.numpy as jnp
from jax import lax
from jax.experimental import pallas as pl
from jax.experimental.pallas import tpu as pltpu
from jax.sharding import PartitionSpec as P

NS_STEPS = 5
COEF_A = 3.4445
COEF_B = -4.7750
COEF_C = 2.0315
MOMENTUM = 0.95
LEARN_RATE = 0.04
DECAY = 0.2
NORM_EPS = 1e-7
RMS_MATCH = 0.2

GROUP = 8
MESH = pl.DeviceIdType.MESH
NT = (((1,), (1,)), ((), ()))
F32 = jnp.float32
BF16 = jnp.bfloat16

QKV_OWNER = (2, 1, 5)
OUT_OWNER = (3, 4, 7)
EXPERT_COUNT = (2, 0, 4, 5, 8, 1, 4, 0)
EXPERT_BASE = tuple(sum(EXPERT_COUNT[:d]) for d in range(GROUP))
EXPERT_OWNER = tuple(d for d in range(GROUP) for _ in range(EXPERT_COUNT[d]))
N_DOWN = 12
MAX_EXPERTS = 8
VMEM_LIMIT = 40 * 1024 * 1024


def send_order():
    halves = ([], [])
    sizes = {"q": 4, "o": 2, "e": 1}
    for kind, owners in (("o", OUT_OWNER), ("q", QKV_OWNER)):
        for index, owner in enumerate(owners):
            halves[owner // 4].append((kind, index))
    for half in range(2):
        devices = [d for d in range(4 * half, 4 * half + 4) if EXPERT_COUNT[d]]
        slots = []
        for d in devices:
            for t in range(EXPERT_COUNT[d]):
                slots.append(((t + 0.5) / EXPERT_COUNT[d] + (d in QKV_OWNER), d, t))
        for _, d, t in sorted(slots):
            halves[half].append(("e", EXPERT_BASE[d] + t))
    order, sent, place = [], [0, 0], [0, 0]
    while place[0] < len(halves[0]) or place[1] < len(halves[1]):
        half = 0 if sent[0] <= sent[1] else 1
        if place[half] == len(halves[half]):
            half = 1 - half
        item = halves[half][place[half]]
        place[half] += 1
        sent[half] += sizes[item[0]]
        order.append(item)
    return order


ORDER = send_order()


def pick(table, me):
    total = jnp.int32(0)
    for d, value in enumerate(table):
        if value:
            total = total + jnp.where(me == d, jnp.int32(value), jnp.int32(0))
    return total


def ns_step(src, dst, gram, poly, m, block):
    def rows_of(i):
        return pl.ds(pl.multiple_of(i * block, block), block)

    @pl.loop(0, m // block)
    def _(i):
        rows = rows_of(i)
        gram[rows, :] = lax.dot_general(src[rows, :], src[...], NT, preferred_element_type=F32).astype(BF16)

    @pl.loop(0, m // block)
    def _(i):
        rows = rows_of(i)
        part = gram[rows, :]
        square = jnp.dot(part, gram[...], preferred_element_type=F32)
        poly[rows, :] = (COEF_B * part.astype(F32) + COEF_C * square).astype(BF16)

    @pl.loop(0, m // block)
    def _(i):
        rows = rows_of(i)
        product = jnp.dot(poly[rows, :], src[...], preferred_element_type=F32)
        dst[rows, :] = (COEF_A * src[rows, :].astype(F32) + product).astype(BF16)


STACKS = {"q": (3, 128, 2048, 32, 0), "o": (3, 128, 1024, 64, 0), "d": (12, 64, 1024, 64, 0), "u": (12, 128, 512, 128, 12)}
SCALE = {"q": RMS_MATCH * math.sqrt(2048), "o": RMS_MATCH * math.sqrt(1024),
         "d": RMS_MATCH * math.sqrt(1024), "u": RMS_MATCH * math.sqrt(1024)}
SEM_BASE = {"q": 0, "o": 3, "d": 6, "u": 18}


def place_of(kind, index):
    if kind == "q":
        return "q", index, QKV_OWNER[index], 0
    if kind == "o":
        return "o", index, OUT_OWNER[index], 0
    owner = EXPERT_OWNER[index]
    slot = index - EXPERT_BASE[owner]
    return ("d", index, owner, slot) if index < N_DOWN else ("u", index - N_DOWN, owner, slot)


def return_order():
    keys = []
    for number, (kind, index) in enumerate(ORDER):
        stack, position, owner, slot = place_of(kind, index)
        before = 75 * (owner in QKV_OWNER) + 42 * (owner in OUT_OWNER)
        work = before if kind != "e" else before + 10 * (slot + 1)
        keys.append((max(work, 2 * number) + (40 if kind == "q" else 0), len(keys), stack, position))
    return [(stack, position) for _, _, stack, position in sorted(keys)]


RETURNS = return_order()


def kernel(w_q, m_q, g_q, w_o, m_o, g_o, w_u, m_u, g_u, w_d, m_d, g_d,
           nw_q, nm_q, nw_o, nm_o, nw_u, nm_u, nw_d, nm_d,
           big, ebuf, gram, poly, xs_q, xs_o, xs_d, xs_u, bk_q, bk_o, bk_d, gs_u, bk_u,
           part, gath, den,
           m_sem, g_sem, w_sem, norm_send, norm_recv, fwd_send, fwd_recv, ret_send, ret_recv):
    me = lax.axis_index("data")
    weights = {"q": w_q, "o": w_o, "d": w_d, "u": w_u}
    momenta = {"q": m_q, "o": m_o, "d": m_d, "u": m_u}
    gradients = {"q": g_q, "o": g_o, "d": g_d, "u": g_u}
    new_w = {"q": nw_q, "o": nw_o, "d": nw_d, "u": nw_u}
    new_m = {"q": nm_q, "o": nm_o, "d": nm_d, "u": nm_u}
    grad_in = {"q": bk_q, "o": bk_o, "d": bk_d, "u": gs_u}
    scaled = {"q": xs_q, "o": xs_o, "d": xs_d, "u": xs_u}
    back = {"q": bk_q, "o": bk_o, "d": bk_d, "u": bk_u}

    loads = {"q": [("q", i) for i in range(3)], "o": [("o", None)], "d": [("d", None)], "u": [("u", None)]}
    load_sem = {("q", 0): 0, ("q", 1): 1, ("q", 2): 2, ("o", None): 3, ("d", None): 4, ("u", None): 5}

    def part_of(ref, i):
        return ref if i is None else ref.at[i]

    def load_copies(key):
        stack, i = key
        sem = load_sem[key]
        return (pltpu.make_async_copy(part_of(momenta[stack], i), part_of(new_m[stack], i), m_sem.at[sem]),
                pltpu.make_async_copy(part_of(gradients[stack], i), part_of(grad_in[stack], i), g_sem.at[sem]))

    def weight_copy(stack, number):
        return pltpu.make_async_copy(weights[stack], new_w[stack], w_sem.at[number])

    for key in loads["o"] + loads["q"]:
        for copy in load_copies(key):
            copy.start()

    barrier = pltpu.get_barrier_semaphore()
    for k in range(1, GROUP):
        pl.semaphore_signal(barrier, inc=1, device_id={"data": lax.rem(me + k, GROUP)}, device_id_type=MESH)

    part[...] = jnp.zeros_like(part)
    lane = lax.broadcasted_iota(jnp.int32, (8, 128), 1)

    def momentum_rows(stack, i, number, column):
        _, rows, cols, chunk, _ = STACKS[stack]
        lanes = jnp.zeros((1, 128), F32)
        for r in range(0, rows, chunk):
            at = pl.ds(r, chunk)
            mom = MOMENTUM * new_m[stack][i, at, :] + grad_in[stack][i, at, :].astype(F32)
            new_m[stack][i, at, :] = mom
            square = jnp.sum(mom * mom, axis=0, keepdims=True)
            for c in range(0, cols, 128):
                lanes = lanes + square[:, c:c + 128]
        total = jnp.sum(lanes, axis=1, keepdims=True)
        part[number] = jnp.where(lane == column, jnp.broadcast_to(total, (8, 128)), part[number])

    def push_norms(number):
        gath[number, me] = part[number]
        for k in range(1, GROUP):
            pltpu.make_async_remote_copy(
                src_ref=part.at[number], dst_ref=gath.at[number, me], send_sem=norm_send.at[number],
                recv_sem=norm_recv.at[number], device_id={"data": lax.rem(me + k, GROUP)}, device_id_type=MESH).start()

    def read_norms(number):
        seven = gath.at[number, pl.ds(0, GROUP - 1)]
        pltpu.make_async_copy(seven, seven, norm_recv.at[number]).wait()
        total = gath[number, 0]
        for d in range(1, GROUP):
            total = total + gath[number, d]
        den[number] = jnp.sqrt(total) + NORM_EPS

    def scale_rows(stack, i, number, column):
        _, rows, cols, chunk, _ = STACKS[stack]
        divisor = jnp.sum(jnp.where(lane[:1] == column, den[number, 0:1, :], 0.0), axis=1, keepdims=True)
        for r in range(0, rows, chunk):
            at = pl.ds(r, chunk)
            x = new_m[stack][i, at, :] / jnp.broadcast_to(divisor, (chunk, cols))
            if stack == "u":
                scaled[stack][i] = x.T.astype(BF16)
            else:
                scaled[stack][i, at, :] = x.astype(BF16)

    def block_of(stack, slot_ref, d):
        if stack == "u":
            return slot_ref.at[:, pl.ds(d * 128, 128)]
        rows = STACKS[stack][1]
        return slot_ref.at[pl.ds(d * rows, rows), :]

    def slot_of(stack, slot):
        if stack == "q":
            return big.at[0]
        if stack == "o":
            return big.at[0, :, pl.ds(0, 1024)]
        return ebuf.at[slot]

    def send_rows(stack, i, owner, slot):
        sem = SEM_BASE[stack] + i
        target = block_of(stack, slot_of(stack, slot), me)

        @pl.when(me != owner)
        def _():
            pltpu.make_async_remote_copy(
                src_ref=scaled[stack].at[i], dst_ref=target, send_sem=fwd_send.at[sem], recv_sem=fwd_recv.at[sem],
                device_id={"data": owner}, device_id_type=MESH).start()

        @pl.when(me == owner)
        def _():
            if stack == "u":
                for d in range(GROUP):
                    @pl.when(me == d)
                    def _():
                        ebuf[slot, :, d * 128:(d + 1) * 128] = scaled[stack][i]
            else:
                target[...] = scaled[stack][i]

    def momentum_stack(stack, number):
        for copy in load_copies((stack, None)):
            copy.wait()

        @pl.loop(0, STACKS[stack][0])
        def _(i):
            momentum_rows(stack, i, number, STACKS[stack][4] + i)

    places = [place_of(kind, index) for kind, index in ORDER]

    def scale_and_send(stack, number):
        for kind, i, owner, slot in places:
            if kind == stack:
                scale_rows(stack, i, number, i)
                send_rows(stack, i, owner, slot)

    momentum_stack("o", 0)
    pl.semaphore_wait(barrier, GROUP - 1)
    push_norms(0)
    for stack in ("d", "u"):
        for copy in load_copies((stack, None)):
            copy.start()
    for i in range(3):
        for copy in load_copies(("q", i)):
            copy.wait()
        momentum_rows("q", i, 1, i)
    push_norms(1)
    momentum_stack("d", 2)
    read_norms(0)
    scale_and_send("o", 0)
    momentum_stack("u", 2)
    push_norms(2)
    read_norms(1)
    scale_and_send("q", 1)
    for number, stack in enumerate(("q", "o", "d", "u")):
        weight_copy(stack, number).start()
    read_norms(2)
    for stack in ("d", "u"):
        @pl.loop(0, STACKS[stack][0])
        def _(i):
            scale_rows(stack, i, 2, STACKS[stack][4] + i)
    for stack, i, owner, slot in places:
        if stack in "du":
            send_rows(stack, i, owner, slot)

    def wait_parts(stack, slot_ref, sem):
        rows = 7 * STACKS[stack][1]
        part = slot_ref.at[:, pl.ds(0, rows)] if stack == "u" else slot_ref.at[pl.ds(0, rows), :]
        pltpu.make_async_copy(part, part, sem).wait()

    def give_back(stack, slot_ref, i, send_sem, recv_sem):
        half = me // 4
        crossing = [(1 - half) * 4 + k for k in range(4)]
        for dst in crossing + [half * 4 + lax.rem(me + k, 4) for k in range(1, 4)]:
            pltpu.make_async_remote_copy(
                src_ref=block_of(stack, slot_ref, dst), dst_ref=back[stack].at[i], send_sem=send_sem, recv_sem=recv_sem,
                device_id={"data": dst}, device_id_type=MESH).start()

    def new_weight(w, x, stack):
        return w - LEARN_RATE * (SCALE[stack] * x.astype(F32) + DECAY * w)

    def finish(stack, i, source):
        _, rows, cols, chunk, _ = STACKS[stack]
        for r in range(0, rows, chunk):
            at = pl.ds(r, chunk)
            x = source(at)
            if stack == "u":
                x = x.astype(F32).T
            new_w[stack][i, at, :] = new_weight(new_w[stack][i, at, :], x, stack)

    for index, owner in enumerate(QKV_OWNER):
        @pl.when(me == owner)
        def _():
            wait_parts("q", big.at[0], fwd_recv.at[index])

    @pl.when((me == QKV_OWNER[0]) | (me == QKV_OWNER[1]) | (me == QKV_OWNER[2]))
    def _():
        @pl.loop(0, NS_STEPS)
        def _(it):
            now = lax.rem(it, 2)
            ns_step(big.at[now], big.at[1 - now], gram, poly, 1024, 256)

    for index, owner in enumerate(QKV_OWNER):
        @pl.when(me == owner)
        def _():
            give_back("q", big.at[1], index, ret_send.at[0], ret_recv.at[index])
            back["q"][index] = big[1, pl.ds(owner * 128, 128), :]

    for index, owner in enumerate(OUT_OWNER):
        @pl.when(me == owner)
        def _():
            wait_parts("o", big.at[0, :, pl.ds(0, 1024)], fwd_recv.at[3 + index])

    @pl.when((me == OUT_OWNER[0]) | (me == OUT_OWNER[1]) | (me == OUT_OWNER[2]))
    def _():
        @pl.loop(0, NS_STEPS)
        def _(it):
            now = lax.rem(it, 2)
            ns_step(big.at[now, :, pl.ds(0, 1024)], big.at[1 - now, :, pl.ds(0, 1024)], gram, poly, 1024, 256)

    for index, owner in enumerate(OUT_OWNER):
        @pl.when(me == owner)
        def _():
            give_back("o", big.at[1, :, pl.ds(0, 1024)], index, ret_send.at[1], ret_recv.at[3 + index])
            back["o"][index] = big[1, pl.ds(owner * 128, 128), 0:1024]

    base, count = pick(EXPERT_BASE, me), pick(EXPERT_COUNT, me)
    small_gram, small_poly = gram.at[pl.ds(0, 512), pl.ds(0, 512)], poly.at[pl.ds(0, 512), pl.ds(0, 512)]

    @pl.loop(0, count)
    def _(t):
        rank = base + t

        @pl.when(rank < N_DOWN)
        def _():
            wait_parts("d", ebuf.at[t], fwd_recv.at[6 + rank])

        @pl.when(rank >= N_DOWN)
        def _():
            wait_parts("u", ebuf.at[t], fwd_recv.at[6 + rank])

        @pl.loop(0, NS_STEPS)
        def _(it):
            src = jnp.where(it == 0, t, MAX_EXPERTS + lax.rem(it + 1, 2))
            dst = jnp.where(it == NS_STEPS - 1, t, MAX_EXPERTS + lax.rem(it, 2))
            ns_step(ebuf.at[src], ebuf.at[dst], small_gram, small_poly, 512, 256)

        @pl.when(rank < N_DOWN)
        def _():
            give_back("d", ebuf.at[t], rank, ret_send.at[2 + t], ret_recv.at[6 + rank])
            back["d"][rank] = ebuf[t, pl.ds(pl.multiple_of(me * 64, 64), 64), :]

        @pl.when(rank >= N_DOWN)
        def _():
            give_back("u", ebuf.at[t], rank - N_DOWN, ret_send.at[2 + t], ret_recv.at[6 + rank])
            for d in range(GROUP):
                if EXPERT_BASE[d] + EXPERT_COUNT[d] > N_DOWN and EXPERT_COUNT[d]:
                    @pl.when(me == d)
                    def _():
                        back["u"][rank - N_DOWN] = ebuf[t, :, d * 128:(d + 1) * 128]

    for number, stack in enumerate(("q", "o", "d", "u")):
        weight_copy(stack, number).wait()
    owners = {(stack, i): owner for stack, i, owner, _ in places}
    for stack, i in RETURNS:
        owner, sem = owners[stack, i], SEM_BASE[stack] + i

        @pl.when(me != owner)
        def _():
            row = back[stack].at[i]
            pltpu.make_async_copy(row, row, ret_recv.at[sem]).wait()

        if stack == "u":
            finish(stack, i, lambda at: back["u"][i])
        else:
            finish(stack, i, lambda at: back[stack][i, at, :])

    for number in range(3):
        seven = gath.at[number, pl.ds(0, GROUP - 1)]
        pltpu.make_async_copy(seven, seven, norm_send.at[number]).wait()
    for stack, i, owner, slot in places:
        @pl.when(me != owner)
        def _():
            block = scaled[stack].at[i]
            pltpu.make_async_copy(block, block, fwd_send.at[SEM_BASE[stack] + i]).wait()
    for owner in QKV_OWNER:
        @pl.when(me == owner)
        def _():
            wait_parts("q", big.at[1], ret_send.at[0])
    for owner in OUT_OWNER:
        @pl.when(me == owner)
        def _():
            wait_parts("o", big.at[1, :, pl.ds(0, 1024)], ret_send.at[1])

    @pl.loop(0, count)
    def _(t):
        @pl.when(base + t < N_DOWN)
        def _():
            wait_parts("d", ebuf.at[t], ret_send.at[2 + t])

        @pl.when(base + t >= N_DOWN)
        def _():
            wait_parts("u", ebuf.at[t], ret_send.at[2 + t])


OUT_SPACE = pltpu.VMEM


def store_kernel(*refs):
    copies = [pltpu.make_async_copy(refs[k], refs[8 + k], refs[16].at[k]) for k in range(8)]
    for copy in copies:
        copy.start()
    for copy in copies:
        copy.wait()


def solution(mesh):
    row_spec = P("stage", "data", None)

    def local_step(*args):
        shapes = [args[k].shape for k in (0, 3, 6, 9) for _ in range(2)]
        any_space = pl.BlockSpec(memory_space=pl.ANY)
        kept = pl.pallas_call(
            kernel,
            out_shape=[OUT_SPACE(shape, F32) for shape in shapes],
            in_specs=[any_space] * 12,
            out_specs=[pl.BlockSpec(memory_space=OUT_SPACE)] * 8,
            scratch_shapes=[
                pltpu.VMEM((2, 1024, 2048), BF16),
                pltpu.VMEM((MAX_EXPERTS + 2, 512, 1024), BF16),
                pltpu.VMEM((1024, 1024), BF16),
                pltpu.VMEM((1024, 1024), BF16),
                pltpu.VMEM((3, 128, 2048), BF16),
                pltpu.VMEM((3, 128, 1024), BF16),
                pltpu.VMEM((12, 64, 1024), BF16),
                pltpu.VMEM((12, 512, 128), BF16),
                pltpu.VMEM((3, 128, 2048), BF16),
                pltpu.VMEM((3, 128, 1024), BF16),
                pltpu.VMEM((12, 64, 1024), BF16),
                pltpu.VMEM((12, 128, 512), BF16),
                pltpu.VMEM((12, 512, 128), BF16),
                pltpu.VMEM((3, 8, 128), F32),
                pltpu.VMEM((3, GROUP, 8, 128), F32),
                pltpu.VMEM((3, 8, 128), F32),
                pltpu.SemaphoreType.DMA((6,)),
                pltpu.SemaphoreType.DMA((6,)),
                pltpu.SemaphoreType.DMA((4,)),
                pltpu.SemaphoreType.DMA((3,)),
                pltpu.SemaphoreType.DMA((3,)),
                pltpu.SemaphoreType.DMA((30,)),
                pltpu.SemaphoreType.DMA((30,)),
                pltpu.SemaphoreType.DMA((2 + MAX_EXPERTS,)),
                pltpu.SemaphoreType.DMA((30,)),
            ],
            compiler_params=pltpu.CompilerParams(
                collective_id=0, has_side_effects=True, vmem_limit_bytes=VMEM_LIMIT),
        )(*args)
        return tuple(pl.pallas_call(
            store_kernel,
            out_shape=[jax.ShapeDtypeStruct(shape, F32) for shape in shapes],
            in_specs=[any_space] * 8,
            out_specs=[any_space] * 8,
            scratch_shapes=[pltpu.SemaphoreType.DMA((8,))],
            compiler_params=pltpu.CompilerParams(vmem_limit_bytes=1024 * 1024),
        )(*kept))

    return jax.shard_map(local_step, mesh=mesh, in_specs=(row_spec,) * 12, out_specs=(row_spec,) * 8, check_vma=False)
```

```python
import math
import jax
import jax.numpy as jnp
from jax import lax
from jax.experimental import pallas as pl
from jax.experimental.pallas import tpu as pltpu
from jax.sharding import PartitionSpec as P

NS_STEPS = 5
COEF_A = 3.4445
COEF_B = -4.7750
COEF_C = 2.0315
MOMENTUM = 0.95
LEARN_RATE = 0.04
DECAY = 0.2
NORM_EPS = 1e-7
RMS_MATCH = 0.2

GROUP = 8
MESH = pl.DeviceIdType.MESH
NT = (((1,), (1,)), ((), ()))
F32 = jnp.float32
BF16 = jnp.bfloat16

QKV_OWNER = (2, 1, 5)
OUT_OWNER = (3, 4, 7)
EXPERT_COUNT = (2, 0, 4, 5, 8, 1, 4, 0)
EXPERT_BASE = tuple(sum(EXPERT_COUNT[:d]) for d in range(GROUP))
EXPERT_OWNER = tuple(d for d in range(GROUP) for _ in range(EXPERT_COUNT[d]))
N_DOWN = 12
MAX_EXPERTS = 8
VMEM_LIMIT = 40 * 1024 * 1024


def send_order():
    halves = ([], [])
    sizes = {"q": 4, "o": 2, "e": 1}
    for kind, owners in (("o", OUT_OWNER), ("q", QKV_OWNER)):
        for index, owner in enumerate(owners):
            halves[owner // 4].append((kind, index))
    for half in range(2):
        devices = [d for d in range(4 * half, 4 * half + 4) if EXPERT_COUNT[d]]
        slots = []
        for d in devices:
            for t in range(EXPERT_COUNT[d]):
                slots.append(((t + 0.5) / EXPERT_COUNT[d] + (d in QKV_OWNER), d, t))
        for _, d, t in sorted(slots):
            halves[half].append(("e", EXPERT_BASE[d] + t))
    order, sent, place = [], [0, 0], [0, 0]
    while place[0] < len(halves[0]) or place[1] < len(halves[1]):
        half = 0 if sent[0] <= sent[1] else 1
        if place[half] == len(halves[half]):
            half = 1 - half
        item = halves[half][place[half]]
        place[half] += 1
        sent[half] += sizes[item[0]]
        order.append(item)
    return order


ORDER = send_order()


def pick(table, me):
    total = jnp.int32(0)
    for d, value in enumerate(table):
        if value:
            total = total + jnp.where(me == d, jnp.int32(value), jnp.int32(0))
    return total


def ns_step(src, dst, gram, poly, m, block):
    def rows_of(i):
        return pl.ds(pl.multiple_of(i * block, block), block)

    @pl.loop(0, m // block)
    def _(i):
        rows = rows_of(i)
        gram[rows, :] = lax.dot_general(src[rows, :], src[...], NT, preferred_element_type=F32).astype(BF16)

    @pl.loop(0, m // block)
    def _(i):
        rows = rows_of(i)
        part = gram[rows, :]
        square = jnp.dot(part, gram[...], preferred_element_type=F32)
        poly[rows, :] = (COEF_B * part.astype(F32) + COEF_C * square).astype(BF16)

    @pl.loop(0, m // block)
    def _(i):
        rows = rows_of(i)
        product = jnp.dot(poly[rows, :], src[...], preferred_element_type=F32)
        dst[rows, :] = (COEF_A * src[rows, :].astype(F32) + product).astype(BF16)


STACKS = {"q": (3, 128, 2048, 32, 0), "o": (3, 128, 1024, 64, 0), "d": (12, 64, 1024, 64, 0), "u": (12, 128, 512, 128, 12)}
SCALE = {"q": RMS_MATCH * math.sqrt(2048), "o": RMS_MATCH * math.sqrt(1024),
         "d": RMS_MATCH * math.sqrt(1024), "u": RMS_MATCH * math.sqrt(1024)}
SEM_BASE = {"q": 0, "o": 3, "d": 6, "u": 18}


def place_of(kind, index):
    if kind == "q":
        return "q", index, QKV_OWNER[index], 0
    if kind == "o":
        return "o", index, OUT_OWNER[index], 0
    owner = EXPERT_OWNER[index]
    slot = index - EXPERT_BASE[owner]
    return ("d", index, owner, slot) if index < N_DOWN else ("u", index - N_DOWN, owner, slot)


def return_order():
    keys = []
    for kind, index in ORDER:
        stack, position, owner, slot = place_of(kind, index)
        held = 4 * (owner in QKV_OWNER) + 2 * (owner in OUT_OWNER)
        keys.append((held + (slot + 1 if kind == "e" else 0), len(keys), stack, position))
    return [(stack, position) for _, _, stack, position in sorted(keys)]


RETURNS = return_order()


def kernel(w_q, m_q, g_q, w_o, m_o, g_o, w_u, m_u, g_u, w_d, m_d, g_d,
           nw_q, nm_q, nw_o, nm_o, nw_u, nm_u, nw_d, nm_d,
           big, ebuf, gram, poly, xs_q, xs_o, xs_d, xs_u, bk_q, bk_o, bk_d, gs_u, bk_u,
           part, gath, den,
           m_sem, g_sem, w_sem, norm_send, norm_recv, fwd_send, fwd_recv, ret_send, ret_recv):
    me = lax.axis_index("data")
    weights = {"q": w_q, "o": w_o, "d": w_d, "u": w_u}
    momenta = {"q": m_q, "o": m_o, "d": m_d, "u": m_u}
    gradients = {"q": g_q, "o": g_o, "d": g_d, "u": g_u}
    new_w = {"q": nw_q, "o": nw_o, "d": nw_d, "u": nw_u}
    new_m = {"q": nm_q, "o": nm_o, "d": nm_d, "u": nm_u}
    grad_in = {"q": bk_q, "o": bk_o, "d": bk_d, "u": gs_u}
    scaled = {"q": xs_q, "o": xs_o, "d": xs_d, "u": xs_u}
    back = {"q": bk_q, "o": bk_o, "d": bk_d, "u": bk_u}

    loads = {"q": [("q", i) for i in range(3)], "o": [("o", None)], "d": [("d", None)], "u": [("u", None)]}
    load_sem = {("q", 0): 0, ("q", 1): 1, ("q", 2): 2, ("o", None): 3, ("d", None): 4, ("u", None): 5}

    def part_of(ref, i):
        return ref if i is None else ref.at[i]

    def load_copies(key):
        stack, i = key
        sem = load_sem[key]
        return (pltpu.make_async_copy(part_of(momenta[stack], i), part_of(new_m[stack], i), m_sem.at[sem]),
                pltpu.make_async_copy(part_of(gradients[stack], i), part_of(grad_in[stack], i), g_sem.at[sem]))

    def weight_copy(stack, number):
        return pltpu.make_async_copy(weights[stack], new_w[stack], w_sem.at[number])

    for key in loads["o"] + loads["q"]:
        for copy in load_copies(key):
            copy.start()

    barrier = pltpu.get_barrier_semaphore()
    for k in range(1, GROUP):
        pl.semaphore_signal(barrier, inc=1, device_id={"data": lax.rem(me + k, GROUP)}, device_id_type=MESH)

    part[...] = jnp.zeros_like(part)
    lane = lax.broadcasted_iota(jnp.int32, (8, 128), 1)

    def momentum_rows(stack, i, number, column):
        _, rows, cols, chunk, _ = STACKS[stack]
        lanes = jnp.zeros((1, 128), F32)
        for r in range(0, rows, chunk):
            at = pl.ds(r, chunk)
            mom = MOMENTUM * new_m[stack][i, at, :] + grad_in[stack][i, at, :].astype(F32)
            new_m[stack][i, at, :] = mom
            square = jnp.sum(mom * mom, axis=0, keepdims=True)
            for c in range(0, cols, 128):
                lanes = lanes + square[:, c:c + 128]
        total = jnp.sum(lanes, axis=1, keepdims=True)
        part[number] = jnp.where(lane == column, jnp.broadcast_to(total, (8, 128)), part[number])

    def push_norms(number):
        gath[number, me] = part[number]
        for k in range(1, GROUP):
            pltpu.make_async_remote_copy(
                src_ref=part.at[number], dst_ref=gath.at[number, me], send_sem=norm_send.at[number],
                recv_sem=norm_recv.at[number], device_id={"data": lax.rem(me + k, GROUP)}, device_id_type=MESH).start()

    def read_norms(number):
        seven = gath.at[number, pl.ds(0, GROUP - 1)]
        pltpu.make_async_copy(seven, seven, norm_recv.at[number]).wait()
        total = gath[number, 0]
        for d in range(1, GROUP):
            total = total + gath[number, d]
        den[number] = jnp.sqrt(total) + NORM_EPS

    def scale_rows(stack, i, number, column):
        _, rows, cols, chunk, _ = STACKS[stack]
        divisor = jnp.sum(jnp.where(lane[:1] == column, den[number, 0:1, :], 0.0), axis=1, keepdims=True)
        for r in range(0, rows, chunk):
            at = pl.ds(r, chunk)
            x = new_m[stack][i, at, :] / jnp.broadcast_to(divisor, (chunk, cols))
            if stack == "u":
                scaled[stack][i] = x.T.astype(BF16)
            else:
                scaled[stack][i, at, :] = x.astype(BF16)

    def block_of(stack, slot_ref, d):
        if stack == "u":
            return slot_ref.at[:, pl.ds(d * 128, 128)]
        rows = STACKS[stack][1]
        return slot_ref.at[pl.ds(d * rows, rows), :]

    def slot_of(stack, slot):
        if stack == "q":
            return big.at[0]
        if stack == "o":
            return big.at[0, :, pl.ds(0, 1024)]
        return ebuf.at[slot]

    def send_rows(stack, i, owner, slot):
        sem = SEM_BASE[stack] + i
        target = block_of(stack, slot_of(stack, slot), me)

        @pl.when(me != owner)
        def _():
            pltpu.make_async_remote_copy(
                src_ref=scaled[stack].at[i], dst_ref=target, send_sem=fwd_send.at[sem], recv_sem=fwd_recv.at[sem],
                device_id={"data": owner}, device_id_type=MESH).start()

        @pl.when(me == owner)
        def _():
            if stack == "u":
                for d in range(GROUP):
                    @pl.when(me == d)
                    def _():
                        ebuf[slot, :, d * 128:(d + 1) * 128] = scaled[stack][i]
            else:
                target[...] = scaled[stack][i]

    def momentum_stack(stack, number):
        for copy in load_copies((stack, None)):
            copy.wait()
        momentum_loop(stack, number)

    def momentum_loop(stack, number):
        @pl.loop(0, STACKS[stack][0])
        def _(i):
            momentum_rows(stack, i, number, STACKS[stack][4] + i)

    places = [place_of(kind, index) for kind, index in ORDER]

    def scale_and_send(stack, number):
        for kind, i, owner, slot in places:
            if kind == stack:
                scale_rows(stack, i, number, i)
                send_rows(stack, i, owner, slot)

    for copy in load_copies(("o", None)):
        copy.wait()
    for stack in ("d", "u"):
        for copy in load_copies((stack, None)):
            copy.start()
    momentum_loop("o", 0)
    pl.semaphore_wait(barrier, GROUP - 1)
    push_norms(0)
    for i in range(3):
        for copy in load_copies(("q", i)):
            copy.wait()
        momentum_rows("q", i, 1, i)
    push_norms(1)
    momentum_stack("d", 2)
    read_norms(0)
    scale_and_send("o", 0)
    momentum_stack("u", 2)
    push_norms(2)
    read_norms(1)
    scale_and_send("q", 1)
    for number, stack in enumerate(("q", "o", "d", "u")):
        weight_copy(stack, number).start()
    read_norms(2)
    for stack in ("d", "u"):
        @pl.loop(0, STACKS[stack][0])
        def _(i):
            scale_rows(stack, i, 2, STACKS[stack][4] + i)
    for stack, i, owner, slot in places:
        if stack in "du":
            send_rows(stack, i, owner, slot)

    def wait_parts(stack, slot_ref, sem):
        rows = 7 * STACKS[stack][1]
        part = slot_ref.at[:, pl.ds(0, rows)] if stack == "u" else slot_ref.at[pl.ds(0, rows), :]
        pltpu.make_async_copy(part, part, sem).wait()

    def give_back(stack, slot_ref, i, send_sem, recv_sem):
        half = me // 4
        crossing = [(1 - half) * 4 + k for k in range(4)]
        for dst in crossing + [half * 4 + lax.rem(me + k, 4) for k in range(1, 4)]:
            pltpu.make_async_remote_copy(
                src_ref=block_of(stack, slot_ref, dst), dst_ref=back[stack].at[i], send_sem=send_sem, recv_sem=recv_sem,
                device_id={"data": dst}, device_id_type=MESH).start()

    def new_weight(w, x, stack):
        return w - LEARN_RATE * (SCALE[stack] * x.astype(F32) + DECAY * w)

    def finish(stack, i, source):
        _, rows, cols, chunk, _ = STACKS[stack]
        for r in range(0, rows, chunk):
            at = pl.ds(r, chunk)
            x = source(at)
            if stack == "u":
                x = x.astype(F32).T
            new_w[stack][i, at, :] = new_weight(new_w[stack][i, at, :], x, stack)

    for index, owner in enumerate(QKV_OWNER):
        @pl.when(me == owner)
        def _():
            wait_parts("q", big.at[0], fwd_recv.at[index])

    @pl.when((me == QKV_OWNER[0]) | (me == QKV_OWNER[1]) | (me == QKV_OWNER[2]))
    def _():
        @pl.loop(0, NS_STEPS)
        def _(it):
            now = lax.rem(it, 2)
            ns_step(big.at[now], big.at[1 - now], gram, poly, 1024, 256)

    for index, owner in enumerate(QKV_OWNER):
        @pl.when(me == owner)
        def _():
            give_back("q", big.at[1], index, ret_send.at[0], ret_recv.at[index])
            back["q"][index] = big[1, pl.ds(owner * 128, 128), :]

    for index, owner in enumerate(OUT_OWNER):
        @pl.when(me == owner)
        def _():
            wait_parts("o", big.at[0, :, pl.ds(0, 1024)], fwd_recv.at[3 + index])

    @pl.when((me == OUT_OWNER[0]) | (me == OUT_OWNER[1]) | (me == OUT_OWNER[2]))
    def _():
        @pl.loop(0, NS_STEPS)
        def _(it):
            now = lax.rem(it, 2)
            ns_step(big.at[now, :, pl.ds(0, 1024)], big.at[1 - now, :, pl.ds(0, 1024)], gram, poly, 1024, 256)

    for index, owner in enumerate(OUT_OWNER):
        @pl.when(me == owner)
        def _():
            give_back("o", big.at[1, :, pl.ds(0, 1024)], index, ret_send.at[1], ret_recv.at[3 + index])
            back["o"][index] = big[1, pl.ds(owner * 128, 128), 0:1024]

    base, count = pick(EXPERT_BASE, me), pick(EXPERT_COUNT, me)
    small_gram, small_poly = gram.at[pl.ds(0, 512), pl.ds(0, 512)], poly.at[pl.ds(0, 512), pl.ds(0, 512)]

    @pl.loop(0, count)
    def _(t):
        rank = base + t

        @pl.when(rank < N_DOWN)
        def _():
            wait_parts("d", ebuf.at[t], fwd_recv.at[6 + rank])

        @pl.when(rank >= N_DOWN)
        def _():
            wait_parts("u", ebuf.at[t], fwd_recv.at[6 + rank])

        @pl.loop(0, NS_STEPS)
        def _(it):
            src = jnp.where(it == 0, t, MAX_EXPERTS + lax.rem(it + 1, 2))
            dst = jnp.where(it == NS_STEPS - 1, t, MAX_EXPERTS + lax.rem(it, 2))
            ns_step(ebuf.at[src], ebuf.at[dst], small_gram, small_poly, 512, 256)

        @pl.when(rank < N_DOWN)
        def _():
            give_back("d", ebuf.at[t], rank, ret_send.at[2 + t], ret_recv.at[6 + rank])
            back["d"][rank] = ebuf[t, pl.ds(pl.multiple_of(me * 64, 64), 64), :]

        @pl.when(rank >= N_DOWN)
        def _():
            give_back("u", ebuf.at[t], rank - N_DOWN, ret_send.at[2 + t], ret_recv.at[6 + rank])
            for d in range(GROUP):
                if EXPERT_BASE[d] + EXPERT_COUNT[d] > N_DOWN and EXPERT_COUNT[d]:
                    @pl.when(me == d)
                    def _():
                        back["u"][rank - N_DOWN] = ebuf[t, :, d * 128:(d + 1) * 128]

    for number, stack in enumerate(("q", "o", "d", "u")):
        weight_copy(stack, number).wait()
    owners = {(stack, i): owner for stack, i, owner, _ in places}
    for stack, i in RETURNS:
        owner, sem = owners[stack, i], SEM_BASE[stack] + i

        @pl.when(me != owner)
        def _():
            row = back[stack].at[i]
            pltpu.make_async_copy(row, row, ret_recv.at[sem]).wait()

        if stack == "u":
            finish(stack, i, lambda at: back["u"][i])
        else:
            finish(stack, i, lambda at: back[stack][i, at, :])

    for number in range(3):
        seven = gath.at[number, pl.ds(0, GROUP - 1)]
        pltpu.make_async_copy(seven, seven, norm_send.at[number]).wait()
    for stack, i, owner, slot in places:
        @pl.when(me != owner)
        def _():
            block = scaled[stack].at[i]
            pltpu.make_async_copy(block, block, fwd_send.at[SEM_BASE[stack] + i]).wait()
    for owner in QKV_OWNER:
        @pl.when(me == owner)
        def _():
            wait_parts("q", big.at[1], ret_send.at[0])
    for owner in OUT_OWNER:
        @pl.when(me == owner)
        def _():
            wait_parts("o", big.at[1, :, pl.ds(0, 1024)], ret_send.at[1])

    @pl.loop(0, count)
    def _(t):
        @pl.when(base + t < N_DOWN)
        def _():
            wait_parts("d", ebuf.at[t], ret_send.at[2 + t])

        @pl.when(base + t >= N_DOWN)
        def _():
            wait_parts("u", ebuf.at[t], ret_send.at[2 + t])


OUT_SPACE = pltpu.VMEM


def store_kernel(*refs):
    copies = [pltpu.make_async_copy(refs[k], refs[8 + k], refs[16].at[k]) for k in range(8)]
    for copy in copies:
        copy.start()
    for copy in copies:
        copy.wait()


def solution(mesh):
    row_spec = P("stage", "data", None)

    def local_step(*args):
        shapes = [args[k].shape for k in (0, 3, 6, 9) for _ in range(2)]
        any_space = pl.BlockSpec(memory_space=pl.ANY)
        kept = pl.pallas_call(
            kernel,
            out_shape=[OUT_SPACE(shape, F32) for shape in shapes],
            in_specs=[any_space] * 12,
            out_specs=[pl.BlockSpec(memory_space=OUT_SPACE)] * 8,
            scratch_shapes=[
                pltpu.VMEM((2, 1024, 2048), BF16),
                pltpu.VMEM((MAX_EXPERTS + 2, 512, 1024), BF16),
                pltpu.VMEM((1024, 1024), BF16),
                pltpu.VMEM((1024, 1024), BF16),
                pltpu.VMEM((3, 128, 2048), BF16),
                pltpu.VMEM((3, 128, 1024), BF16),
                pltpu.VMEM((12, 64, 1024), BF16),
                pltpu.VMEM((12, 512, 128), BF16),
                pltpu.VMEM((3, 128, 2048), BF16),
                pltpu.VMEM((3, 128, 1024), BF16),
                pltpu.VMEM((12, 64, 1024), BF16),
                pltpu.VMEM((12, 128, 512), BF16),
                pltpu.VMEM((12, 512, 128), BF16),
                pltpu.VMEM((3, 8, 128), F32),
                pltpu.VMEM((3, GROUP, 8, 128), F32),
                pltpu.VMEM((3, 8, 128), F32),
                pltpu.SemaphoreType.DMA((6,)),
                pltpu.SemaphoreType.DMA((6,)),
                pltpu.SemaphoreType.DMA((4,)),
                pltpu.SemaphoreType.DMA((3,)),
                pltpu.SemaphoreType.DMA((3,)),
                pltpu.SemaphoreType.DMA((30,)),
                pltpu.SemaphoreType.DMA((30,)),
                pltpu.SemaphoreType.DMA((2 + MAX_EXPERTS,)),
                pltpu.SemaphoreType.DMA((30,)),
            ],
            compiler_params=pltpu.CompilerParams(
                collective_id=0, has_side_effects=True, vmem_limit_bytes=VMEM_LIMIT),
        )(*args)
        return tuple(pl.pallas_call(
            store_kernel,
            out_shape=[jax.ShapeDtypeStruct(shape, F32) for shape in shapes],
            in_specs=[any_space] * 8,
            out_specs=[any_space] * 8,
            scratch_shapes=[pltpu.SemaphoreType.DMA((8,))],
            compiler_params=pltpu.CompilerParams(vmem_limit_bytes=1024 * 1024),
        )(*kept))

    return jax.shard_map(local_step, mesh=mesh, in_specs=(row_spec,) * 12, out_specs=(row_spec,) * 8, check_vma=False)
```

```python
import math
import jax
import jax.numpy as jnp
from jax import lax
from jax.experimental import pallas as pl
from jax.experimental.pallas import tpu as pltpu
from jax.sharding import PartitionSpec as P

NS_STEPS = 5
COEF_A = 3.4445
COEF_B = -4.7750
COEF_C = 2.0315
MOMENTUM = 0.95
LEARN_RATE = 0.04
DECAY = 0.2
NORM_EPS = 1e-7
RMS_MATCH = 0.2

GROUP = 8
MESH = pl.DeviceIdType.MESH
NT = (((1,), (1,)), ((), ()))
F32 = jnp.float32
BF16 = jnp.bfloat16

QKV_OWNER = (2, 1, 5)
OUT_OWNER = (3, 4, 7)
EXPERT_COUNT = (2, 0, 4, 5, 8, 1, 4, 0)
EXPERT_BASE = tuple(sum(EXPERT_COUNT[:d]) for d in range(GROUP))
EXPERT_OWNER = tuple(d for d in range(GROUP) for _ in range(EXPERT_COUNT[d]))
N_DOWN = 12
MAX_EXPERTS = 8
VMEM_LIMIT = 40 * 1024 * 1024


def send_order():
    halves = ([], [])
    sizes = {"q": 4, "o": 2, "e": 1}
    for kind, owners in (("o", OUT_OWNER), ("q", QKV_OWNER)):
        for index, owner in enumerate(owners):
            halves[owner // 4].append((kind, index))
    for half in range(2):
        devices = [d for d in range(4 * half, 4 * half + 4) if EXPERT_COUNT[d]]
        slots = []
        for d in devices:
            for t in range(EXPERT_COUNT[d]):
                slots.append(((t + 0.5) / EXPERT_COUNT[d] + (d in QKV_OWNER), d, t))
        for _, d, t in sorted(slots):
            halves[half].append(("e", EXPERT_BASE[d] + t))
    order, sent, place = [], [0, 0], [0, 0]
    while place[0] < len(halves[0]) or place[1] < len(halves[1]):
        half = 0 if sent[0] <= sent[1] else 1
        if place[half] == len(halves[half]):
            half = 1 - half
        item = halves[half][place[half]]
        place[half] += 1
        sent[half] += sizes[item[0]]
        order.append(item)
    return order


ORDER = send_order()


def pick(table, me):
    total = jnp.int32(0)
    for d, value in enumerate(table):
        if value:
            total = total + jnp.where(me == d, jnp.int32(value), jnp.int32(0))
    return total


def ns_step(src, dst, gram, poly, m, block):
    def rows_of(i):
        return pl.ds(pl.multiple_of(i * block, block), block)

    @pl.loop(0, m // block)
    def _(i):
        rows = rows_of(i)
        gram[rows, :] = lax.dot_general(src[rows, :], src[...], NT, preferred_element_type=F32).astype(BF16)

    @pl.loop(0, m // block)
    def _(i):
        rows = rows_of(i)
        part = gram[rows, :]
        square = jnp.dot(part, gram[...], preferred_element_type=F32)
        poly[rows, :] = (COEF_B * part.astype(F32) + COEF_C * square).astype(BF16)

    @pl.loop(0, m // block)
    def _(i):
        rows = rows_of(i)
        product = jnp.dot(poly[rows, :], src[...], preferred_element_type=F32)
        dst[rows, :] = (COEF_A * src[rows, :].astype(F32) + product).astype(BF16)


STACKS = {"q": (3, 128, 2048, 32, 0), "o": (3, 128, 1024, 64, 0), "d": (12, 64, 1024, 64, 0), "u": (12, 128, 512, 128, 12)}
SCALE = {"q": RMS_MATCH * math.sqrt(2048), "o": RMS_MATCH * math.sqrt(1024),
         "d": RMS_MATCH * math.sqrt(1024), "u": RMS_MATCH * math.sqrt(1024)}
SEM_BASE = {"q": 0, "o": 3, "d": 6, "u": 18}


def place_of(kind, index):
    if kind == "q":
        return "q", index, QKV_OWNER[index], 0
    if kind == "o":
        return "o", index, OUT_OWNER[index], 0
    owner = EXPERT_OWNER[index]
    slot = index - EXPERT_BASE[owner]
    return ("d", index, owner, slot) if index < N_DOWN else ("u", index - N_DOWN, owner, slot)


def return_order():
    keys = []
    for kind, index in ORDER:
        stack, position, owner, slot = place_of(kind, index)
        held = 4 * (owner in QKV_OWNER) + 2 * (owner in OUT_OWNER)
        keys.append((held + (slot + 1 if kind == "e" else 0), len(keys), stack, position))
    return [(stack, position) for _, _, stack, position in sorted(keys)]


RETURNS = return_order()


def kernel(w_q, m_q, g_q, w_o, m_o, g_o, w_u, m_u, g_u, w_d, m_d, g_d,
           nw_q, nm_q, nw_o, nm_o, nw_u, nm_u, nw_d, nm_d,
           big, ebuf, gram, poly, xs_q, xs_o, xs_d, xs_u, bk_q, bk_o, bk_d, gs_u, bk_u,
           part, gath, den,
           m_sem, g_sem, w_sem, norm_send, norm_recv, fwd_send, fwd_recv, ret_send, ret_recv):
    me = lax.axis_index("data")
    weights = {"q": w_q, "o": w_o, "d": w_d, "u": w_u}
    momenta = {"q": m_q, "o": m_o, "d": m_d, "u": m_u}
    gradients = {"q": g_q, "o": g_o, "d": g_d, "u": g_u}
    new_w = {"q": nw_q, "o": nw_o, "d": nw_d, "u": nw_u}
    new_m = {"q": nm_q, "o": nm_o, "d": nm_d, "u": nm_u}
    grad_in = {"q": bk_q, "o": bk_o, "d": bk_d, "u": gs_u}
    scaled = {"q": xs_q, "o": xs_o, "d": xs_d, "u": xs_u}
    back = {"q": bk_q, "o": bk_o, "d": bk_d, "u": bk_u}

    loads = {"q": [("q", i) for i in range(3)], "o": [("o", None)], "d": [("d", None)], "u": [("u", None)]}
    load_sem = {("q", 0): 0, ("q", 1): 1, ("q", 2): 2, ("o", None): 3, ("d", None): 4, ("u", None): 5}

    def part_of(ref, i):
        return ref if i is None else ref.at[i]

    def load_copies(key):
        stack, i = key
        sem = load_sem[key]
        return (pltpu.make_async_copy(part_of(momenta[stack], i), part_of(new_m[stack], i), m_sem.at[sem]),
                pltpu.make_async_copy(part_of(gradients[stack], i), part_of(grad_in[stack], i), g_sem.at[sem]))

    def weight_copy(stack, number):
        return pltpu.make_async_copy(weights[stack], new_w[stack], w_sem.at[number])

    for key in loads["o"]:
        for copy in load_copies(key):
            copy.start()

    barrier = pltpu.get_barrier_semaphore()
    for k in range(1, GROUP):
        pl.semaphore_signal(barrier, inc=1, device_id={"data": lax.rem(me + k, GROUP)}, device_id_type=MESH)

    part[...] = jnp.zeros_like(part)
    lane = lax.broadcasted_iota(jnp.int32, (8, 128), 1)

    def momentum_rows(stack, i, number, column):
        _, rows, cols, chunk, _ = STACKS[stack]
        lanes = jnp.zeros((1, 128), F32)
        for r in range(0, rows, chunk):
            at = pl.ds(r, chunk)
            mom = MOMENTUM * new_m[stack][i, at, :] + grad_in[stack][i, at, :].astype(F32)
            new_m[stack][i, at, :] = mom
            square = jnp.sum(mom * mom, axis=0, keepdims=True)
            for c in range(0, cols, 128):
                lanes = lanes + square[:, c:c + 128]
        total = jnp.sum(lanes, axis=1, keepdims=True)
        part[number] = jnp.where(lane == column, jnp.broadcast_to(total, (8, 128)), part[number])

    def push_norms(number):
        gath[number, me] = part[number]
        for k in range(1, GROUP):
            pltpu.make_async_remote_copy(
                src_ref=part.at[number], dst_ref=gath.at[number, me], send_sem=norm_send.at[number],
                recv_sem=norm_recv.at[number], device_id={"data": lax.rem(me + k, GROUP)}, device_id_type=MESH).start()

    def read_norms(number):
        seven = gath.at[number, pl.ds(0, GROUP - 1)]
        pltpu.make_async_copy(seven, seven, norm_recv.at[number]).wait()
        total = gath[number, 0]
        for d in range(1, GROUP):
            total = total + gath[number, d]
        den[number] = jnp.sqrt(total) + NORM_EPS

    def scale_rows(stack, i, number, column):
        _, rows, cols, chunk, _ = STACKS[stack]
        divisor = jnp.sum(jnp.where(lane[:1] == column, den[number, 0:1, :], 0.0), axis=1, keepdims=True)
        for r in range(0, rows, chunk):
            at = pl.ds(r, chunk)
            x = new_m[stack][i, at, :] / jnp.broadcast_to(divisor, (chunk, cols))
            if stack == "u":
                scaled[stack][i] = x.T.astype(BF16)
            else:
                scaled[stack][i, at, :] = x.astype(BF16)

    def block_of(stack, slot_ref, d):
        if stack == "u":
            return slot_ref.at[:, pl.ds(d * 128, 128)]
        rows = STACKS[stack][1]
        return slot_ref.at[pl.ds(d * rows, rows), :]

    def slot_of(stack, slot):
        if stack == "q":
            return big.at[0]
        if stack == "o":
            return big.at[0, :, pl.ds(0, 1024)]
        return ebuf.at[slot]

    def send_rows(stack, i, owner, slot):
        sem = SEM_BASE[stack] + i
        target = block_of(stack, slot_of(stack, slot), me)

        @pl.when(me != owner)
        def _():
            pltpu.make_async_remote_copy(
                src_ref=scaled[stack].at[i], dst_ref=target, send_sem=fwd_send.at[sem], recv_sem=fwd_recv.at[sem],
                device_id={"data": owner}, device_id_type=MESH).start()

        @pl.when(me == owner)
        def _():
            if stack == "u":
                for d in range(GROUP):
                    @pl.when(me == d)
                    def _():
                        ebuf[slot, :, d * 128:(d + 1) * 128] = scaled[stack][i]
            else:
                target[...] = scaled[stack][i]

    def momentum_stack(stack, number):
        for copy in load_copies((stack, None)):
            copy.wait()
        momentum_loop(stack, number)

    def momentum_loop(stack, number):
        @pl.loop(0, STACKS[stack][0])
        def _(i):
            momentum_rows(stack, i, number, STACKS[stack][4] + i)

    places = [place_of(kind, index) for kind, index in ORDER]

    def scale_and_send(stack, number):
        for kind, i, owner, slot in places:
            if kind == stack:
                scale_rows(stack, i, number, i)
                send_rows(stack, i, owner, slot)

    for copy in load_copies(("o", None)):
        copy.wait()
    for key in loads["q"] + loads["d"] + loads["u"]:
        for copy in load_copies(key):
            copy.start()
    momentum_loop("o", 0)
    pl.semaphore_wait(barrier, GROUP - 1)
    push_norms(0)
    for i in range(3):
        for copy in load_copies(("q", i)):
            copy.wait()
        momentum_rows("q", i, 1, i)
    push_norms(1)
    read_norms(0)
    scale_and_send("o", 0)
    momentum_stack("d", 2)
    momentum_stack("u", 2)
    push_norms(2)
    read_norms(1)
    scale_and_send("q", 1)
    for number, stack in enumerate(("q", "o", "d", "u")):
        weight_copy(stack, number).start()
    read_norms(2)
    for stack in ("d", "u"):
        @pl.loop(0, STACKS[stack][0])
        def _(i):
            scale_rows(stack, i, 2, STACKS[stack][4] + i)
    for stack, i, owner, slot in places:
        if stack in "du":
            send_rows(stack, i, owner, slot)

    def wait_parts(stack, slot_ref, sem):
        rows = 7 * STACKS[stack][1]
        part = slot_ref.at[:, pl.ds(0, rows)] if stack == "u" else slot_ref.at[pl.ds(0, rows), :]
        pltpu.make_async_copy(part, part, sem).wait()

    def give_back(stack, slot_ref, i, send_sem, recv_sem):
        half = me // 4
        crossing = [(1 - half) * 4 + k for k in range(4)]
        for dst in crossing + [half * 4 + lax.rem(me + k, 4) for k in range(1, 4)]:
            pltpu.make_async_remote_copy(
                src_ref=block_of(stack, slot_ref, dst), dst_ref=back[stack].at[i], send_sem=send_sem, recv_sem=recv_sem,
                device_id={"data": dst}, device_id_type=MESH).start()

    def new_weight(w, x, stack):
        return w - LEARN_RATE * (SCALE[stack] * x.astype(F32) + DECAY * w)

    def finish(stack, i, source):
        _, rows, cols, chunk, _ = STACKS[stack]
        for r in range(0, rows, chunk):
            at = pl.ds(r, chunk)
            x = source(at)
            if stack == "u":
                x = x.astype(F32).T
            new_w[stack][i, at, :] = new_weight(new_w[stack][i, at, :], x, stack)

    for index, owner in enumerate(QKV_OWNER):
        @pl.when(me == owner)
        def _():
            wait_parts("q", big.at[0], fwd_recv.at[index])

    @pl.when((me == QKV_OWNER[0]) | (me == QKV_OWNER[1]) | (me == QKV_OWNER[2]))
    def _():
        @pl.loop(0, NS_STEPS)
        def _(it):
            now = lax.rem(it, 2)
            ns_step(big.at[now], big.at[1 - now], gram, poly, 1024, 256)

    for index, owner in enumerate(QKV_OWNER):
        @pl.when(me == owner)
        def _():
            give_back("q", big.at[1], index, ret_send.at[0], ret_recv.at[index])
            back["q"][index] = big[1, pl.ds(owner * 128, 128), :]

    for index, owner in enumerate(OUT_OWNER):
        @pl.when(me == owner)
        def _():
            wait_parts("o", big.at[0, :, pl.ds(0, 1024)], fwd_recv.at[3 + index])

    @pl.when((me == OUT_OWNER[0]) | (me == OUT_OWNER[1]) | (me == OUT_OWNER[2]))
    def _():
        @pl.loop(0, NS_STEPS)
        def _(it):
            now = lax.rem(it, 2)
            ns_step(big.at[now, :, pl.ds(0, 1024)], big.at[1 - now, :, pl.ds(0, 1024)], gram, poly, 1024, 256)

    for index, owner in enumerate(OUT_OWNER):
        @pl.when(me == owner)
        def _():
            give_back("o", big.at[1, :, pl.ds(0, 1024)], index, ret_send.at[1], ret_recv.at[3 + index])
            back["o"][index] = big[1, pl.ds(owner * 128, 128), 0:1024]

    base, count = pick(EXPERT_BASE, me), pick(EXPERT_COUNT, me)
    small_gram, small_poly = gram.at[pl.ds(0, 512), pl.ds(0, 512)], poly.at[pl.ds(0, 512), pl.ds(0, 512)]

    @pl.loop(0, count)
    def _(t):
        rank = base + t

        @pl.when(rank < N_DOWN)
        def _():
            wait_parts("d", ebuf.at[t], fwd_recv.at[6 + rank])

        @pl.when(rank >= N_DOWN)
        def _():
            wait_parts("u", ebuf.at[t], fwd_recv.at[6 + rank])

        @pl.loop(0, NS_STEPS)
        def _(it):
            src = jnp.where(it == 0, t, MAX_EXPERTS + lax.rem(it + 1, 2))
            dst = jnp.where(it == NS_STEPS - 1, t, MAX_EXPERTS + lax.rem(it, 2))
            ns_step(ebuf.at[src], ebuf.at[dst], small_gram, small_poly, 512, 256)

        @pl.when(rank < N_DOWN)
        def _():
            give_back("d", ebuf.at[t], rank, ret_send.at[2 + t], ret_recv.at[6 + rank])
            back["d"][rank] = ebuf[t, pl.ds(pl.multiple_of(me * 64, 64), 64), :]

        @pl.when(rank >= N_DOWN)
        def _():
            give_back("u", ebuf.at[t], rank - N_DOWN, ret_send.at[2 + t], ret_recv.at[6 + rank])
            for d in range(GROUP):
                if EXPERT_BASE[d] + EXPERT_COUNT[d] > N_DOWN and EXPERT_COUNT[d]:
                    @pl.when(me == d)
                    def _():
                        back["u"][rank - N_DOWN] = ebuf[t, :, d * 128:(d + 1) * 128]

    for number, stack in enumerate(("q", "o", "d", "u")):
        weight_copy(stack, number).wait()
    owners = {(stack, i): owner for stack, i, owner, _ in places}
    for stack, i in RETURNS:
        owner, sem = owners[stack, i], SEM_BASE[stack] + i

        @pl.when(me != owner)
        def _():
            row = back[stack].at[i]
            pltpu.make_async_copy(row, row, ret_recv.at[sem]).wait()

        if stack == "u":
            finish(stack, i, lambda at: back["u"][i])
        else:
            finish(stack, i, lambda at: back[stack][i, at, :])

    for number in range(3):
        seven = gath.at[number, pl.ds(0, GROUP - 1)]
        pltpu.make_async_copy(seven, seven, norm_send.at[number]).wait()
    for stack, i, owner, slot in places:
        @pl.when(me != owner)
        def _():
            block = scaled[stack].at[i]
            pltpu.make_async_copy(block, block, fwd_send.at[SEM_BASE[stack] + i]).wait()
    for owner in QKV_OWNER:
        @pl.when(me == owner)
        def _():
            wait_parts("q", big.at[1], ret_send.at[0])
    for owner in OUT_OWNER:
        @pl.when(me == owner)
        def _():
            wait_parts("o", big.at[1, :, pl.ds(0, 1024)], ret_send.at[1])

    @pl.loop(0, count)
    def _(t):
        @pl.when(base + t < N_DOWN)
        def _():
            wait_parts("d", ebuf.at[t], ret_send.at[2 + t])

        @pl.when(base + t >= N_DOWN)
        def _():
            wait_parts("u", ebuf.at[t], ret_send.at[2 + t])


OUT_SPACE = pltpu.VMEM


def store_kernel(*refs):
    copies = [pltpu.make_async_copy(refs[k], refs[8 + k], refs[16].at[k]) for k in range(8)]
    for copy in copies:
        copy.start()
    for copy in copies:
        copy.wait()


def solution(mesh):
    row_spec = P("stage", "data", None)

    def local_step(*args):
        shapes = [args[k].shape for k in (0, 3, 6, 9) for _ in range(2)]
        any_space = pl.BlockSpec(memory_space=pl.ANY)
        kept = pl.pallas_call(
            kernel,
            out_shape=[OUT_SPACE(shape, F32) for shape in shapes],
            in_specs=[any_space] * 12,
            out_specs=[pl.BlockSpec(memory_space=OUT_SPACE)] * 8,
            scratch_shapes=[
                pltpu.VMEM((2, 1024, 2048), BF16),
                pltpu.VMEM((MAX_EXPERTS + 2, 512, 1024), BF16),
                pltpu.VMEM((1024, 1024), BF16),
                pltpu.VMEM((1024, 1024), BF16),
                pltpu.VMEM((3, 128, 2048), BF16),
                pltpu.VMEM((3, 128, 1024), BF16),
                pltpu.VMEM((12, 64, 1024), BF16),
                pltpu.VMEM((12, 512, 128), BF16),
                pltpu.VMEM((3, 128, 2048), BF16),
                pltpu.VMEM((3, 128, 1024), BF16),
                pltpu.VMEM((12, 64, 1024), BF16),
                pltpu.VMEM((12, 128, 512), BF16),
                pltpu.VMEM((12, 512, 128), BF16),
                pltpu.VMEM((3, 8, 128), F32),
                pltpu.VMEM((3, GROUP, 8, 128), F32),
                pltpu.VMEM((3, 8, 128), F32),
                pltpu.SemaphoreType.DMA((6,)),
                pltpu.SemaphoreType.DMA((6,)),
                pltpu.SemaphoreType.DMA((4,)),
                pltpu.SemaphoreType.DMA((3,)),
                pltpu.SemaphoreType.DMA((3,)),
                pltpu.SemaphoreType.DMA((30,)),
                pltpu.SemaphoreType.DMA((30,)),
                pltpu.SemaphoreType.DMA((2 + MAX_EXPERTS,)),
                pltpu.SemaphoreType.DMA((30,)),
            ],
            compiler_params=pltpu.CompilerParams(
                collective_id=0, has_side_effects=True, vmem_limit_bytes=VMEM_LIMIT),
        )(*args)
        return tuple(pl.pallas_call(
            store_kernel,
            out_shape=[jax.ShapeDtypeStruct(shape, F32) for shape in shapes],
            in_specs=[any_space] * 8,
            out_specs=[any_space] * 8,
            scratch_shapes=[pltpu.SemaphoreType.DMA((8,))],
            compiler_params=pltpu.CompilerParams(vmem_limit_bytes=1024 * 1024),
        )(*kept))

    return jax.shard_map(local_step, mesh=mesh, in_specs=(row_spec,) * 12, out_specs=(row_spec,) * 8, check_vma=False)
```

```python
import math
import jax
import jax.numpy as jnp
from jax import lax
from jax.experimental import pallas as pl
from jax.experimental.pallas import tpu as pltpu
from jax.sharding import PartitionSpec as P

NS_STEPS = 5
COEF_A = 3.4445
COEF_B = -4.7750
COEF_C = 2.0315
MOMENTUM = 0.95
LEARN_RATE = 0.04
DECAY = 0.2
NORM_EPS = 1e-7
RMS_MATCH = 0.2

GROUP = 8
MESH = pl.DeviceIdType.MESH
NT = (((1,), (1,)), ((), ()))
F32 = jnp.float32
BF16 = jnp.bfloat16

QKV_OWNER = (2, 1, 5)
OUT_OWNER = (3, 4, 7)
EXPERT_COUNT = (2, 0, 4, 5, 8, 1, 4, 0)
EXPERT_BASE = tuple(sum(EXPERT_COUNT[:d]) for d in range(GROUP))
EXPERT_OWNER = tuple(d for d in range(GROUP) for _ in range(EXPERT_COUNT[d]))
N_DOWN = 12
MAX_EXPERTS = 8
VMEM_LIMIT = 40 * 1024 * 1024


def send_order():
    halves = ([], [])
    sizes = {"q": 4, "o": 2, "e": 1}
    for kind, owners in (("o", OUT_OWNER), ("q", QKV_OWNER)):
        for index, owner in enumerate(owners):
            halves[owner // 4].append((kind, index))
    for half in range(2):
        devices = [d for d in range(4 * half, 4 * half + 4) if EXPERT_COUNT[d]]
        slots = []
        for d in devices:
            for t in range(EXPERT_COUNT[d]):
                slots.append(((t + 0.5) / EXPERT_COUNT[d] + (d in QKV_OWNER), d, t))
        for _, d, t in sorted(slots):
            halves[half].append(("e", EXPERT_BASE[d] + t))
    order, sent, place = [], [0, 0], [0, 0]
    while place[0] < len(halves[0]) or place[1] < len(halves[1]):
        half = 0 if sent[0] <= sent[1] else 1
        if place[half] == len(halves[half]):
            half = 1 - half
        item = halves[half][place[half]]
        place[half] += 1
        sent[half] += sizes[item[0]]
        order.append(item)
    return order


ORDER = send_order()


def pick(table, me):
    total = jnp.int32(0)
    for d, value in enumerate(table):
        if value:
            total = total + jnp.where(me == d, jnp.int32(value), jnp.int32(0))
    return total


def ns_step(src, dst, gram, poly, m, block):
    def rows_of(i):
        return pl.ds(pl.multiple_of(i * block, block), block)

    @pl.loop(0, m // block)
    def _(i):
        rows = rows_of(i)
        gram[rows, :] = lax.dot_general(src[rows, :], src[...], NT, preferred_element_type=F32).astype(BF16)

    @pl.loop(0, m // block)
    def _(i):
        rows = rows_of(i)
        part = gram[rows, :]
        square = jnp.dot(part, gram[...], preferred_element_type=F32)
        poly[rows, :] = (COEF_B * part.astype(F32) + COEF_C * square).astype(BF16)

    @pl.loop(0, m // block)
    def _(i):
        rows = rows_of(i)
        product = jnp.dot(poly[rows, :], src[...], preferred_element_type=F32)
        dst[rows, :] = (COEF_A * src[rows, :].astype(F32) + product).astype(BF16)


STACKS = {"q": (3, 128, 2048, 32, 0), "o": (3, 128, 1024, 64, 0), "d": (12, 64, 1024, 64, 0), "u": (12, 128, 512, 128, 12)}
SCALE = {"q": RMS_MATCH * math.sqrt(2048), "o": RMS_MATCH * math.sqrt(1024),
         "d": RMS_MATCH * math.sqrt(1024), "u": RMS_MATCH * math.sqrt(1024)}
EARLY = {("o", 0): 32, ("o", 1): 32}
EARLY_ROWS = 32
SEM_BASE = {"q": 0, "o": 3, "d": 6, "u": 18}


def place_of(kind, index):
    if kind == "q":
        return "q", index, QKV_OWNER[index], 0
    if kind == "o":
        return "o", index, OUT_OWNER[index], 0
    owner = EXPERT_OWNER[index]
    slot = index - EXPERT_BASE[owner]
    return ("d", index, owner, slot) if index < N_DOWN else ("u", index - N_DOWN, owner, slot)


def return_order():
    keys = []
    for kind, index in ORDER:
        stack, position, owner, slot = place_of(kind, index)
        held = 4 * (owner in QKV_OWNER) + 2 * (owner in OUT_OWNER)
        keys.append((held + (slot + 1 if kind == "e" else 0), len(keys), stack, position))
    return [(stack, position) for _, _, stack, position in sorted(keys)]


RETURNS = return_order()


def kernel(w_q, m_q, g_q, w_o, m_o, g_o, w_u, m_u, g_u, w_d, m_d, g_d,
           nw_q, nm_q, nw_o, nm_o, nw_u, nm_u, nw_d, nm_d,
           big, ebuf, gram, poly, xs_q, xs_o, xs_d, xs_u, bk_q, bk_o, bk_d, gs_u, bk_u,
           part, gath, den, early,
           m_sem, g_sem, w_sem, norm_send, norm_recv, fwd_send, fwd_recv, ret_send, ret_recv, early_send, early_recv):
    me = lax.axis_index("data")
    weights = {"q": w_q, "o": w_o, "d": w_d, "u": w_u}
    momenta = {"q": m_q, "o": m_o, "d": m_d, "u": m_u}
    gradients = {"q": g_q, "o": g_o, "d": g_d, "u": g_u}
    new_w = {"q": nw_q, "o": nw_o, "d": nw_d, "u": nw_u}
    new_m = {"q": nm_q, "o": nm_o, "d": nm_d, "u": nm_u}
    grad_in = {"q": bk_q, "o": bk_o, "d": bk_d, "u": gs_u}
    scaled = {"q": xs_q, "o": xs_o, "d": xs_d, "u": xs_u}
    back = {"q": bk_q, "o": bk_o, "d": bk_d, "u": bk_u}

    loads = {"q": [("q", i) for i in range(3)], "o": [("o", None)], "d": [("d", None)], "u": [("u", None)]}
    load_sem = {("q", 0): 0, ("q", 1): 1, ("q", 2): 2, ("o", None): 3, ("d", None): 4, ("u", None): 5}

    def part_of(ref, i):
        return ref if i is None else ref.at[i]

    def load_copies(key):
        stack, i = key
        sem = load_sem[key]
        return (pltpu.make_async_copy(part_of(momenta[stack], i), part_of(new_m[stack], i), m_sem.at[sem]),
                pltpu.make_async_copy(part_of(gradients[stack], i), part_of(grad_in[stack], i), g_sem.at[sem]))

    def weight_copy(stack, number):
        return pltpu.make_async_copy(weights[stack], new_w[stack], w_sem.at[number])

    for key in loads["o"]:
        for copy in load_copies(key):
            copy.start()

    barrier = pltpu.get_barrier_semaphore()
    for k in range(1, GROUP):
        pl.semaphore_signal(barrier, inc=1, device_id={"data": lax.rem(me + k, GROUP)}, device_id_type=MESH)

    part[...] = jnp.zeros_like(part)
    lane = lax.broadcasted_iota(jnp.int32, (8, 128), 1)

    def momentum_rows(stack, i, number, column):
        _, rows, cols, chunk, _ = STACKS[stack]
        lanes = jnp.zeros((1, 128), F32)
        for r in range(0, rows, chunk):
            at = pl.ds(r, chunk)
            mom = MOMENTUM * new_m[stack][i, at, :] + grad_in[stack][i, at, :].astype(F32)
            new_m[stack][i, at, :] = mom
            square = jnp.sum(mom * mom, axis=0, keepdims=True)
            for c in range(0, cols, 128):
                lanes = lanes + square[:, c:c + 128]
        total = jnp.sum(lanes, axis=1, keepdims=True)
        part[number] = jnp.where(lane == column, jnp.broadcast_to(total, (8, 128)), part[number])

    def push_norms(number):
        gath[number, me] = part[number]
        for k in range(1, GROUP):
            pltpu.make_async_remote_copy(
                src_ref=part.at[number], dst_ref=gath.at[number, me], send_sem=norm_send.at[number],
                recv_sem=norm_recv.at[number], device_id={"data": lax.rem(me + k, GROUP)}, device_id_type=MESH).start()

    def read_norms(number):
        seven = gath.at[number, pl.ds(0, GROUP - 1)]
        pltpu.make_async_copy(seven, seven, norm_recv.at[number]).wait()
        total = gath[number, 0]
        for d in range(1, GROUP):
            total = total + gath[number, d]
        den[number] = jnp.sqrt(total) + NORM_EPS

    def scale_rows(stack, i, number, column):
        _, rows, cols, chunk, _ = STACKS[stack]
        divisor = jnp.sum(jnp.where(lane[:1] == column, den[number, 0:1, :], 0.0), axis=1, keepdims=True)
        for r in range(0, rows, chunk):
            at = pl.ds(r, chunk)
            x = new_m[stack][i, at, :] / jnp.broadcast_to(divisor, (chunk, cols))
            if stack == "u":
                scaled[stack][i] = x.T.astype(BF16)
            else:
                scaled[stack][i, at, :] = x.astype(BF16)

    def block_of(stack, slot_ref, d):
        if stack == "u":
            return slot_ref.at[:, pl.ds(d * 128, 128)]
        rows = STACKS[stack][1]
        return slot_ref.at[pl.ds(d * rows, rows), :]

    def slot_of(stack, slot):
        if stack == "q":
            return big.at[0]
        if stack == "o":
            return big.at[0, :, pl.ds(0, 1024)]
        return ebuf.at[slot]

    def send_rows(stack, i, owner, slot):
        sem = SEM_BASE[stack] + i
        target = block_of(stack, slot_of(stack, slot), me)
        skip = EARLY.get((stack, i), 0)
        source, rest = scaled[stack].at[i], target
        if skip:
            source = scaled[stack].at[i, pl.ds(skip, 128 - skip), :]
            rest = slot_of(stack, slot).at[pl.ds(me * 128 + skip, 128 - skip), :]

        @pl.when(me != owner)
        def _():
            pltpu.make_async_remote_copy(
                src_ref=source, dst_ref=rest, send_sem=fwd_send.at[sem], recv_sem=fwd_recv.at[sem],
                device_id={"data": owner}, device_id_type=MESH).start()

        @pl.when(me == owner)
        def _():
            if stack == "u":
                for d in range(GROUP):
                    @pl.when(me == d)
                    def _():
                        ebuf[slot, :, d * 128:(d + 1) * 128] = scaled[stack][i]
            else:
                target[...] = scaled[stack][i]

    def momentum_stack(stack, number):
        for copy in load_copies((stack, None)):
            copy.wait()
        momentum_loop(stack, number)

    def momentum_loop(stack, number):
        @pl.loop(0, STACKS[stack][0])
        def _(i):
            momentum_rows(stack, i, number, STACKS[stack][4] + i)

    places = [place_of(kind, index) for kind, index in ORDER]

    def scale_and_send(stack, number):
        for kind, i, owner, slot in places:
            if kind == stack:
                scale_rows(stack, i, number, i)
                send_rows(stack, i, owner, slot)

    def early_copy(i):
        return pltpu.make_async_remote_copy(
            src_ref=new_m["o"].at[i, pl.ds(0, EARLY_ROWS), :], dst_ref=early.at[me], send_sem=early_send.at[i],
            recv_sem=early_recv.at[0], device_id={"data": OUT_OWNER[i]}, device_id_type=MESH)

    for copy in load_copies(("o", None)):
        copy.wait()
    for key in loads["q"] + loads["d"] + loads["u"]:
        for copy in load_copies(key):
            copy.start()
    momentum_loop("o", 0)
    pl.semaphore_wait(barrier, GROUP - 1)
    push_norms(0)
    for i in range(2):
        @pl.when(me != OUT_OWNER[i])
        def _():
            early_copy(i).start()
    for i in range(3):
        for copy in load_copies(("q", i)):
            copy.wait()
        momentum_rows("q", i, 1, i)
    push_norms(1)
    read_norms(0)
    scale_and_send("o", 0)
    momentum_stack("d", 2)
    momentum_stack("u", 2)
    push_norms(2)
    read_norms(1)
    scale_and_send("q", 1)
    for number, stack in enumerate(("q", "o", "d", "u")):
        weight_copy(stack, number).start()
    read_norms(2)
    for stack in ("d", "u"):
        @pl.loop(0, STACKS[stack][0])
        def _(i):
            scale_rows(stack, i, 2, STACKS[stack][4] + i)
    for stack, i, owner, slot in places:
        if stack in "du":
            send_rows(stack, i, owner, slot)

    def wait_parts(stack, slot_ref, sem):
        rows = 7 * STACKS[stack][1]
        part = slot_ref.at[:, pl.ds(0, rows)] if stack == "u" else slot_ref.at[pl.ds(0, rows), :]
        pltpu.make_async_copy(part, part, sem).wait()

    def give_back(stack, slot_ref, i, send_sem, recv_sem):
        half = me // 4
        crossing = [(1 - half) * 4 + k for k in range(4)]
        for dst in crossing + [half * 4 + lax.rem(me + k, 4) for k in range(1, 4)]:
            pltpu.make_async_remote_copy(
                src_ref=block_of(stack, slot_ref, dst), dst_ref=back[stack].at[i], send_sem=send_sem, recv_sem=recv_sem,
                device_id={"data": dst}, device_id_type=MESH).start()

    def new_weight(w, x, stack):
        return w - LEARN_RATE * (SCALE[stack] * x.astype(F32) + DECAY * w)

    def finish(stack, i, source):
        _, rows, cols, chunk, _ = STACKS[stack]
        for r in range(0, rows, chunk):
            at = pl.ds(r, chunk)
            x = source(at)
            if stack == "u":
                x = x.astype(F32).T
            new_w[stack][i, at, :] = new_weight(new_w[stack][i, at, :], x, stack)

    for index, owner in enumerate(QKV_OWNER):
        @pl.when(me == owner)
        def _():
            wait_parts("q", big.at[0], fwd_recv.at[index])

    @pl.when((me == QKV_OWNER[0]) | (me == QKV_OWNER[1]) | (me == QKV_OWNER[2]))
    def _():
        @pl.loop(0, NS_STEPS)
        def _(it):
            now = lax.rem(it, 2)
            ns_step(big.at[now], big.at[1 - now], gram, poly, 1024, 256)

    for index, owner in enumerate(QKV_OWNER):
        @pl.when(me == owner)
        def _():
            give_back("q", big.at[1], index, ret_send.at[0], ret_recv.at[index])
            back["q"][index] = big[1, pl.ds(owner * 128, 128), :]

    for index, owner in enumerate(OUT_OWNER):
        @pl.when(me == owner)
        def _():
            if ("o", index) not in EARLY:
                wait_parts("o", big.at[0, :, pl.ds(0, 1024)], fwd_recv.at[3 + index])
                return
            part_rows = big.at[0, pl.ds(0, 7 * (128 - EARLY_ROWS)), pl.ds(0, 1024)]
            pltpu.make_async_copy(part_rows, part_rows, fwd_recv.at[3 + index]).wait()
            seven = early.at[pl.ds(0, GROUP - 1)]
            pltpu.make_async_copy(seven, seven, early_recv.at[0]).wait()
            divisor = jnp.sum(jnp.where(lane[:1] == index, den[0, 0:1, :], 0.0), axis=1, keepdims=True)

            @pl.loop(0, GROUP)
            def _(d):
                @pl.when(d != me)
                def _():
                    x = early[d] / jnp.broadcast_to(divisor, (EARLY_ROWS, 1024))
                    big[0, pl.ds(pl.multiple_of(d * 128, 128), EARLY_ROWS), 0:1024] = x.astype(BF16)

    @pl.when((me == OUT_OWNER[0]) | (me == OUT_OWNER[1]) | (me == OUT_OWNER[2]))
    def _():
        @pl.loop(0, NS_STEPS)
        def _(it):
            now = lax.rem(it, 2)
            ns_step(big.at[now, :, pl.ds(0, 1024)], big.at[1 - now, :, pl.ds(0, 1024)], gram, poly, 1024, 256)

    for index, owner in enumerate(OUT_OWNER):
        @pl.when(me == owner)
        def _():
            give_back("o", big.at[1, :, pl.ds(0, 1024)], index, ret_send.at[1], ret_recv.at[3 + index])
            back["o"][index] = big[1, pl.ds(owner * 128, 128), 0:1024]

    base, count = pick(EXPERT_BASE, me), pick(EXPERT_COUNT, me)
    small_gram, small_poly = gram.at[pl.ds(0, 512), pl.ds(0, 512)], poly.at[pl.ds(0, 512), pl.ds(0, 512)]

    @pl.loop(0, count)
    def _(t):
        rank = base + t

        @pl.when(rank < N_DOWN)
        def _():
            wait_parts("d", ebuf.at[t], fwd_recv.at[6 + rank])

        @pl.when(rank >= N_DOWN)
        def _():
            wait_parts("u", ebuf.at[t], fwd_recv.at[6 + rank])

        @pl.loop(0, NS_STEPS)
        def _(it):
            src = jnp.where(it == 0, t, MAX_EXPERTS + lax.rem(it + 1, 2))
            dst = jnp.where(it == NS_STEPS - 1, t, MAX_EXPERTS + lax.rem(it, 2))
            ns_step(ebuf.at[src], ebuf.at[dst], small_gram, small_poly, 512, 256)

        @pl.when(rank < N_DOWN)
        def _():
            give_back("d", ebuf.at[t], rank, ret_send.at[2 + t], ret_recv.at[6 + rank])
            back["d"][rank] = ebuf[t, pl.ds(pl.multiple_of(me * 64, 64), 64), :]

        @pl.when(rank >= N_DOWN)
        def _():
            give_back("u", ebuf.at[t], rank - N_DOWN, ret_send.at[2 + t], ret_recv.at[6 + rank])
            for d in range(GROUP):
                if EXPERT_BASE[d] + EXPERT_COUNT[d] > N_DOWN and EXPERT_COUNT[d]:
                    @pl.when(me == d)
                    def _():
                        back["u"][rank - N_DOWN] = ebuf[t, :, d * 128:(d + 1) * 128]

    for number, stack in enumerate(("q", "o", "d", "u")):
        weight_copy(stack, number).wait()
    owners = {(stack, i): owner for stack, i, owner, _ in places}
    for stack, i in RETURNS:
        owner, sem = owners[stack, i], SEM_BASE[stack] + i

        @pl.when(me != owner)
        def _():
            row = back[stack].at[i]
            pltpu.make_async_copy(row, row, ret_recv.at[sem]).wait()

        if stack == "u":
            finish(stack, i, lambda at: back["u"][i])
        else:
            finish(stack, i, lambda at: back[stack][i, at, :])

    for number in range(3):
        seven = gath.at[number, pl.ds(0, GROUP - 1)]
        pltpu.make_async_copy(seven, seven, norm_send.at[number]).wait()
    for stack, i, owner, slot in places:
        @pl.when(me != owner)
        def _():
            block = scaled[stack].at[i]
            if (stack, i) in EARLY:
                block = scaled[stack].at[i, pl.ds(EARLY_ROWS, 128 - EARLY_ROWS), :]
                early_copy(i).wait_send()
            pltpu.make_async_copy(block, block, fwd_send.at[SEM_BASE[stack] + i]).wait()
    for owner in QKV_OWNER:
        @pl.when(me == owner)
        def _():
            wait_parts("q", big.at[1], ret_send.at[0])
    for owner in OUT_OWNER:
        @pl.when(me == owner)
        def _():
            wait_parts("o", big.at[1, :, pl.ds(0, 1024)], ret_send.at[1])

    @pl.loop(0, count)
    def _(t):
        @pl.when(base + t < N_DOWN)
        def _():
            wait_parts("d", ebuf.at[t], ret_send.at[2 + t])

        @pl.when(base + t >= N_DOWN)
        def _():
            wait_parts("u", ebuf.at[t], ret_send.at[2 + t])


OUT_SPACE = pltpu.VMEM


def store_kernel(*refs):
    copies = [pltpu.make_async_copy(refs[k], refs[8 + k], refs[16].at[k]) for k in range(8)]
    for copy in copies:
        copy.start()
    for copy in copies:
        copy.wait()


def solution(mesh):
    row_spec = P("stage", "data", None)

    def local_step(*args):
        shapes = [args[k].shape for k in (0, 3, 6, 9) for _ in range(2)]
        any_space = pl.BlockSpec(memory_space=pl.ANY)
        kept = pl.pallas_call(
            kernel,
            out_shape=[OUT_SPACE(shape, F32) for shape in shapes],
            in_specs=[any_space] * 12,
            out_specs=[pl.BlockSpec(memory_space=OUT_SPACE)] * 8,
            scratch_shapes=[
                pltpu.VMEM((2, 1024, 2048), BF16),
                pltpu.VMEM((MAX_EXPERTS + 2, 512, 1024), BF16),
                pltpu.VMEM((1024, 1024), BF16),
                pltpu.VMEM((1024, 1024), BF16),
                pltpu.VMEM((3, 128, 2048), BF16),
                pltpu.VMEM((3, 128, 1024), BF16),
                pltpu.VMEM((12, 64, 1024), BF16),
                pltpu.VMEM((12, 512, 128), BF16),
                pltpu.VMEM((3, 128, 2048), BF16),
                pltpu.VMEM((3, 128, 1024), BF16),
                pltpu.VMEM((12, 64, 1024), BF16),
                pltpu.VMEM((12, 128, 512), BF16),
                pltpu.VMEM((12, 512, 128), BF16),
                pltpu.VMEM((3, 8, 128), F32),
                pltpu.VMEM((3, GROUP, 8, 128), F32),
                pltpu.VMEM((3, 8, 128), F32),
                pltpu.VMEM((GROUP, EARLY_ROWS, 1024), F32),
                pltpu.SemaphoreType.DMA((6,)),
                pltpu.SemaphoreType.DMA((6,)),
                pltpu.SemaphoreType.DMA((4,)),
                pltpu.SemaphoreType.DMA((3,)),
                pltpu.SemaphoreType.DMA((3,)),
                pltpu.SemaphoreType.DMA((30,)),
                pltpu.SemaphoreType.DMA((30,)),
                pltpu.SemaphoreType.DMA((2 + MAX_EXPERTS,)),
                pltpu.SemaphoreType.DMA((30,)),
                pltpu.SemaphoreType.DMA((2,)),
                pltpu.SemaphoreType.DMA((1,)),
            ],
            compiler_params=pltpu.CompilerParams(
                collective_id=0, has_side_effects=True, vmem_limit_bytes=VMEM_LIMIT),
        )(*args)
        return tuple(pl.pallas_call(
            store_kernel,
            out_shape=[jax.ShapeDtypeStruct(shape, F32) for shape in shapes],
            in_specs=[any_space] * 8,
            out_specs=[any_space] * 8,
            scratch_shapes=[pltpu.SemaphoreType.DMA((8,))],
            compiler_params=pltpu.CompilerParams(vmem_limit_bytes=1024 * 1024),
        )(*kept))

    return jax.shard_map(local_step, mesh=mesh, in_specs=(row_spec,) * 12, out_specs=(row_spec,) * 8, check_vma=False)
```

```python
import math
import jax
import jax.numpy as jnp
from jax import lax
from jax.experimental import pallas as pl
from jax.experimental.pallas import tpu as pltpu
from jax.sharding import PartitionSpec as P

NS_STEPS = 5
COEF_A = 3.4445
COEF_B = -4.7750
COEF_C = 2.0315
MOMENTUM = 0.95
LEARN_RATE = 0.04
DECAY = 0.2
NORM_EPS = 1e-7
RMS_MATCH = 0.2

GROUP = 8
MESH = pl.DeviceIdType.MESH
NT = (((1,), (1,)), ((), ()))
F32 = jnp.float32
BF16 = jnp.bfloat16

QKV_OWNER = (2, 3, 4)
OUT_OWNER = (0, 5, 6)
EXPERT_COUNT = (3, 6, 1, 1, 1, 3, 3, 6)
EXPERT_BASE = tuple(sum(EXPERT_COUNT[:d]) for d in range(GROUP))
EXPERT_OWNER = tuple(d for d in range(GROUP) for _ in range(EXPERT_COUNT[d]))
N_DOWN = 12
MAX_EXPERTS = 8
VMEM_LIMIT = 40 * 1024 * 1024


def send_order():
    halves = ([], [])
    sizes = {"q": 4, "o": 2, "e": 1}
    for kind, owners in (("o", OUT_OWNER), ("q", QKV_OWNER)):
        for index, owner in enumerate(owners):
            halves[owner // 4].append((kind, index))
    for half in range(2):
        devices = [d for d in range(4 * half, 4 * half + 4) if EXPERT_COUNT[d]]
        slots = []
        for d in devices:
            for t in range(EXPERT_COUNT[d]):
                slots.append(((t + 0.5) / EXPERT_COUNT[d] + (d in QKV_OWNER), d, t))
        for _, d, t in sorted(slots):
            halves[half].append(("e", EXPERT_BASE[d] + t))
    order, sent, place = [], [0, 0], [0, 0]
    while place[0] < len(halves[0]) or place[1] < len(halves[1]):
        half = 0 if sent[0] <= sent[1] else 1
        if place[half] == len(halves[half]):
            half = 1 - half
        item = halves[half][place[half]]
        place[half] += 1
        sent[half] += sizes[item[0]]
        order.append(item)
    return order


ORDER = send_order()


def pick(table, me):
    total = jnp.int32(0)
    for d, value in enumerate(table):
        if value:
            total = total + jnp.where(me == d, jnp.int32(value), jnp.int32(0))
    return total


def ns_step(src, dst, gram, poly, m, block):
    def rows_of(i):
        return pl.ds(pl.multiple_of(i * block, block), block)

    @pl.loop(0, m // block)
    def _(i):
        rows = rows_of(i)
        gram[rows, :] = lax.dot_general(src[rows, :], src[...], NT, preferred_element_type=F32).astype(BF16)

    @pl.loop(0, m // block)
    def _(i):
        rows = rows_of(i)
        part = gram[rows, :]
        square = jnp.dot(part, gram[...], preferred_element_type=F32)
        poly[rows, :] = (COEF_B * part.astype(F32) + COEF_C * square).astype(BF16)

    @pl.loop(0, m // block)
    def _(i):
        rows = rows_of(i)
        product = jnp.dot(poly[rows, :], src[...], preferred_element_type=F32)
        dst[rows, :] = (COEF_A * src[rows, :].astype(F32) + product).astype(BF16)


STACKS = {"q": (3, 128, 2048, 32, 0), "o": (3, 128, 1024, 64, 0), "d": (12, 64, 1024, 64, 0), "u": (12, 128, 512, 128, 12)}
SCALE = {"q": RMS_MATCH * math.sqrt(2048), "o": RMS_MATCH * math.sqrt(1024),
         "d": RMS_MATCH * math.sqrt(1024), "u": RMS_MATCH * math.sqrt(1024)}
EARLY = {("o", 0): 32, ("o", 1): 32}
EARLY_ROWS = 32
SEM_BASE = {"q": 0, "o": 3, "d": 6, "u": 18}


def place_of(kind, index):
    if kind == "q":
        return "q", index, QKV_OWNER[index], 0
    if kind == "o":
        return "o", index, OUT_OWNER[index], 0
    owner = EXPERT_OWNER[index]
    slot = index - EXPERT_BASE[owner]
    return ("d", index, owner, slot) if index < N_DOWN else ("u", index - N_DOWN, owner, slot)


def return_order():
    keys = []
    for kind, index in ORDER:
        stack, position, owner, slot = place_of(kind, index)
        held = 4 * (owner in QKV_OWNER) + 2 * (owner in OUT_OWNER)
        keys.append((held + (slot + 1 if kind == "e" else 0), len(keys), stack, position))
    return [(stack, position) for _, _, stack, position in sorted(keys)]


RETURNS = return_order()


def kernel(w_q, m_q, g_q, w_o, m_o, g_o, w_u, m_u, g_u, w_d, m_d, g_d,
           nw_q, nm_q, nw_o, nm_o, nw_u, nm_u, nw_d, nm_d,
           big, ebuf, gram, poly, xs_q, xs_o, xs_d, xs_u, bk_q, bk_o, bk_d, gs_u, bk_u,
           part, gath, den, early,
           m_sem, g_sem, w_sem, norm_send, norm_recv, fwd_send, fwd_recv, ret_send, ret_recv, early_send, early_recv):
    me = lax.axis_index("data")
    weights = {"q": w_q, "o": w_o, "d": w_d, "u": w_u}
    momenta = {"q": m_q, "o": m_o, "d": m_d, "u": m_u}
    gradients = {"q": g_q, "o": g_o, "d": g_d, "u": g_u}
    new_w = {"q": nw_q, "o": nw_o, "d": nw_d, "u": nw_u}
    new_m = {"q": nm_q, "o": nm_o, "d": nm_d, "u": nm_u}
    grad_in = {"q": bk_q, "o": bk_o, "d": bk_d, "u": gs_u}
    scaled = {"q": xs_q, "o": xs_o, "d": xs_d, "u": xs_u}
    back = {"q": bk_q, "o": bk_o, "d": bk_d, "u": bk_u}

    loads = {"q": [("q", i) for i in range(3)], "o": [("o", None)], "d": [("d", None)], "u": [("u", None)]}
    load_sem = {("q", 0): 0, ("q", 1): 1, ("q", 2): 2, ("o", None): 3, ("d", None): 4, ("u", None): 5}

    def part_of(ref, i):
        return ref if i is None else ref.at[i]

    def load_copies(key):
        stack, i = key
        sem = load_sem[key]
        return (pltpu.make_async_copy(part_of(momenta[stack], i), part_of(new_m[stack], i), m_sem.at[sem]),
                pltpu.make_async_copy(part_of(gradients[stack], i), part_of(grad_in[stack], i), g_sem.at[sem]))

    def weight_copy(stack, number):
        return pltpu.make_async_copy(weights[stack], new_w[stack], w_sem.at[number])

    for key in loads["o"]:
        for copy in load_copies(key):
            copy.start()

    barrier = pltpu.get_barrier_semaphore()
    for k in range(1, GROUP):
        pl.semaphore_signal(barrier, inc=1, device_id={"data": lax.rem(me + k, GROUP)}, device_id_type=MESH)

    part[...] = jnp.zeros_like(part)
    lane = lax.broadcasted_iota(jnp.int32, (8, 128), 1)

    def momentum_rows(stack, i, number, column):
        _, rows, cols, chunk, _ = STACKS[stack]
        lanes = jnp.zeros((1, 128), F32)
        for r in range(0, rows, chunk):
            at = pl.ds(r, chunk)
            mom = MOMENTUM * new_m[stack][i, at, :] + grad_in[stack][i, at, :].astype(F32)
            new_m[stack][i, at, :] = mom
            square = jnp.sum(mom * mom, axis=0, keepdims=True)
            for c in range(0, cols, 128):
                lanes = lanes + square[:, c:c + 128]
        total = jnp.sum(lanes, axis=1, keepdims=True)
        part[number] = jnp.where(lane == column, jnp.broadcast_to(total, (8, 128)), part[number])

    def push_norms(number):
        gath[number, me] = part[number]
        for k in range(1, GROUP):
            pltpu.make_async_remote_copy(
                src_ref=part.at[number], dst_ref=gath.at[number, me], send_sem=norm_send.at[number],
                recv_sem=norm_recv.at[number], device_id={"data": lax.rem(me + k, GROUP)}, device_id_type=MESH).start()

    def read_norms(number):
        seven = gath.at[number, pl.ds(0, GROUP - 1)]
        pltpu.make_async_copy(seven, seven, norm_recv.at[number]).wait()
        total = gath[number, 0]
        for d in range(1, GROUP):
            total = total + gath[number, d]
        den[number] = jnp.sqrt(total) + NORM_EPS

    def scale_rows(stack, i, number, column):
        _, rows, cols, chunk, _ = STACKS[stack]
        divisor = jnp.sum(jnp.where(lane[:1] == column, den[number, 0:1, :], 0.0), axis=1, keepdims=True)
        for r in range(0, rows, chunk):
            at = pl.ds(r, chunk)
            x = new_m[stack][i, at, :] / jnp.broadcast_to(divisor, (chunk, cols))
            if stack == "u":
                scaled[stack][i] = x.T.astype(BF16)
            else:
                scaled[stack][i, at, :] = x.astype(BF16)

    def block_of(stack, slot_ref, d):
        if stack == "u":
            return slot_ref.at[:, pl.ds(d * 128, 128)]
        rows = STACKS[stack][1]
        return slot_ref.at[pl.ds(d * rows, rows), :]

    def slot_of(stack, slot):
        if stack == "q":
            return big.at[0]
        if stack == "o":
            return big.at[0, :, pl.ds(0, 1024)]
        return ebuf.at[slot]

    def send_rows(stack, i, owner, slot):
        sem = SEM_BASE[stack] + i
        target = block_of(stack, slot_of(stack, slot), me)
        skip = EARLY.get((stack, i), 0)
        source, rest = scaled[stack].at[i], target
        if skip:
            source = scaled[stack].at[i, pl.ds(skip, 128 - skip), :]
            rest = slot_of(stack, slot).at[pl.ds(me * 128 + skip, 128 - skip), :]

        @pl.when(me != owner)
        def _():
            pltpu.make_async_remote_copy(
                src_ref=source, dst_ref=rest, send_sem=fwd_send.at[sem], recv_sem=fwd_recv.at[sem],
                device_id={"data": owner}, device_id_type=MESH).start()

        @pl.when(me == owner)
        def _():
            if stack == "u":
                for d in range(GROUP):
                    @pl.when(me == d)
                    def _():
                        ebuf[slot, :, d * 128:(d + 1) * 128] = scaled[stack][i]
            else:
                target[...] = scaled[stack][i]

    def momentum_stack(stack, number):
        for copy in load_copies((stack, None)):
            copy.wait()
        momentum_loop(stack, number)

    def momentum_loop(stack, number):
        @pl.loop(0, STACKS[stack][0])
        def _(i):
            momentum_rows(stack, i, number, STACKS[stack][4] + i)

    places = [place_of(kind, index) for kind, index in ORDER]

    def scale_and_send(stack, number):
        for kind, i, owner, slot in places:
            if kind == stack:
                scale_rows(stack, i, number, i)
                send_rows(stack, i, owner, slot)

    def early_copy(i):
        return pltpu.make_async_remote_copy(
            src_ref=new_m["o"].at[i, pl.ds(0, EARLY_ROWS), :], dst_ref=early.at[me], send_sem=early_send.at[i],
            recv_sem=early_recv.at[0], device_id={"data": OUT_OWNER[i]}, device_id_type=MESH)

    for copy in load_copies(("o", None)):
        copy.wait()
    for key in loads["q"] + loads["d"] + loads["u"]:
        for copy in load_copies(key):
            copy.start()
    momentum_loop("o", 0)
    pl.semaphore_wait(barrier, GROUP - 1)
    push_norms(0)
    for i in range(2):
        @pl.when(me != OUT_OWNER[i])
        def _():
            early_copy(i).start()
    for i in range(3):
        for copy in load_copies(("q", i)):
            copy.wait()
        momentum_rows("q", i, 1, i)
    push_norms(1)
    read_norms(0)
    scale_and_send("o", 0)
    momentum_stack("d", 2)
    momentum_stack("u", 2)
    push_norms(2)
    read_norms(1)
    scale_and_send("q", 1)
    for number, stack in enumerate(("q", "o", "d", "u")):
        weight_copy(stack, number).start()
    read_norms(2)
    for stack in ("d", "u"):
        @pl.loop(0, STACKS[stack][0])
        def _(i):
            scale_rows(stack, i, 2, STACKS[stack][4] + i)
    for stack, i, owner, slot in places:
        if stack in "du":
            send_rows(stack, i, owner, slot)

    def wait_parts(stack, slot_ref, sem):
        rows = 7 * STACKS[stack][1]
        part = slot_ref.at[:, pl.ds(0, rows)] if stack == "u" else slot_ref.at[pl.ds(0, rows), :]
        pltpu.make_async_copy(part, part, sem).wait()

    def give_back(stack, slot_ref, i, send_sem, recv_sem):
        half = me // 4
        crossing = [(1 - half) * 4 + k for k in range(4)]
        for dst in crossing + [half * 4 + lax.rem(me + k, 4) for k in range(1, 4)]:
            pltpu.make_async_remote_copy(
                src_ref=block_of(stack, slot_ref, dst), dst_ref=back[stack].at[i], send_sem=send_sem, recv_sem=recv_sem,
                device_id={"data": dst}, device_id_type=MESH).start()

    def new_weight(w, x, stack):
        return w - LEARN_RATE * (SCALE[stack] * x.astype(F32) + DECAY * w)

    def finish(stack, i, source):
        _, rows, cols, chunk, _ = STACKS[stack]
        for r in range(0, rows, chunk):
            at = pl.ds(r, chunk)
            x = source(at)
            if stack == "u":
                x = x.astype(F32).T
            new_w[stack][i, at, :] = new_weight(new_w[stack][i, at, :], x, stack)

    for index, owner in enumerate(QKV_OWNER):
        @pl.when(me == owner)
        def _():
            wait_parts("q", big.at[0], fwd_recv.at[index])

    @pl.when((me == QKV_OWNER[0]) | (me == QKV_OWNER[1]) | (me == QKV_OWNER[2]))
    def _():
        @pl.loop(0, NS_STEPS)
        def _(it):
            now = lax.rem(it, 2)
            ns_step(big.at[now], big.at[1 - now], gram, poly, 1024, 256)

    for index, owner in enumerate(QKV_OWNER):
        @pl.when(me == owner)
        def _():
            give_back("q", big.at[1], index, ret_send.at[0], ret_recv.at[index])
            back["q"][index] = big[1, pl.ds(owner * 128, 128), :]

    for index, owner in enumerate(OUT_OWNER):
        @pl.when(me == owner)
        def _():
            if ("o", index) not in EARLY:
                wait_parts("o", big.at[0, :, pl.ds(0, 1024)], fwd_recv.at[3 + index])
                return
            part_rows = big.at[0, pl.ds(0, 7 * (128 - EARLY_ROWS)), pl.ds(0, 1024)]
            pltpu.make_async_copy(part_rows, part_rows, fwd_recv.at[3 + index]).wait()
            seven = early.at[pl.ds(0, GROUP - 1)]
            pltpu.make_async_copy(seven, seven, early_recv.at[0]).wait()
            divisor = jnp.sum(jnp.where(lane[:1] == index, den[0, 0:1, :], 0.0), axis=1, keepdims=True)

            @pl.loop(0, GROUP)
            def _(d):
                @pl.when(d != me)
                def _():
                    x = early[d] / jnp.broadcast_to(divisor, (EARLY_ROWS, 1024))
                    big[0, pl.ds(pl.multiple_of(d * 128, 128), EARLY_ROWS), 0:1024] = x.astype(BF16)

    @pl.when((me == OUT_OWNER[0]) | (me == OUT_OWNER[1]) | (me == OUT_OWNER[2]))
    def _():
        @pl.loop(0, NS_STEPS)
        def _(it):
            now = lax.rem(it, 2)
            ns_step(big.at[now, :, pl.ds(0, 1024)], big.at[1 - now, :, pl.ds(0, 1024)], gram, poly, 1024, 256)

    for index, owner in enumerate(OUT_OWNER):
        @pl.when(me == owner)
        def _():
            give_back("o", big.at[1, :, pl.ds(0, 1024)], index, ret_send.at[1], ret_recv.at[3 + index])
            back["o"][index] = big[1, pl.ds(owner * 128, 128), 0:1024]

    base, count = pick(EXPERT_BASE, me), pick(EXPERT_COUNT, me)
    small_gram, small_poly = gram.at[pl.ds(0, 512), pl.ds(0, 512)], poly.at[pl.ds(0, 512), pl.ds(0, 512)]

    @pl.loop(0, count)
    def _(t):
        rank = base + t

        @pl.when(rank < N_DOWN)
        def _():
            wait_parts("d", ebuf.at[t], fwd_recv.at[6 + rank])

        @pl.when(rank >= N_DOWN)
        def _():
            wait_parts("u", ebuf.at[t], fwd_recv.at[6 + rank])

        @pl.loop(0, NS_STEPS)
        def _(it):
            src = jnp.where(it == 0, t, MAX_EXPERTS + lax.rem(it + 1, 2))
            dst = jnp.where(it == NS_STEPS - 1, t, MAX_EXPERTS + lax.rem(it, 2))
            ns_step(ebuf.at[src], ebuf.at[dst], small_gram, small_poly, 512, 256)

        @pl.when(rank < N_DOWN)
        def _():
            give_back("d", ebuf.at[t], rank, ret_send.at[2 + t], ret_recv.at[6 + rank])
            back["d"][rank] = ebuf[t, pl.ds(pl.multiple_of(me * 64, 64), 64), :]

        @pl.when(rank >= N_DOWN)
        def _():
            give_back("u", ebuf.at[t], rank - N_DOWN, ret_send.at[2 + t], ret_recv.at[6 + rank])
            for d in range(GROUP):
                if EXPERT_BASE[d] + EXPERT_COUNT[d] > N_DOWN and EXPERT_COUNT[d]:
                    @pl.when(me == d)
                    def _():
                        back["u"][rank - N_DOWN] = ebuf[t, :, d * 128:(d + 1) * 128]

    for number, stack in enumerate(("q", "o", "d", "u")):
        weight_copy(stack, number).wait()
    owners = {(stack, i): owner for stack, i, owner, _ in places}
    for stack, i in RETURNS:
        owner, sem = owners[stack, i], SEM_BASE[stack] + i

        @pl.when(me != owner)
        def _():
            row = back[stack].at[i]
            pltpu.make_async_copy(row, row, ret_recv.at[sem]).wait()

        if stack == "u":
            finish(stack, i, lambda at: back["u"][i])
        else:
            finish(stack, i, lambda at: back[stack][i, at, :])

    for number in range(3):
        seven = gath.at[number, pl.ds(0, GROUP - 1)]
        pltpu.make_async_copy(seven, seven, norm_send.at[number]).wait()
    for stack, i, owner, slot in places:
        @pl.when(me != owner)
        def _():
            block = scaled[stack].at[i]
            if (stack, i) in EARLY:
                block = scaled[stack].at[i, pl.ds(EARLY_ROWS, 128 - EARLY_ROWS), :]
                early_copy(i).wait_send()
            pltpu.make_async_copy(block, block, fwd_send.at[SEM_BASE[stack] + i]).wait()
    for owner in QKV_OWNER:
        @pl.when(me == owner)
        def _():
            wait_parts("q", big.at[1], ret_send.at[0])
    for owner in OUT_OWNER:
        @pl.when(me == owner)
        def _():
            wait_parts("o", big.at[1, :, pl.ds(0, 1024)], ret_send.at[1])

    @pl.loop(0, count)
    def _(t):
        @pl.when(base + t < N_DOWN)
        def _():
            wait_parts("d", ebuf.at[t], ret_send.at[2 + t])

        @pl.when(base + t >= N_DOWN)
        def _():
            wait_parts("u", ebuf.at[t], ret_send.at[2 + t])


OUT_SPACE = pltpu.VMEM


def store_kernel(*refs):
    copies = [pltpu.make_async_copy(refs[k], refs[8 + k], refs[16].at[k]) for k in range(8)]
    for copy in copies:
        copy.start()
    for copy in copies:
        copy.wait()


def solution(mesh):
    row_spec = P("stage", "data", None)

    def local_step(*args):
        shapes = [args[k].shape for k in (0, 3, 6, 9) for _ in range(2)]
        any_space = pl.BlockSpec(memory_space=pl.ANY)
        kept = pl.pallas_call(
            kernel,
            out_shape=[OUT_SPACE(shape, F32) for shape in shapes],
            in_specs=[any_space] * 12,
            out_specs=[pl.BlockSpec(memory_space=OUT_SPACE)] * 8,
            scratch_shapes=[
                pltpu.VMEM((2, 1024, 2048), BF16),
                pltpu.VMEM((MAX_EXPERTS + 2, 512, 1024), BF16),
                pltpu.VMEM((1024, 1024), BF16),
                pltpu.VMEM((1024, 1024), BF16),
                pltpu.VMEM((3, 128, 2048), BF16),
                pltpu.VMEM((3, 128, 1024), BF16),
                pltpu.VMEM((12, 64, 1024), BF16),
                pltpu.VMEM((12, 512, 128), BF16),
                pltpu.VMEM((3, 128, 2048), BF16),
                pltpu.VMEM((3, 128, 1024), BF16),
                pltpu.VMEM((12, 64, 1024), BF16),
                pltpu.VMEM((12, 128, 512), BF16),
                pltpu.VMEM((12, 512, 128), BF16),
                pltpu.VMEM((3, 8, 128), F32),
                pltpu.VMEM((3, GROUP, 8, 128), F32),
                pltpu.VMEM((3, 8, 128), F32),
                pltpu.VMEM((GROUP, EARLY_ROWS, 1024), F32),
                pltpu.SemaphoreType.DMA((6,)),
                pltpu.SemaphoreType.DMA((6,)),
                pltpu.SemaphoreType.DMA((4,)),
                pltpu.SemaphoreType.DMA((3,)),
                pltpu.SemaphoreType.DMA((3,)),
                pltpu.SemaphoreType.DMA((30,)),
                pltpu.SemaphoreType.DMA((30,)),
                pltpu.SemaphoreType.DMA((2 + MAX_EXPERTS,)),
                pltpu.SemaphoreType.DMA((30,)),
                pltpu.SemaphoreType.DMA((2,)),
                pltpu.SemaphoreType.DMA((1,)),
            ],
            compiler_params=pltpu.CompilerParams(
                collective_id=0, has_side_effects=True, vmem_limit_bytes=VMEM_LIMIT),
        )(*args)
        return tuple(pl.pallas_call(
            store_kernel,
            out_shape=[jax.ShapeDtypeStruct(shape, F32) for shape in shapes],
            in_specs=[any_space] * 8,
            out_specs=[any_space] * 8,
            scratch_shapes=[pltpu.SemaphoreType.DMA((8,))],
            compiler_params=pltpu.CompilerParams(vmem_limit_bytes=1024 * 1024),
        )(*kept))

    return jax.shard_map(local_step, mesh=mesh, in_specs=(row_spec,) * 12, out_specs=(row_spec,) * 8, check_vma=False)
```

```python
import math
import jax
import jax.numpy as jnp
from jax import lax
from jax.experimental import pallas as pl
from jax.experimental.pallas import tpu as pltpu
from jax.sharding import PartitionSpec as P

NS_STEPS = 5
COEF_A = 3.4445
COEF_B = -4.7750
COEF_C = 2.0315
MOMENTUM = 0.95
LEARN_RATE = 0.04
DECAY = 0.2
NORM_EPS = 1e-7
RMS_MATCH = 0.2

GROUP = 8
MESH = pl.DeviceIdType.MESH
NT = (((1,), (1,)), ((), ()))
F32 = jnp.float32
BF16 = jnp.bfloat16

QKV_OWNER = (2, 1, 5)
OUT_OWNER = (3, 4, 7)
EXPERT_COUNT = (2, 0, 4, 5, 8, 1, 4, 0)
EXPERT_BASE = tuple(sum(EXPERT_COUNT[:d]) for d in range(GROUP))
EXPERT_OWNER = tuple(d for d in range(GROUP) for _ in range(EXPERT_COUNT[d]))
N_DOWN = 12
MAX_EXPERTS = 8
VMEM_LIMIT = 42 * 1024 * 1024


def send_order():
    halves = ([], [])
    sizes = {"q": 4, "o": 2, "e": 1}
    for kind, owners in (("o", OUT_OWNER), ("q", QKV_OWNER)):
        for index, owner in enumerate(owners):
            halves[owner // 4].append((kind, index))
    for half in range(2):
        devices = [d for d in range(4 * half, 4 * half + 4) if EXPERT_COUNT[d]]
        slots = []
        for d in devices:
            for t in range(EXPERT_COUNT[d]):
                slots.append(((t + 0.5) / EXPERT_COUNT[d] + (d in QKV_OWNER), d, t))
        for _, d, t in sorted(slots):
            halves[half].append(("e", EXPERT_BASE[d] + t))
    order, sent, place = [], [0, 0], [0, 0]
    while place[0] < len(halves[0]) or place[1] < len(halves[1]):
        half = 0 if sent[0] <= sent[1] else 1
        if place[half] == len(halves[half]):
            half = 1 - half
        item = halves[half][place[half]]
        place[half] += 1
        sent[half] += sizes[item[0]]
        order.append(item)
    return order


ORDER = send_order()


def pick(table, me):
    total = jnp.int32(0)
    for d, value in enumerate(table):
        if value:
            total = total + jnp.where(me == d, jnp.int32(value), jnp.int32(0))
    return total


def ns_step(src, dst, gram, poly, m, block):
    def rows_of(i):
        return pl.ds(pl.multiple_of(i * block, block), block)

    @pl.loop(0, m // block)
    def _(i):
        rows = rows_of(i)
        gram[rows, :] = lax.dot_general(src[rows, :], src[...], NT, preferred_element_type=F32).astype(BF16)

    @pl.loop(0, m // block)
    def _(i):
        rows = rows_of(i)
        part = gram[rows, :]
        square = jnp.dot(part, gram[...], preferred_element_type=F32)
        poly[rows, :] = (COEF_B * part.astype(F32) + COEF_C * square).astype(BF16)

    @pl.loop(0, m // block)
    def _(i):
        rows = rows_of(i)
        product = jnp.dot(poly[rows, :], src[...], preferred_element_type=F32)
        dst[rows, :] = (COEF_A * src[rows, :].astype(F32) + product).astype(BF16)


STACKS = {"q": (3, 128, 2048, 32, 0), "o": (3, 128, 1024, 64, 0), "d": (12, 64, 1024, 64, 0), "u": (12, 128, 512, 128, 12)}
SCALE = {"q": RMS_MATCH * math.sqrt(2048), "o": RMS_MATCH * math.sqrt(1024),
         "d": RMS_MATCH * math.sqrt(1024), "u": RMS_MATCH * math.sqrt(1024)}
EARLY = {("o", 0): 32, ("o", 1): 32}
EARLY_ROWS = 32
SEM_BASE = {"q": 0, "o": 3, "d": 6, "u": 18}


def place_of(kind, index):
    if kind == "q":
        return "q", index, QKV_OWNER[index], 0
    if kind == "o":
        return "o", index, OUT_OWNER[index], 0
    owner = EXPERT_OWNER[index]
    slot = index - EXPERT_BASE[owner]
    return ("d", index, owner, slot) if index < N_DOWN else ("u", index - N_DOWN, owner, slot)


def return_order():
    keys = []
    for kind, index in ORDER:
        stack, position, owner, slot = place_of(kind, index)
        held = 4 * (owner in QKV_OWNER) + 2 * (owner in OUT_OWNER)
        keys.append((held + (slot + 1 if kind == "e" else 0), len(keys), stack, position))
    return [(stack, position) for _, _, stack, position in sorted(keys)]


RETURNS = return_order()


def kernel(w_q, m_q, g_q, w_o, m_o, g_o, w_u, m_u, g_u, w_d, m_d, g_d,
           nw_q, nm_q, nw_o, nm_o, nw_u, nm_u, nw_d, nm_d,
           big, ebuf, gram, poly, xs_q, xs_o, xs_d, xs_u, bk_q, bk_o, bk_d, gs_u, bk_u,
           part, gath, den, early,
           m_sem, g_sem, w_sem, norm_send, norm_recv, fwd_send, fwd_recv, ret_send, ret_recv, early_send, early_recv):
    me = lax.axis_index("data")
    weights = {"q": w_q, "o": w_o, "d": w_d, "u": w_u}
    momenta = {"q": m_q, "o": m_o, "d": m_d, "u": m_u}
    gradients = {"q": g_q, "o": g_o, "d": g_d, "u": g_u}
    new_w = {"q": nw_q, "o": nw_o, "d": nw_d, "u": nw_u}
    new_m = {"q": nm_q, "o": nm_o, "d": nm_d, "u": nm_u}
    grad_in = {"q": bk_q, "o": bk_o, "d": bk_d, "u": gs_u}
    scaled = {"q": xs_q, "o": xs_o, "d": xs_d, "u": xs_u}
    back = {"q": bk_q, "o": bk_o, "d": bk_d, "u": bk_u}

    loads = {"q": [("q", i) for i in range(3)], "o": [("o", None)], "d": [("d", None)], "u": [("u", None)]}
    load_sem = {("q", 0): 0, ("q", 1): 1, ("q", 2): 2, ("o", None): 3, ("d", None): 4, ("u", None): 5}

    def part_of(ref, i):
        return ref if i is None else ref.at[i]

    def load_copies(key):
        stack, i = key
        sem = load_sem[key]
        return (pltpu.make_async_copy(part_of(momenta[stack], i), part_of(new_m[stack], i), m_sem.at[sem]),
                pltpu.make_async_copy(part_of(gradients[stack], i), part_of(grad_in[stack], i), g_sem.at[sem]))

    def weight_copy(stack, number):
        return pltpu.make_async_copy(weights[stack], new_w[stack], w_sem.at[number])

    for key in loads["o"]:
        for copy in load_copies(key):
            copy.start()

    barrier = pltpu.get_barrier_semaphore()
    for k in range(1, GROUP):
        pl.semaphore_signal(barrier, inc=1, device_id={"data": lax.rem(me + k, GROUP)}, device_id_type=MESH)

    part[...] = jnp.zeros_like(part)
    lane = lax.broadcasted_iota(jnp.int32, (8, 128), 1)

    def momentum_rows(stack, i, number, column):
        _, rows, cols, chunk, _ = STACKS[stack]
        lanes = jnp.zeros((1, 128), F32)
        for r in range(0, rows, chunk):
            at = pl.ds(r, chunk)
            mom = MOMENTUM * new_m[stack][i, at, :] + grad_in[stack][i, at, :].astype(F32)
            new_m[stack][i, at, :] = mom
            square = jnp.sum(mom * mom, axis=0, keepdims=True)
            for c in range(0, cols, 128):
                lanes = lanes + square[:, c:c + 128]
        total = jnp.sum(lanes, axis=1, keepdims=True)
        part[number] = jnp.where(lane == column, jnp.broadcast_to(total, (8, 128)), part[number])

    def push_norms(number):
        gath[number, me] = part[number]
        for k in range(1, GROUP):
            pltpu.make_async_remote_copy(
                src_ref=part.at[number], dst_ref=gath.at[number, me], send_sem=norm_send.at[number],
                recv_sem=norm_recv.at[number], device_id={"data": lax.rem(me + k, GROUP)}, device_id_type=MESH).start()

    def read_norms(number):
        seven = gath.at[number, pl.ds(0, GROUP - 1)]
        pltpu.make_async_copy(seven, seven, norm_recv.at[number]).wait()
        total = gath[number, 0]
        for d in range(1, GROUP):
            total = total + gath[number, d]
        den[number] = jnp.sqrt(total) + NORM_EPS

    def scale_rows(stack, i, number, column):
        _, rows, cols, chunk, _ = STACKS[stack]
        divisor = jnp.sum(jnp.where(lane[:1] == column, den[number, 0:1, :], 0.0), axis=1, keepdims=True)
        for r in range(0, rows, chunk):
            at = pl.ds(r, chunk)
            x = new_m[stack][i, at, :] / jnp.broadcast_to(divisor, (chunk, cols))
            if stack == "u":
                scaled[stack][i] = x.T.astype(BF16)
            else:
                scaled[stack][i, at, :] = x.astype(BF16)

    def block_of(stack, slot_ref, d):
        if stack == "u":
            return slot_ref.at[:, pl.ds(d * 128, 128)]
        rows = STACKS[stack][1]
        return slot_ref.at[pl.ds(d * rows, rows), :]

    def slot_of(stack, slot):
        if stack == "q":
            return big.at[0]
        if stack == "o":
            return big.at[0, :, pl.ds(0, 1024)]
        return ebuf.at[slot]

    def send_rows(stack, i, owner, slot):
        sem = SEM_BASE[stack] + i
        target = block_of(stack, slot_of(stack, slot), me)
        skip = EARLY.get((stack, i), 0)
        source, rest = scaled[stack].at[i], target
        if skip:
            source = scaled[stack].at[i, pl.ds(skip, 128 - skip), :]
            rest = slot_of(stack, slot).at[pl.ds(me * 128 + skip, 128 - skip), :]

        @pl.when(me != owner)
        def _():
            pltpu.make_async_remote_copy(
                src_ref=source, dst_ref=rest, send_sem=fwd_send.at[sem], recv_sem=fwd_recv.at[sem],
                device_id={"data": owner}, device_id_type=MESH).start()

        @pl.when(me == owner)
        def _():
            if stack == "u":
                for d in range(GROUP):
                    @pl.when(me == d)
                    def _():
                        ebuf[slot, :, d * 128:(d + 1) * 128] = scaled[stack][i]
            else:
                target[...] = scaled[stack][i]

    def momentum_stack(stack, number):
        for copy in load_copies((stack, None)):
            copy.wait()
        momentum_loop(stack, number)

    def momentum_loop(stack, number):
        @pl.loop(0, STACKS[stack][0])
        def _(i):
            momentum_rows(stack, i, number, STACKS[stack][4] + i)

    places = [place_of(kind, index) for kind, index in ORDER]

    def scale_and_send(stack, number):
        for kind, i, owner, slot in places:
            if kind == stack:
                scale_rows(stack, i, number, i)
                send_rows(stack, i, owner, slot)

    def early_copy(i):
        return pltpu.make_async_remote_copy(
            src_ref=new_m["o"].at[i, pl.ds(0, EARLY_ROWS), :], dst_ref=early.at[me], send_sem=early_send.at[i],
            recv_sem=early_recv.at[0], device_id={"data": OUT_OWNER[i]}, device_id_type=MESH)

    for copy in load_copies(("o", None)):
        copy.wait()
    for key in loads["q"] + loads["d"] + loads["u"]:
        for copy in load_copies(key):
            copy.start()
    momentum_loop("o", 0)
    pl.semaphore_wait(barrier, GROUP - 1)
    push_norms(0)
    for i in range(2):
        @pl.when(me != OUT_OWNER[i])
        def _():
            early_copy(i).start()
    for i in range(3):
        for copy in load_copies(("q", i)):
            copy.wait()
        momentum_rows("q", i, 1, i)
    push_norms(1)
    read_norms(0)
    scale_and_send("o", 0)
    momentum_stack("d", 2)
    momentum_stack("u", 2)
    push_norms(2)
    read_norms(1)
    scale_and_send("q", 1)
    for number, stack in enumerate(("q", "o", "d", "u")):
        weight_copy(stack, number).start()
    read_norms(2)
    for stack in ("d", "u"):
        @pl.loop(0, STACKS[stack][0])
        def _(i):
            scale_rows(stack, i, 2, STACKS[stack][4] + i)
    for stack, i, owner, slot in places:
        if stack in "du":
            send_rows(stack, i, owner, slot)

    def wait_parts(stack, slot_ref, sem):
        rows = 7 * STACKS[stack][1]
        part = slot_ref.at[:, pl.ds(0, rows)] if stack == "u" else slot_ref.at[pl.ds(0, rows), :]
        pltpu.make_async_copy(part, part, sem).wait()

    def give_back(stack, slot_ref, i, send_sem, recv_sem):
        half = me // 4
        crossing = [(1 - half) * 4 + k for k in range(4)]
        for dst in crossing + [half * 4 + lax.rem(me + k, 4) for k in range(1, 4)]:
            pltpu.make_async_remote_copy(
                src_ref=block_of(stack, slot_ref, dst), dst_ref=back[stack].at[i], send_sem=send_sem, recv_sem=recv_sem,
                device_id={"data": dst}, device_id_type=MESH).start()

    def new_weight(w, x, stack):
        return w - LEARN_RATE * (SCALE[stack] * x.astype(F32) + DECAY * w)

    def finish(stack, i, source):
        _, rows, cols, chunk, _ = STACKS[stack]
        for r in range(0, rows, chunk):
            at = pl.ds(r, chunk)
            x = source(at)
            if stack == "u":
                x = x.astype(F32).T
            new_w[stack][i, at, :] = new_weight(new_w[stack][i, at, :], x, stack)

    for index, owner in enumerate(QKV_OWNER):
        @pl.when(me == owner)
        def _():
            wait_parts("q", big.at[0], fwd_recv.at[index])

    @pl.when((me == QKV_OWNER[0]) | (me == QKV_OWNER[1]) | (me == QKV_OWNER[2]))
    def _():
        @pl.loop(0, NS_STEPS)
        def _(it):
            now = lax.rem(it, 2)
            ns_step(big.at[now], big.at[1 - now], gram, poly, 1024, 256)

    for index, owner in enumerate(QKV_OWNER):
        @pl.when(me == owner)
        def _():
            give_back("q", big.at[1], index, ret_send.at[0], ret_recv.at[index])
            back["q"][index] = big[1, pl.ds(owner * 128, 128), :]

    for index, owner in enumerate(OUT_OWNER):
        @pl.when(me == owner)
        def _():
            if ("o", index) not in EARLY:
                wait_parts("o", big.at[0, :, pl.ds(0, 1024)], fwd_recv.at[3 + index])
                return
            part_rows = big.at[0, pl.ds(0, 7 * (128 - EARLY_ROWS)), pl.ds(0, 1024)]
            pltpu.make_async_copy(part_rows, part_rows, fwd_recv.at[3 + index]).wait()
            seven = early.at[pl.ds(0, GROUP - 1)]
            pltpu.make_async_copy(seven, seven, early_recv.at[0]).wait()
            divisor = jnp.sum(jnp.where(lane[:1] == index, den[0, 0:1, :], 0.0), axis=1, keepdims=True)

            @pl.loop(0, GROUP)
            def _(d):
                @pl.when(d != me)
                def _():
                    x = early[d] / jnp.broadcast_to(divisor, (EARLY_ROWS, 1024))
                    big[0, pl.ds(pl.multiple_of(d * 128, 128), EARLY_ROWS), 0:1024] = x.astype(BF16)

    @pl.when((me == OUT_OWNER[0]) | (me == OUT_OWNER[1]) | (me == OUT_OWNER[2]))
    def _():
        @pl.loop(0, NS_STEPS)
        def _(it):
            now = lax.rem(it, 2)
            ns_step(big.at[now, :, pl.ds(0, 1024)], big.at[1 - now, :, pl.ds(0, 1024)], gram, poly, 1024, 512)

    for index, owner in enumerate(OUT_OWNER):
        @pl.when(me == owner)
        def _():
            give_back("o", big.at[1, :, pl.ds(0, 1024)], index, ret_send.at[1], ret_recv.at[3 + index])
            back["o"][index] = big[1, pl.ds(owner * 128, 128), 0:1024]

    base, count = pick(EXPERT_BASE, me), pick(EXPERT_COUNT, me)
    small_gram, small_poly = gram.at[pl.ds(0, 512), pl.ds(0, 512)], poly.at[pl.ds(0, 512), pl.ds(0, 512)]

    @pl.loop(0, count)
    def _(t):
        rank = base + t

        @pl.when(rank < N_DOWN)
        def _():
            wait_parts("d", ebuf.at[t], fwd_recv.at[6 + rank])

        @pl.when(rank >= N_DOWN)
        def _():
            wait_parts("u", ebuf.at[t], fwd_recv.at[6 + rank])

        @pl.loop(0, NS_STEPS)
        def _(it):
            src = jnp.where(it == 0, t, MAX_EXPERTS + lax.rem(it + 1, 2))
            dst = jnp.where(it == NS_STEPS - 1, t, MAX_EXPERTS + lax.rem(it, 2))
            ns_step(ebuf.at[src], ebuf.at[dst], small_gram, small_poly, 512, 512)

        @pl.when(rank < N_DOWN)
        def _():
            give_back("d", ebuf.at[t], rank, ret_send.at[2 + t], ret_recv.at[6 + rank])
            back["d"][rank] = ebuf[t, pl.ds(pl.multiple_of(me * 64, 64), 64), :]

        @pl.when(rank >= N_DOWN)
        def _():
            give_back("u", ebuf.at[t], rank - N_DOWN, ret_send.at[2 + t], ret_recv.at[6 + rank])
            for d in range(GROUP):
                if EXPERT_BASE[d] + EXPERT_COUNT[d] > N_DOWN and EXPERT_COUNT[d]:
                    @pl.when(me == d)
                    def _():
                        back["u"][rank - N_DOWN] = ebuf[t, :, d * 128:(d + 1) * 128]

    for number, stack in enumerate(("q", "o", "d", "u")):
        weight_copy(stack, number).wait()
    owners = {(stack, i): owner for stack, i, owner, _ in places}
    for stack, i in RETURNS:
        owner, sem = owners[stack, i], SEM_BASE[stack] + i

        @pl.when(me != owner)
        def _():
            row = back[stack].at[i]
            pltpu.make_async_copy(row, row, ret_recv.at[sem]).wait()

        if stack == "u":
            finish(stack, i, lambda at: back["u"][i])
        else:
            finish(stack, i, lambda at: back[stack][i, at, :])

    for number in range(3):
        seven = gath.at[number, pl.ds(0, GROUP - 1)]
        pltpu.make_async_copy(seven, seven, norm_send.at[number]).wait()
    for stack, i, owner, slot in places:
        @pl.when(me != owner)
        def _():
            block = scaled[stack].at[i]
            if (stack, i) in EARLY:
                block = scaled[stack].at[i, pl.ds(EARLY_ROWS, 128 - EARLY_ROWS), :]
                early_copy(i).wait_send()
            pltpu.make_async_copy(block, block, fwd_send.at[SEM_BASE[stack] + i]).wait()
    for owner in QKV_OWNER:
        @pl.when(me == owner)
        def _():
            wait_parts("q", big.at[1], ret_send.at[0])
    for owner in OUT_OWNER:
        @pl.when(me == owner)
        def _():
            wait_parts("o", big.at[1, :, pl.ds(0, 1024)], ret_send.at[1])

    @pl.loop(0, count)
    def _(t):
        @pl.when(base + t < N_DOWN)
        def _():
            wait_parts("d", ebuf.at[t], ret_send.at[2 + t])

        @pl.when(base + t >= N_DOWN)
        def _():
            wait_parts("u", ebuf.at[t], ret_send.at[2 + t])


OUT_SPACE = pltpu.VMEM


def store_kernel(*refs):
    copies = [pltpu.make_async_copy(refs[k], refs[8 + k], refs[16].at[k]) for k in range(8)]
    for copy in copies:
        copy.start()
    for copy in copies:
        copy.wait()


def solution(mesh):
    row_spec = P("stage", "data", None)

    def local_step(*args):
        shapes = [args[k].shape for k in (0, 3, 6, 9) for _ in range(2)]
        any_space = pl.BlockSpec(memory_space=pl.ANY)
        kept = pl.pallas_call(
            kernel,
            out_shape=[OUT_SPACE(shape, F32) for shape in shapes],
            in_specs=[any_space] * 12,
            out_specs=[pl.BlockSpec(memory_space=OUT_SPACE)] * 8,
            scratch_shapes=[
                pltpu.VMEM((2, 1024, 2048), BF16),
                pltpu.VMEM((MAX_EXPERTS + 2, 512, 1024), BF16),
                pltpu.VMEM((1024, 1024), BF16),
                pltpu.VMEM((1024, 1024), BF16),
                pltpu.VMEM((3, 128, 2048), BF16),
                pltpu.VMEM((3, 128, 1024), BF16),
                pltpu.VMEM((12, 64, 1024), BF16),
                pltpu.VMEM((12, 512, 128), BF16),
                pltpu.VMEM((3, 128, 2048), BF16),
                pltpu.VMEM((3, 128, 1024), BF16),
                pltpu.VMEM((12, 64, 1024), BF16),
                pltpu.VMEM((12, 128, 512), BF16),
                pltpu.VMEM((12, 512, 128), BF16),
                pltpu.VMEM((3, 8, 128), F32),
                pltpu.VMEM((3, GROUP, 8, 128), F32),
                pltpu.VMEM((3, 8, 128), F32),
                pltpu.VMEM((GROUP, EARLY_ROWS, 1024), F32),
                pltpu.SemaphoreType.DMA((6,)),
                pltpu.SemaphoreType.DMA((6,)),
                pltpu.SemaphoreType.DMA((4,)),
                pltpu.SemaphoreType.DMA((3,)),
                pltpu.SemaphoreType.DMA((3,)),
                pltpu.SemaphoreType.DMA((30,)),
                pltpu.SemaphoreType.DMA((30,)),
                pltpu.SemaphoreType.DMA((2 + MAX_EXPERTS,)),
                pltpu.SemaphoreType.DMA((30,)),
                pltpu.SemaphoreType.DMA((2,)),
                pltpu.SemaphoreType.DMA((1,)),
            ],
            compiler_params=pltpu.CompilerParams(
                collective_id=0, has_side_effects=True, vmem_limit_bytes=VMEM_LIMIT),
        )(*args)
        return tuple(pl.pallas_call(
            store_kernel,
            out_shape=[jax.ShapeDtypeStruct(shape, F32) for shape in shapes],
            in_specs=[any_space] * 8,
            out_specs=[any_space] * 8,
            scratch_shapes=[pltpu.SemaphoreType.DMA((8,))],
            compiler_params=pltpu.CompilerParams(vmem_limit_bytes=1024 * 1024),
        )(*kept))

    return jax.shard_map(local_step, mesh=mesh, in_specs=(row_spec,) * 12, out_specs=(row_spec,) * 8, check_vma=False)
```
